128 devices in a mesh: gx: 8 (over z_lo, x), gy: 16 (over z_hi, y, core).
Axes of the slice: x: 4, y: 4, z: 4 (z_hi: 2, z_lo: 2; z = z_hi * 2 + z_lo), core: 2. Of those that a mesh axis runs over, the one named last changes fastest.
Arguments:
- gradient: float32 [16, 1024, 2048], P(None, 'gy', 'gx'), may hold values from -6 to 6
- members: float32 [8, 16, 512, 1024], P(None, None, 'gy', 'gx'), may hold values from -6 to 6
Outputs:
- covariance_product: float32 [16, 1024, 2048], P(None, 'gy', 'gx')
The draws below stay inside these ranges and needn't reach their ends.
All inputs are finite; a program needn't handle non-finite values.
Results may differ from the reference program's by a relative error of at most 0.0001.
Values sent between devices are 32-bit elements; how exact they have to be, the bound alone decides.
A program may use at most 128 MiB of HBM per device.

```python
import jax
import jax.numpy as jnp
from jax import lax

LEV = 16
MEM = 8
NYF = 1024
NXF = 2048
NYE = 512
NXE = 1024


def level_of(own_key, extent, cuts, low, top_value):
    loudness, own = 1.0, jax.random.fold_in(own_key, 6)
    for dim, blocks in cuts:
        steps = jnp.exp(jax.random.uniform(jax.random.fold_in(own, dim), (blocks,), jnp.float32, low / len(cuts), top_value / len(cuts)))
        loudness = loudness * jnp.repeat(steps, extent[dim] // blocks).reshape([-1 if axis == dim else 1 for axis in range(len(extent))])
    return loudness


def normal_values(own_key, dims, width, bound, split=(), kind=jnp.bfloat16):
    gain = level_of(own_key, dims, split, -0.22, 0.18) if split else 1.0
    values = jax.random.normal(own_key, dims, jnp.float32) * width * gain
    return jnp.minimum(jnp.maximum(values, -bound), bound).astype(kind)


def setup_inputs(seed: int = 0) -> dict:
    key_list = jax.random.split(jax.random.key(seed), 3)
    gradient = normal_values(key_list[0], (LEV, NYF, NXF), 1.0, 6.0, ((1, 16), (2, 8)), jnp.float32)
    members = normal_values(key_list[1], (MEM, LEV, NYE, NXE), 1.0, 6.0, ((2, 16), (3, 8)), jnp.float32)
    return {"gradient": gradient, "members": members}


beta_raw = [(1.0 - (offset - 4) ** 2 / 25.0) ** 2 for offset in range(9)]
beta_taps = [value / sum(beta_raw) for value in beta_raw]
generations = ((1, 0.5), (2, 0.075), (4, 0.0125))


def convolve(padded):
    across = padded.shape[-1] - 8
    result = beta_taps[0] * padded[..., 0:across]
    for offset in range(1, 9):
        result = result + beta_taps[offset] * padded[..., offset:offset + across]
    height = result.shape[-2] - 8
    output = beta_taps[0] * result[..., 0:height, :]
    for offset in range(1, 9):
        output = output + beta_taps[offset] * result[..., offset:offset + height, :]
    return output


def coarsen(field, factor):
    shape = field.shape
    lead = tuple(shape[:-2])
    return field.reshape(lead + (shape[-2] // factor, factor, shape[-1] // factor, factor)).sum(axis=(-3, -1))


def refine(field, factor):
    return jnp.repeat(jnp.repeat(field, factor, axis=-2), factor, axis=-1)


def pad_rim(field):
    return jnp.pad(field, ((0, 0), (4, 4), (4, 4)))


def localise(member_field):
    total = jnp.zeros(member_field.shape, jnp.float32)
    for factor, weight in generations:
        block = coarsen(member_field, factor)
        once = convolve(pad_rim(block))
        twice = convolve(pad_rim(once))
        total = total + weight * refine(twice, factor)
    return total


def reference(gradient, members):
    odd = gradient[:, :, 1::2]
    earlier = jnp.pad(odd[:, :, :-1], ((0, 0), (0, 0), (1, 0)))
    across = gradient[:, :, 0::2] + 0.5 * (odd + earlier)
    odd_rows = across[:, 1::2, :]
    earlier_rows = jnp.pad(odd_rows[:, :-1, :], ((0, 0), (1, 0), (0, 0)))
    coarse = across[:, 0::2, :] + 0.5 * (odd_rows + earlier_rows)

    def per_member(member):
        return member * localise(member * coarse)

    weighted = lax.map(per_member, members)
    combined = jnp.sum(weighted, axis=0) / (MEM - 1)
    later_rows = jnp.pad(combined[:, 1:, :], ((0, 0), (0, 1), (0, 0)))
    half_rows = 0.5 * (combined + later_rows)
    rows = jnp.stack([combined, half_rows], axis=2).reshape(LEV, 2 * NYE, NXE)
    later_cols = jnp.pad(rows[:, :, 1:], ((0, 0), (0, 0), (0, 1)))
    half_cols = 0.5 * (rows + later_cols)
    return jnp.stack([rows, half_cols], axis=3).reshape(LEV, NYF, NXF)
```

```python
import functools

import jax
import jax.numpy as jnp
import ml_dtypes
import numpy as np
from jax import lax
from jax.experimental import pallas as pl
from jax.experimental.pallas import tpu as pltpu
from jax.sharding import PartitionSpec as P

MESH = pl.DeviceIdType.MESH
F32, BF16 = jnp.float32, jnp.bfloat16
LEV, MEM = 16, 8
CHUNKS = 4
MPAD = 40
APAD = 72

beta_raw = [(1.0 - (offset - 4) ** 2 / 25.0) ** 2 for offset in range(9)]
beta_taps = [value / sum(beta_raw) for value in beta_raw]
generations = ((1, 0.5), (2, 0.075), (4, 0.0125))
row_taps = [beta_taps[4 + k] / beta_taps[4] for k in range(5)]


def halves(matrix):
    hi = matrix.astype(ml_dtypes.bfloat16)
    lo = (matrix - hi.astype(np.float64)).astype(ml_dtypes.bfloat16)
    return np.stack([hi, lo])


def band(outputs):
    matrix = np.zeros((outputs + 8, outputs))
    for column in range(outputs):
        matrix[column : column + 9, column] = beta_taps
    return matrix


def column_filter(factor, weight, west_edge, east_edge):
    count = 128 // factor
    inside = np.ones(count + 8)
    if west_edge:
        inside[:4] = 0.0
    if east_edge:
        inside[-4:] = 0.0
    both = band(count + 8) @ (inside[:, None] * band(count))
    both = np.repeat(both, factor, axis=1) * (weight / (MEM - 1) * beta_taps[4] ** 2)
    result = np.zeros((256, 128 * factor))
    for part in range(factor):
        columns = slice(part * 128, part * 128 + 128)
        start = part * count
        result[start : start + count, columns] = both[8 : count + 8]
        result[128 + start : 136 + start, columns] = both[:8]
        result[136 + start : 144 + start, columns] = both[count + 8 :]
    return halves(result)


def constants():
    filters = []
    for factor, weight in generations:
        kinds = [column_filter(factor, weight, *edges) for edges in ((True, False), (False, False), (False, True))]
        filters.append(np.stack(kinds))
    pairs = np.zeros((256, 128))
    reduce_columns = np.zeros((256, 128))
    for lane in range(128):
        pairs[2 * lane : 2 * lane + 2, lane] = 1.0
        reduce_columns[2 * lane, lane] = 1.0
        reduce_columns[2 * lane + 1, lane] = 0.5
        if lane:
            reduce_columns[2 * lane - 1, lane] = 0.5
    small = np.stack([pairs, reduce_columns]).astype(ml_dtypes.bfloat16)
    spread = np.zeros((256, 256))
    for lane in range(128):
        spread[lane, 2 * lane] = 1.0
        spread[lane, 2 * lane + 1] = 0.5
        spread[lane + 1, 2 * lane + 1] = 0.5
    return filters, small, spread.astype(ml_dtypes.bfloat16)


def split(value):
    hi = value.astype(BF16)
    return hi, (value - hi.astype(F32)).astype(BF16)


def dot(a, b):
    return jnp.dot(a, b, preferred_element_type=F32)


def exact_dot(value, matrix):
    rows = value.shape[0]
    hi, lo = split(value)
    both = dot(jnp.concatenate([hi, lo], axis=0), matrix)
    return both[:rows] + both[rows:]


def full_dot(value, hi_matrix, lo_matrix):
    hi, lo = split(value)
    return dot(hi, hi_matrix) + dot(lo, hi_matrix) + dot(hi, lo_matrix)


def roll(value, shift):
    shift %= 128
    return value if shift == 0 else pltpu.roll(value, shift, 1)


def main_kernel(
    nx, ny,
    g_hbm, m_hbm, w1_hbm, w2_hbm, w4_hbm, small_hbm,
    comb, extra,
    gv, mv, w1, w2, w4, small,
    ac, cz, px, p2x, p4x, y1, y2, y4, sp, rp, o2, o4,
    col_out, col_in, row_out, row_in, corner_out, corner_in,
    end_row_in, end_col_out, end_col_in, end_corner_in,
    local_sem, s1, r1, ys, yr, xs, xr, s3, r3,
):
    gx, gy = lax.axis_index("gx"), lax.axis_index("gy")
    has_w, has_e = gx > 0, gx < nx - 1
    has_s, has_n = gy > 0, gy < ny - 1

    kind = 1 - (gx == 0).astype(jnp.int32) + (gx == nx - 1).astype(jnp.int32)
    g_copies = [
        pltpu.make_async_copy(g_hbm.at[:, :, pl.ds(side * 128, 128)], gv.at[side], local_sem.at[side * 6])
        for side in range(2)
    ]
    m_copy = pltpu.make_async_copy(m_hbm, mv.at[:, :, pl.ds(0, 32), :], local_sem.at[1])
    small_copy = pltpu.make_async_copy(small_hbm, small, local_sem.at[2])
    w1_copy = pltpu.make_async_copy(w1_hbm.at[kind], w1, local_sem.at[3])
    w2_copy = pltpu.make_async_copy(w2_hbm.at[kind], w2, local_sem.at[4])
    w4_copy = pltpu.make_async_copy(w4_hbm.at[kind], w4, local_sem.at[5])
    for copy in (*g_copies, small_copy, m_copy, w1_copy, w2_copy, w4_copy):
        copy.start()

    barrier = pltpu.get_barrier_semaphore()
    around = [
        (has_w, -1, 0), (has_e, 1, 0), (has_s, 0, -1), (has_n, 0, 1),
        (has_w & has_s, -1, -1), (has_e & has_n, 1, 1),
    ]

    def at(dx, dy):
        return {"gx": gx + dx, "gy": gy + dy}

    for there, dx, dy in around:
        @pl.when(there)
        def _(dx=dx, dy=dy):
            pl.semaphore_signal(barrier, inc=1, device_id=at(dx, dy), device_id_type=MESH)

    @pl.when(jnp.logical_not(has_s))
    def _():
        px[:, pl.ds(0, 8)] = jnp.zeros((CHUNKS, 8, 32, 128), F32)
        p2x[:, pl.ds(0, 4)] = jnp.zeros((CHUNKS, 4, 16, 128), F32)
        p4x[:, pl.ds(0, 4)] = jnp.zeros((CHUNKS, 4, 8, 128), F32)
        row_in[...] = jnp.zeros((16, 128), F32)

    @pl.when(jnp.logical_not(has_n))
    def _():
        px[:, pl.ds(40, 8)] = jnp.zeros((CHUNKS, 8, 32, 128), F32)
        p2x[:, pl.ds(28, 4)] = jnp.zeros((CHUNKS, 4, 16, 128), F32)
        p4x[:, pl.ds(20, 4)] = jnp.zeros((CHUNKS, 4, 8, 128), F32)
        end_row_in[...] = jnp.zeros((16, 128), F32)

    @pl.when(jnp.logical_not(has_w))
    def _():
        rp[0] = jnp.zeros((CHUNKS, 112, 128), F32)
        col_in[...] = jnp.zeros((8, 128), F32)

    @pl.when(jnp.logical_not(has_e))
    def _():
        rp[1] = jnp.zeros((CHUNKS, 112, 128), F32)
        end_col_in[...] = jnp.zeros((16, 128), F32)

    @pl.when(jnp.logical_not(has_w & has_s))
    def _():
        corner_in[...] = jnp.zeros((16, 128), F32)

    @pl.when(jnp.logical_not(has_e & has_n))
    def _():
        end_corner_in[...] = jnp.zeros((16, 128), F32)

    def remote(src, dst, send, recv, dx, dy):
        return pltpu.make_async_remote_copy(
            src_ref=src, dst_ref=dst, send_sem=send, recv_sem=recv, device_id=at(dx, dy), device_id_type=MESH
        )

    col_copy = remote(col_out, col_in, s1.at[0], r1.at[0], 1, 0)
    row_copy = remote(row_out, row_in, s1.at[1], r1.at[1], 0, 1)
    corner_copy = remote(corner_out, corner_in, s1.at[2], r1.at[2], 1, 1)
    end_row_copy = remote(comb.at[0], end_row_in, s3.at[0], r3.at[0], 0, -1)
    end_col_copy = remote(end_col_out, end_col_in, s3.at[1], r3.at[1], -1, 0)
    end_corner_copy = remote(end_col_out, end_corner_in, s3.at[2], r3.at[2], -1, -1)

    def y_copies(c, direction):
        if direction == 0:
            places = ((px, 32, 0, 8), (p2x, 16, 0, 4), (p4x, 8, 0, 4))
            dy = 1
        else:
            places = ((px, 8, 40, 8), (p2x, 12, 28, 4), (p4x, 12, 20, 4))
            dy = -1
        return [
            remote(ref.at[c, pl.ds(src, n)], ref.at[c, pl.ds(dst, n)], ys.at[direction, c, i], yr.at[direction, c, i], 0, dy)
            for i, (ref, src, dst, n) in enumerate(places)
        ]

    def x_copy(c, direction):
        if direction == 0:
            return remote(sp.at[0, c], rp.at[0, c], xs.at[0, c], xr.at[0, c], 1, 0)
        return remote(sp.at[1, c], rp.at[1, c], xs.at[1, c], xr.at[1, c], -1, 0)

    lane = lax.broadcasted_iota(jnp.int32, (8, 128), 1)
    first_lane = lane == 0

    for copy in g_copies:
        copy.wait()
    gr = gv.at[1].reshape(LEV * 64, 128)
    parts = []
    for quarter in range(4):
        packed = jnp.zeros((8, 128), F32)
        for i in range(quarter * 32, quarter * 32 + 32):
            value = gr[pl.ds(i * 8, 8), :]
            packed = jnp.where(lane == i, roll(value, i + 1), packed)
        parts.append(packed)
    col_out[...] = jnp.where(lane < 64, jnp.where(lane < 32, parts[0], parts[1]), jnp.where(lane < 96, parts[2], parts[3]))
    for h in range(2):
        corner_out[pl.ds(h * 8, 8), :] = gr[pl.ds(h * 8 * 64 + 63, 8, stride=64), :]

    small_copy.wait()

    def reduce_columns(l, carry):
        ac[l, pl.ds(0, 64), :] = exact_dot(jnp.concatenate([gv[0, l], gv[1, l]], axis=1), small[1])
        return carry

    lax.fori_loop(0, LEV, reduce_columns, 0)
    ar = ac.reshape(LEV * APAD, 128)

    def across_row(y, h):
        return ar[pl.ds(h * 8 * APAD + y, 8, stride=APAD), :]

    for h in range(2):
        row_out[pl.ds(h * 8, 8), :] = across_row(63, h)

    pl.semaphore_wait(barrier, sum(there.astype(jnp.int32) for there, _, _ in around))

    @pl.when(has_e)
    def _():
        col_copy.start()

    @pl.when(has_n)
    def _():
        row_copy.start()

    @pl.when(has_e & has_n)
    def _():
        corner_copy.start()

    @pl.when(has_w)
    def _():
        col_copy.wait_recv()
        value = 0.5 * col_in[...]
        for l in range(LEV):
            for block in range(8):
                tile = ac[l, pl.ds(block * 8, 8), :]
                ac[l, pl.ds(block * 8, 8), :] = tile + jnp.where(first_lane, roll(value, -(l * 8 + block)), 0.0)

    @pl.when(has_s)
    def _():
        row_copy.wait_recv()

    @pl.when(has_w & has_s)
    def _():
        corner_copy.wait_recv()

    before = []
    for h in range(2):
        corner = corner_in[pl.ds(h * 8, 8), :]
        before.append(row_in[pl.ds(h * 8, 8), :] + jnp.where(first_lane, 0.5 * roll(corner, 1), 0.0))

    def reduce_rows(j, carry):
        odd_rows = []
        for h in range(2):
            odd = across_row(2 * j + 1, h)
            cz[j, pl.ds(h * 8, 8), :] = across_row(2 * j, h) + 0.5 * (odd + carry[h])
            odd_rows.append(odd)
        return tuple(odd_rows)

    lax.fori_loop(0, 32, reduce_rows, tuple(before))

    mr = mv.reshape(MEM * LEV * MPAD, 128)

    def member(c, m2, h, y):
        return mr[pl.ds(((2 * c + m2) * LEV + h * 8) * MPAD + y, 8, stride=MPAD), :]

    def half_blocks(c, first, count):
        rows = []
        for k in range(count):
            pair = px[c, 2 * (first + k) - 8] + px[c, 2 * (first + k) - 7]
            for m2 in range(2):
                rows.append(jnp.concatenate([pair[m2 * 16 : m2 * 16 + 8], pair[m2 * 16 + 8 : m2 * 16 + 16]], axis=1))
        value = exact_dot(jnp.concatenate(rows, axis=0), small[0])
        p2x[c, pl.ds(first, count)] = value.reshape(count, 16, 128)

    def quarter_blocks(c, first, count):
        rows = []
        for k in range(count):
            pair = p2x[c, 2 * (first + k) - 8] + p2x[c, 2 * (first + k) - 7]
            rows.append(jnp.concatenate([pair[:8], pair[8:]], axis=1))
        value = exact_dot(jnp.concatenate(rows, axis=0), small[0])
        p4x[c, pl.ds(first, count)] = value.reshape(count, 8, 128)

    m_copy.wait()

    def make_products(c, carry):
        def row(y, carry):
            for m2 in range(2):
                for h in range(2):
                    px[c, 8 + y, pl.ds(m2 * 16 + h * 8, 8), :] = member(c, m2, h, y) * cz[y, pl.ds(h * 8, 8), :]
            return carry

        lax.fori_loop(0, 32, row, 0, unroll=4)
        half_blocks(c, 8, 8)
        half_blocks(c, 16, 8)
        quarter_blocks(c, 8, 8)

        @pl.when(has_n)
        def _():
            for copy in y_copies(c, 0):
                copy.start()

        @pl.when(has_s)
        def _():
            for copy in y_copies(c, 1):
                copy.start()

        return carry

    lax.fori_loop(0, CHUNKS, make_products, 0)

    low = jnp.where(has_s, 1.0, 0.0).astype(F32)
    high = jnp.where(has_n, 1.0, 0.0).astype(F32)

    def one_pass(window):
        total = window[4]
        for k in range(1, 5):
            total = total + row_taps[k] * (window[4 - k] + window[4 + k])
        return total

    def filter_rows(c, source, target, rows, fields, width, base):
        group = width // 8
        place = (lane % width) // 8

        def column(f, carry):
            at_f = pl.ds(pl.multiple_of(f * 8, 8), 8)
            window, passed = [], []
            east = west = None
            for row in range(rows):
                window.append(source[c, row, at_f, :])
                if row < 8:
                    continue
                once = one_pass(window[-9:])
                if row - 8 < 4:
                    once = once * low
                if row >= rows - 4:
                    once = once * high
                passed.append(once)
                if len(passed) < 9:
                    continue
                twice = one_pass(passed[-9:])
                y = row - 16
                target[c, y, at_f, :] = twice
                r = y % group
                to_west, to_east = roll(twice, 8 * r), roll(twice, 8 * r + 8 - width)
                if r == 0:
                    west, east = to_west, to_east
                else:
                    west, east = jnp.where(place == r, to_west, west), jnp.where(place == r, to_east, east)
                if r == group - 1:
                    start = pl.multiple_of(base + (y // group) * fields + f * 8, 8)
                    sp[0, c, pl.ds(start, 8), :] = east
                    sp[1, c, pl.ds(start, 8), :] = west
            return carry

        lax.fori_loop(0, fields // 8, column, 0)

    def rows_stage(c, carry):
        @pl.when(has_s)
        def _():
            for copy in y_copies(c, 0):
                copy.wait_recv()

        @pl.when(has_n)
        def _():
            for copy in y_copies(c, 1):
                copy.wait_recv()

        half_blocks(c, 4, 4)
        half_blocks(c, 24, 4)
        quarter_blocks(c, 4, 4)
        quarter_blocks(c, 16, 4)
        filter_rows(c, px, y1, 48, 32, 128, 0)
        filter_rows(c, p2x, y2, 32, 16, 64, 64)
        filter_rows(c, p4x, y4, 24, 8, 32, 96)

        @pl.when(has_e)
        def _():
            x_copy(c, 0).start()

        @pl.when(has_w)
        def _():
            x_copy(c, 1).start()

        return carry

    lax.fori_loop(0, CHUNKS, rows_stage, 0)

    comb[...] = jnp.zeros((32, 16, 128), F32)
    w1_copy.wait()
    w2_copy.wait()
    w4_copy.wait()

    def halo(c, start, fields, r, width):
        west, east = rp[0, c, pl.ds(start, fields), :], rp[1, c, pl.ds(start, fields), :]
        take_west = lax.broadcasted_iota(jnp.int32, (fields, 128), 1) % width < 8
        return jnp.where(take_west, roll(west, -8 * r), roll(east, 8 - 8 * r))

    def columns_stage(c, carry):
        @pl.when(has_w)
        def _():
            x_copy(c, 0).wait_recv()

        @pl.when(has_e)
        def _():
            x_copy(c, 1).wait_recv()

        sides = [halo(c, 96 + (q // 4) * 8, 8, q % 4, 32) for q in range(8)]
        value = jnp.concatenate([y4[c].reshape(64, 128), jnp.concatenate(sides, axis=0)], axis=1)
        o4[...] = full_dot(value, w4[0], w4[1])
        sides = [halo(c, 64 + (q // 8) * 16, 16, q % 8, 64) for q in range(16)]
        value = jnp.concatenate([y2[c].reshape(256, 128), jnp.concatenate(sides, axis=0)], axis=1)
        o2[...] = full_dot(value, w2[0], w2[1])

        def block(b, carry):
            for part in range(2):
                first = b * 16 + part * 8
                start = pl.multiple_of(b * 32, 32)
                sides = [halo(c, start, 32, part * 8 + r, 128) for r in range(8)]
                rows = y1[c, pl.ds(first, 8)].reshape(256, 128)
                value = full_dot(jnp.concatenate([rows, jnp.concatenate(sides, axis=0)], axis=1), w1[0], w1[1])
                for r in range(8):
                    y = first + r
                    at2 = pl.multiple_of((b * 8 + part * 4 + r // 2) * 16, 16)
                    at4 = pl.multiple_of((b * 4 + part * 2 + r // 4) * 8, 8)
                    for h in range(2):
                        total = comb[y, pl.ds(h * 8, 8), :]
                        for m2 in range(2):
                            begin = r * 32 + m2 * 16 + h * 8
                            local = value[begin : begin + 8]
                            local = local + o2[pl.ds(at2 + m2 * 8, 8), pl.ds(h * 128, 128)]
                            local = local + o4[pl.ds(at4, 8), pl.ds((m2 * 2 + h) * 128, 128)]
                            total = total + member(c, m2, h, y) * local
                        comb[y, pl.ds(h * 8, 8), :] = total
            return carry

        lax.fori_loop(0, 2, block, 0)
        return carry

    lax.fori_loop(0, CHUNKS, columns_stage, 0)

    for h in range(2):
        packed = comb[0, pl.ds(h * 8, 8), :]
        for y in range(1, 32):
            packed = jnp.where(lane == y, roll(comb[y, pl.ds(h * 8, 8), :], y), packed)
        end_col_out[pl.ds(h * 8, 8), :] = packed

    @pl.when(has_s)
    def _():
        end_row_copy.start()

    @pl.when(has_w)
    def _():
        end_col_copy.start()

    @pl.when(has_w & has_s)
    def _():
        end_corner_copy.start()

    def send_waits(c, carry):
        @pl.when(has_n)
        def _():
            for copy in y_copies(c, 0):
                copy.wait_send()

        @pl.when(has_s)
        def _():
            for copy in y_copies(c, 1):
                copy.wait_send()

        @pl.when(has_e)
        def _():
            x_copy(c, 0).wait_send()

        @pl.when(has_w)
        def _():
            x_copy(c, 1).wait_send()

        return carry

    lax.fori_loop(0, CHUNKS, send_waits, 0)

    @pl.when(has_e)
    def _():
        col_copy.wait_send()
        end_col_copy.wait_recv()

    @pl.when(has_n)
    def _():
        row_copy.wait_send()
        end_row_copy.wait_recv()

    @pl.when(has_e & has_n)
    def _():
        corner_copy.wait_send()
        end_corner_copy.wait_recv()

    extra[0] = end_row_in[...]
    extra[1] = end_col_in[...]
    extra[2] = end_corner_in[...]

    @pl.when(has_s)
    def _():
        end_row_copy.wait_send()

    @pl.when(has_w)
    def _():
        end_col_copy.wait_send()

    @pl.when(has_w & has_s)
    def _():
        end_corner_copy.wait_send()


def spread_kernel(comb, extra, spread, out_hbm, ov, sem):
    lane = lax.broadcasted_iota(jnp.int32, (16, 128), 1)
    edge = jnp.where(lane == 32, roll(extra[2], 32), extra[1])
    half_edge = 0.5 * (edge + roll(edge, -1))
    for block in range(4):
        rows = []
        for j in range(block * 8, block * 8 + 8):
            here = comb[j]
            later = comb[j + 1] if j < 31 else extra[0]
            rows.append(jnp.concatenate([here, roll(edge, -j)], axis=1))
            rows.append(jnp.concatenate([0.5 * (here + later), roll(half_edge, -j)], axis=1))
        value = exact_dot(jnp.concatenate(rows, axis=0), spread[...])
        for side in range(2):
            flat = ov.at[side].reshape(LEV * APAD, 128)
            for k in range(16):
                for h in range(2):
                    begin = k * 16 + h * 8
                    flat[pl.ds(h * 8 * APAD + block * 16 + k, 8, stride=APAD), :] = value[
                        begin : begin + 8, side * 128 : side * 128 + 128
                    ]
    copies = [
        pltpu.make_async_copy(
            ov.at[side, :, pl.ds(0, 64), :], out_hbm.at[:, :, pl.ds(side * 128, 128)], sem.at[side]
        )
        for side in range(2)
    ]
    for copy in copies:
        copy.start()
    for copy in copies:
        copy.wait()


def shards(nx, ny, gradient, members):
    filters, small, spread = constants()
    w1, w2, w4 = (jnp.asarray(value) for value in filters)
    any_space = pl.BlockSpec(memory_space=pl.ANY)
    in_vmem = pl.BlockSpec(memory_space=pltpu.VMEM)
    dma = pltpu.SemaphoreType.DMA

    def vmem(*shape, dtype=F32):
        return pltpu.VMEM(shape, dtype)

    comb, extra = pl.pallas_call(
        functools.partial(main_kernel, nx, ny),
        name="localise",
        out_shape=(jax.ShapeDtypeStruct((32, 16, 128), F32), jax.ShapeDtypeStruct((3, 16, 128), F32)),
        in_specs=[any_space] * 6,
        out_specs=(in_vmem, in_vmem),
        scratch_shapes=[
            vmem(2, LEV, 64, 128),
            vmem(MEM, LEV, MPAD, 128),
            vmem(2, 256, 128, dtype=BF16),
            vmem(2, 256, 256, dtype=BF16),
            vmem(2, 256, 512, dtype=BF16),
            vmem(2, 256, 128, dtype=BF16),
            vmem(LEV, APAD, 128),
            vmem(32, 16, 128),
            vmem(CHUNKS, 48, 32, 128),
            vmem(CHUNKS, 32, 16, 128),
            vmem(CHUNKS, 24, 8, 128),
            vmem(CHUNKS, 32, 32, 128),
            vmem(CHUNKS, 16, 16, 128),
            vmem(CHUNKS, 8, 8, 128),
            vmem(2, CHUNKS, 112, 128),
            vmem(2, CHUNKS, 112, 128),
            vmem(256, 256),
            vmem(64, 512),
            vmem(8, 128),
            vmem(8, 128),
            vmem(16, 128),
            vmem(16, 128),
            vmem(16, 128),
            vmem(16, 128),
            vmem(16, 128),
            vmem(16, 128),
            vmem(16, 128),
            vmem(16, 128),
            dma((7,)),
            dma((3,)),
            dma((3,)),
            dma((2, CHUNKS, 3)),
            dma((2, CHUNKS, 3)),
            dma((2, CHUNKS)),
            dma((2, CHUNKS)),
            dma((3,)),
            dma((3,)),
        ],
        compiler_params=pltpu.CompilerParams(collective_id=0, has_side_effects=True, vmem_limit_bytes=48 << 20),
    )(gradient, members, w1, w2, w4, jnp.asarray(small))
    return pl.pallas_call(
        spread_kernel,
        name="spread",
        out_shape=jax.ShapeDtypeStruct((LEV, 64, 256), F32),
        in_specs=[in_vmem] * 3,
        out_specs=any_space,
        scratch_shapes=[vmem(2, LEV, APAD, 128), dma((2,))],
        compiler_params=pltpu.CompilerParams(vmem_limit_bytes=16 << 20),
    )(comb, extra, jnp.asarray(spread))


def solution(mesh):
    in_specs = (P(None, "gy", "gx"), P(None, None, "gy", "gx"))
    return jax.shard_map(
        functools.partial(shards, mesh.shape["gx"], mesh.shape["gy"]),
        mesh=mesh,
        in_specs=in_specs,
        out_specs=P(None, "gy", "gx"),
        check_vma=False,
    )
```

```python
import functools

import jax
import jax.numpy as jnp
import ml_dtypes
import numpy as np
from jax import lax
from jax.experimental import pallas as pl
from jax.experimental.pallas import tpu as pltpu
from jax.sharding import PartitionSpec as P

MESH = pl.DeviceIdType.MESH
F32, BF16 = jnp.float32, jnp.bfloat16
LEV, MEM = 16, 8
CHUNKS = 4
LAG = 2
MPAD = 40
APAD = 72

beta_raw = [(1.0 - (offset - 4) ** 2 / 25.0) ** 2 for offset in range(9)]
beta_taps = [value / sum(beta_raw) for value in beta_raw]
generations = ((1, 0.5), (2, 0.075), (4, 0.0125))
row_taps = [beta_taps[4 + k] / beta_taps[4] for k in range(5)]


def halves(matrix):
    hi = matrix.astype(ml_dtypes.bfloat16)
    lo = (matrix - hi.astype(np.float64)).astype(ml_dtypes.bfloat16)
    return np.stack([hi, lo])


def band(outputs):
    matrix = np.zeros((outputs + 8, outputs))
    for column in range(outputs):
        matrix[column : column + 9, column] = beta_taps
    return matrix


def column_filter(factor, weight, west_edge, east_edge):
    count = 128 // factor
    inside = np.ones(count + 8)
    if west_edge:
        inside[:4] = 0.0
    if east_edge:
        inside[-4:] = 0.0
    both = band(count + 8) @ (inside[:, None] * band(count))
    both = np.repeat(both, factor, axis=1) * (weight / (MEM - 1) * beta_taps[4] ** 2)
    result = np.zeros((256, 128 * factor))
    for part in range(factor):
        columns = slice(part * 128, part * 128 + 128)
        start = part * count
        result[start : start + count, columns] = both[8 : count + 8]
        result[128 + start : 136 + start, columns] = both[:8]
        result[136 + start : 144 + start, columns] = both[count + 8 :]
    return halves(result)


def constants():
    filters = []
    for factor, weight in generations:
        kinds = [column_filter(factor, weight, *edges) for edges in ((True, False), (False, False), (False, True))]
        filters.append(np.stack(kinds))
    pairs = np.zeros((256, 128))
    reduce_columns = np.zeros((256, 128))
    for lane in range(128):
        pairs[2 * lane : 2 * lane + 2, lane] = 1.0
        reduce_columns[2 * lane, lane] = 1.0
        reduce_columns[2 * lane + 1, lane] = 0.5
        if lane:
            reduce_columns[2 * lane - 1, lane] = 0.5
    small = np.stack([pairs, reduce_columns]).astype(ml_dtypes.bfloat16)
    spread = np.zeros((256, 256))
    for lane in range(128):
        spread[lane, 2 * lane] = 1.0
        spread[lane, 2 * lane + 1] = 0.5
        spread[lane + 1, 2 * lane + 1] = 0.5
    return filters, small, spread.astype(ml_dtypes.bfloat16)


def split(value):
    hi = value.astype(BF16)
    return hi, (value - hi.astype(F32)).astype(BF16)


def dot(a, b):
    return jnp.dot(a, b, preferred_element_type=F32)


def exact_dot(value, matrix):
    rows = value.shape[0]
    hi, lo = split(value)
    both = dot(jnp.concatenate([hi, lo], axis=0), matrix)
    return both[:rows] + both[rows:]


def full_dot(value, hi_matrix, lo_matrix):
    hi, lo = split(value)
    return dot(hi, hi_matrix) + dot(lo, hi_matrix) + dot(hi, lo_matrix)


def roll(value, shift):
    shift %= 128
    return value if shift == 0 else pltpu.roll(value, shift, 1)


def main_kernel(
    nx, ny,
    g_hbm, m_hbm, w1_hbm, w2_hbm, w4_hbm, small_hbm,
    comb, extra,
    gv, mv, w1, w2, w4, small,
    ac, cz, px, p2x, p4x, y1, y2, y4, sp, rp, o2, o4,
    col_out, col_in, row_out, row_in, corner_in,
    end_row_in, end_col_out, end_col_in, end_corner_in,
    local_sem, s1, r1, ys, yr, xs, xr, s3, r3,
):
    gx, gy = lax.axis_index("gx"), lax.axis_index("gy")
    has_w, has_e = gx > 0, gx < nx - 1
    has_s, has_n = gy > 0, gy < ny - 1

    kind = 1 - (gx == 0).astype(jnp.int32) + (gx == nx - 1).astype(jnp.int32)
    g_copies = [
        pltpu.make_async_copy(g_hbm.at[:, :, pl.ds(side * 128, 128)], gv.at[side], local_sem.at[side * 6])
        for side in range(2)
    ]
    m_copy = pltpu.make_async_copy(m_hbm, mv.at[:, :, pl.ds(0, 32), :], local_sem.at[1])
    small_copy = pltpu.make_async_copy(small_hbm, small, local_sem.at[2])
    w1_copy = pltpu.make_async_copy(w1_hbm.at[kind], w1, local_sem.at[3])
    w2_copy = pltpu.make_async_copy(w2_hbm.at[kind], w2, local_sem.at[4])
    w4_copy = pltpu.make_async_copy(w4_hbm.at[kind], w4, local_sem.at[5])
    for copy in (g_copies[1], g_copies[0], small_copy, m_copy, w1_copy, w2_copy, w4_copy):
        copy.start()

    barrier = pltpu.get_barrier_semaphore()
    around = [
        (has_w, -1, 0), (has_e, 1, 0), (has_s, 0, -1), (has_n, 0, 1),
        (has_w & has_s, -1, -1), (has_e & has_n, 1, 1),
    ]

    def at(dx, dy):
        return {"gx": gx + dx, "gy": gy + dy}

    for there, dx, dy in around:
        @pl.when(there)
        def _(dx=dx, dy=dy):
            pl.semaphore_signal(barrier, inc=1, device_id=at(dx, dy), device_id_type=MESH)

    @pl.when(jnp.logical_not(has_s))
    def _():
        px[:, pl.ds(0, 8)] = jnp.zeros((CHUNKS, 8, 32, 128), F32)
        p2x[:, pl.ds(0, 4)] = jnp.zeros((CHUNKS, 4, 16, 128), F32)
        p4x[:, pl.ds(0, 4)] = jnp.zeros((CHUNKS, 4, 8, 128), F32)
        row_in[...] = jnp.zeros((2, 16, 128), F32)

    @pl.when(jnp.logical_not(has_n))
    def _():
        px[:, pl.ds(40, 8)] = jnp.zeros((CHUNKS, 8, 32, 128), F32)
        p2x[:, pl.ds(28, 4)] = jnp.zeros((CHUNKS, 4, 16, 128), F32)
        p4x[:, pl.ds(20, 4)] = jnp.zeros((CHUNKS, 4, 8, 128), F32)
        end_row_in[...] = jnp.zeros((16, 128), F32)

    @pl.when(jnp.logical_not(has_w))
    def _():
        rp[0] = jnp.zeros((CHUNKS, 112, 128), F32)
        col_in[...] = jnp.zeros((8, 128), F32)

    @pl.when(jnp.logical_not(has_e))
    def _():
        rp[1] = jnp.zeros((CHUNKS, 112, 128), F32)
        end_col_in[...] = jnp.zeros((16, 128), F32)

    @pl.when(jnp.logical_not(has_w & has_s))
    def _():
        corner_in[...] = jnp.zeros((16, 128), F32)

    @pl.when(jnp.logical_not(has_e & has_n))
    def _():
        end_corner_in[...] = jnp.zeros((16, 128), F32)

    def remote(src, dst, send, recv, dx, dy):
        return pltpu.make_async_remote_copy(
            src_ref=src, dst_ref=dst, send_sem=send, recv_sem=recv, device_id=at(dx, dy), device_id_type=MESH
        )

    col_copy = remote(col_out, col_in, s1.at[0], r1.at[0], 1, 0)
    row_copy = remote(row_out, row_in, s1.at[1], r1.at[1], 0, 1)
    corner_copy = remote(row_out.at[1], corner_in, s1.at[2], r1.at[2], 1, 1)
    end_row_copy = remote(comb.at[0], end_row_in, s3.at[0], r3.at[0], 0, -1)
    end_col_copy = remote(end_col_out, end_col_in, s3.at[1], r3.at[1], -1, 0)
    end_corner_copy = remote(end_col_out, end_corner_in, s3.at[2], r3.at[2], -1, -1)

    def y_copies(c, direction, pieces=slice(0, 4)):
        if direction == 0:
            places = ((px, 32, 0, 8), (p2x, 16, 0, 4), (p4x, 8, 0, 4))
            dy = 1
        else:
            places = ((px, 9, 41, 7), (p2x, 12, 28, 4), (p4x, 12, 20, 4), (px, 8, 40, 1))
            dy = -1
        return [
            remote(ref.at[c, pl.ds(src, n)], ref.at[c, pl.ds(dst, n)], ys.at[direction, c, i], yr.at[direction, c, i], 0, dy)
            for i, (ref, src, dst, n) in list(enumerate(places))[pieces]
        ]

    def start_rows(c, pieces):
        @pl.when(has_n)
        def _():
            for copy in y_copies(c, 0, pieces):
                copy.start()

        @pl.when(has_s)
        def _():
            for copy in y_copies(c, 1, pieces):
                copy.start()

    def x_copy(c, direction):
        if direction == 0:
            return remote(sp.at[0, c], rp.at[0, c], xs.at[0, c], xr.at[0, c], 1, 0)
        return remote(sp.at[1, c], rp.at[1, c], xs.at[1, c], xr.at[1, c], -1, 0)

    lane = lax.broadcasted_iota(jnp.int32, (8, 128), 1)
    first_lane = lane == 0

    g_copies[1].wait()
    g0, g1 = gv.at[0].reshape(LEV * 64, 128), gv.at[1].reshape(LEV * 64, 128)
    parts = []
    for quarter in range(4):
        packed = jnp.zeros((8, 128), F32)
        for i in range(quarter * 32, quarter * 32 + 32):
            packed = jnp.where(lane == i, roll(g1[pl.ds(i * 8, 8), :], i + 1), packed)
        parts.append(packed)
    col_out[...] = jnp.where(lane < 64, jnp.where(lane < 32, parts[0], parts[1]), jnp.where(lane < 96, parts[2], parts[3]))
    pl.semaphore_wait(barrier, sum(there.astype(jnp.int32) for there, _, _ in around))

    @pl.when(has_e)
    def _():
        col_copy.start()

    g_copies[0].wait()
    for h in range(2):
        row_out[0, pl.ds(h * 8, 8), :] = g0[pl.ds(h * 8 * 64 + 63, 8, stride=64), :]
        row_out[1, pl.ds(h * 8, 8), :] = g1[pl.ds(h * 8 * 64 + 63, 8, stride=64), :]

    @pl.when(has_n)
    def _():
        row_copy.start()

    @pl.when(has_e & has_n)
    def _():
        corner_copy.start()

    small_copy.wait()
    for block in range(4):
        levels = pl.ds(block * 4, 4)
        value = jnp.concatenate([gv[0, levels].reshape(256, 128), gv[1, levels].reshape(256, 128)], axis=1)
        ac[levels, pl.ds(0, 64), :] = exact_dot(value, small[1]).reshape(4, 64, 128)
    ar = ac.reshape(LEV * APAD, 128)

    def across_row(y, h):
        return ar[pl.ds(h * 8 * APAD + y, 8, stride=APAD), :]

    @pl.when(has_w)
    def _():
        col_copy.wait_recv()
        value = 0.5 * col_in[...]
        for l in range(LEV):
            for block in range(8):
                tile = ac[l, pl.ds(block * 8, 8), :]
                ac[l, pl.ds(block * 8, 8), :] = tile + jnp.where(first_lane, roll(value, -(l * 8 + block)), 0.0)

    def reduce_rows(j, carry):
        odd_rows = []
        for h in range(2):
            odd = across_row(2 * j + 1, h)
            cz[j, pl.ds(h * 8, 8), :] = across_row(2 * j, h) + 0.5 * (odd + carry[h])
            odd_rows.append(odd)
        return tuple(odd_rows)

    lax.fori_loop(1, 32, reduce_rows, tuple(across_row(1, h) for h in range(2)))

    mr = mv.reshape(MEM * LEV * MPAD, 128)

    def member(c, m2, h, y):
        return mr[pl.ds(((2 * c + m2) * LEV + h * 8) * MPAD + y, 8, stride=MPAD), :]

    def half_blocks(c, first, count):
        rows = []
        for k in range(count):
            pair = px[c, 2 * (first + k) - 8] + px[c, 2 * (first + k) - 7]
            for m2 in range(2):
                rows.append(jnp.concatenate([pair[m2 * 16 : m2 * 16 + 8], pair[m2 * 16 + 8 : m2 * 16 + 16]], axis=1))
        value = exact_dot(jnp.concatenate(rows, axis=0), small[0])
        p2x[c, pl.ds(first, count)] = value.reshape(count, 16, 128)

    def quarter_blocks(c, first, count):
        rows = []
        for k in range(count):
            pair = p2x[c, 2 * (first + k) - 8] + p2x[c, 2 * (first + k) - 7]
            rows.append(jnp.concatenate([pair[:8], pair[8:]], axis=1))
        value = exact_dot(jnp.concatenate(rows, axis=0), small[0])
        p4x[c, pl.ds(first, count)] = value.reshape(count, 8, 128)

    m_copy.wait()

    def product_row(c, y):
        for m2 in range(2):
            for h in range(2):
                px[c, 8 + y, pl.ds(m2 * 16 + h * 8, 8), :] = member(c, m2, h, y) * cz[y, pl.ds(h * 8, 8), :]

    def product_rows(c):
        def row(y, carry):
            product_row(c, y)
            return carry

        lax.fori_loop(1, 32, row, 0, unroll=4)

    early, late = slice(0, 2), slice(2, 4)
    product_rows(0)
    half_blocks(0, 12, 8)
    start_rows(0, early)

    @pl.when(has_s)
    def _():
        row_copy.wait_recv()

    @pl.when(has_w & has_s)
    def _():
        corner_copy.wait_recv()

    before = exact_dot(jnp.concatenate([row_in[0], row_in[1]], axis=1), small[1])
    for h in range(2):
        corner = jnp.where(first_lane, 0.5 * roll(corner_in[pl.ds(h * 8, 8), :], 1), 0.0)
        earlier = before[h * 8 : h * 8 + 8] + corner
        cz[0, pl.ds(h * 8, 8), :] = across_row(0, h) + 0.5 * (across_row(1, h) + earlier)
    for c in range(CHUNKS):
        product_row(c, 0)
    half_blocks(0, 8, 4)
    half_blocks(0, 20, 4)
    quarter_blocks(0, 8, 8)
    start_rows(0, late)

    def make_products(c, carry):
        product_rows(c)
        half_blocks(c, 8, 8)
        half_blocks(c, 16, 8)
        quarter_blocks(c, 8, 8)
        start_rows(c, slice(0, 4))
        return carry

    lax.fori_loop(1, CHUNKS, make_products, 0)

    low = jnp.where(has_s, 1.0, 0.0).astype(F32)
    high = jnp.where(has_n, 1.0, 0.0).astype(F32)

    def one_pass(window):
        total = window[4]
        for k in range(1, 5):
            total = total + row_taps[k] * (window[4 - k] + window[4 + k])
        return total

    def filter_rows(c, source, target, rows, fields, width, base):
        group = width // 8
        place = (lane % width) // 8

        def column(f, carry):
            at_f = pl.ds(pl.multiple_of(f * 8, 8), 8)
            window, passed = [], []
            east = west = None
            for row in range(rows):
                window.append(source[c, row, at_f, :])
                if row < 8:
                    continue
                once = one_pass(window[-9:])
                if row - 8 < 4:
                    once = once * low
                if row >= rows - 4:
                    once = once * high
                passed.append(once)
                if len(passed) < 9:
                    continue
                twice = one_pass(passed[-9:])
                y = row - 16
                target[c, y, at_f, :] = twice
                r = y % group
                to_west, to_east = roll(twice, 8 * r), roll(twice, 8 * r + 8 - width)
                if r == 0:
                    west, east = to_west, to_east
                else:
                    west, east = jnp.where(place == r, to_west, west), jnp.where(place == r, to_east, east)
                if r == group - 1:
                    start = pl.multiple_of(base + (y // group) * fields + f * 8, 8)
                    sp[0, c, pl.ds(start, 8), :] = east
                    sp[1, c, pl.ds(start, 8), :] = west
            return carry

        lax.fori_loop(0, fields // 8, column, 0)

    def rows_stage(c):
        @pl.when(has_s)
        def _():
            for copy in y_copies(c, 0):
                copy.wait_recv()

        @pl.when(has_n)
        def _():
            for copy in y_copies(c, 1):
                copy.wait_recv()

        half_blocks(c, 4, 4)
        half_blocks(c, 24, 4)
        quarter_blocks(c, 4, 4)
        quarter_blocks(c, 16, 4)
        filter_rows(c, px, y1, 48, 32, 128, 0)
        filter_rows(c, p2x, y2, 32, 16, 64, 64)
        filter_rows(c, p4x, y4, 24, 8, 32, 96)

        @pl.when(has_e)
        def _():
            x_copy(c, 0).start()

        @pl.when(has_w)
        def _():
            x_copy(c, 1).start()

    comb[...] = jnp.zeros((32, 16, 128), F32)
    w1_copy.wait()
    w2_copy.wait()
    w4_copy.wait()

    def halo(c, start, fields, r, width):
        west, east = rp[0, c, pl.ds(start, fields), :], rp[1, c, pl.ds(start, fields), :]
        take_west = lax.broadcasted_iota(jnp.int32, (fields, 128), 1) % width < 8
        return jnp.where(take_west, roll(west, -8 * r), roll(east, 8 - 8 * r))

    def columns_stage(c):
        @pl.when(has_w)
        def _():
            x_copy(c, 0).wait_recv()

        @pl.when(has_e)
        def _():
            x_copy(c, 1).wait_recv()

        sides = [halo(c, 96 + (q // 4) * 8, 8, q % 4, 32) for q in range(8)]
        value = jnp.concatenate([y4[c].reshape(64, 128), jnp.concatenate(sides, axis=0)], axis=1)
        o4[...] = full_dot(value, w4[0], w4[1])
        sides = [halo(c, 64 + (q // 8) * 16, 16, q % 8, 64) for q in range(16)]
        value = jnp.concatenate([y2[c].reshape(256, 128), jnp.concatenate(sides, axis=0)], axis=1)
        o2[...] = full_dot(value, w2[0], w2[1])

        def block(b, carry):
            for part in range(2):
                first = b * 16 + part * 8
                start = pl.multiple_of(b * 32, 32)
                sides = [halo(c, start, 32, part * 8 + r, 128) for r in range(8)]
                rows = y1[c, pl.ds(first, 8)].reshape(256, 128)
                value = full_dot(jnp.concatenate([rows, jnp.concatenate(sides, axis=0)], axis=1), w1[0], w1[1])
                for r in range(8):
                    y = first + r
                    at2 = pl.multiple_of((b * 8 + part * 4 + r // 2) * 16, 16)
                    at4 = pl.multiple_of((b * 4 + part * 2 + r // 4) * 8, 8)
                    for h in range(2):
                        total = comb[y, pl.ds(h * 8, 8), :]
                        for m2 in range(2):
                            begin = r * 32 + m2 * 16 + h * 8
                            local = value[begin : begin + 8]
                            local = local + o2[pl.ds(at2 + m2 * 8, 8), pl.ds(h * 128, 128)]
                            local = local + o4[pl.ds(at4, 8), pl.ds((m2 * 2 + h) * 128, 128)]
                            total = total + member(c, m2, h, y) * local
                        comb[y, pl.ds(h * 8, 8), :] = total
            return carry

        lax.fori_loop(0, 2, block, 0)

    def stages(step, carry):
        @pl.when(step < CHUNKS)
        def _():
            rows_stage(step)

        @pl.when(step >= LAG)
        def _():
            columns_stage(step - LAG)

        return carry

    lax.fori_loop(0, CHUNKS + LAG, stages, 0)

    for h in range(2):
        packed = comb[0, pl.ds(h * 8, 8), :]
        for y in range(1, 32):
            packed = jnp.where(lane == y, roll(comb[y, pl.ds(h * 8, 8), :], y), packed)
        end_col_out[pl.ds(h * 8, 8), :] = packed

    @pl.when(has_s)
    def _():
        end_row_copy.start()

    @pl.when(has_w)
    def _():
        end_col_copy.start()

    @pl.when(has_w & has_s)
    def _():
        end_corner_copy.start()

    def send_waits(c, carry):
        @pl.when(has_n)
        def _():
            for copy in y_copies(c, 0):
                copy.wait_send()

        @pl.when(has_s)
        def _():
            for copy in y_copies(c, 1):
                copy.wait_send()

        @pl.when(has_e)
        def _():
            x_copy(c, 0).wait_send()

        @pl.when(has_w)
        def _():
            x_copy(c, 1).wait_send()

        return carry

    lax.fori_loop(0, CHUNKS, send_waits, 0)

    @pl.when(has_e)
    def _():
        col_copy.wait_send()
        end_col_copy.wait_recv()

    @pl.when(has_n)
    def _():
        row_copy.wait_send()
        end_row_copy.wait_recv()

    @pl.when(has_e & has_n)
    def _():
        corner_copy.wait_send()
        end_corner_copy.wait_recv()

    extra[0] = end_row_in[...]
    extra[1] = end_col_in[...]
    extra[2] = end_corner_in[...]

    @pl.when(has_s)
    def _():
        end_row_copy.wait_send()

    @pl.when(has_w)
    def _():
        end_col_copy.wait_send()

    @pl.when(has_w & has_s)
    def _():
        end_corner_copy.wait_send()


def spread_kernel(comb, extra, spread, out_hbm, ov, sem):
    lane = lax.broadcasted_iota(jnp.int32, (16, 128), 1)
    edge = jnp.where(lane == 32, roll(extra[2], 32), extra[1])
    half_edge = 0.5 * (edge + roll(edge, -1))
    for block in range(4):
        rows = []
        for j in range(block * 8, block * 8 + 8):
            here = comb[j]
            later = comb[j + 1] if j < 31 else extra[0]
            rows.append(jnp.concatenate([here, roll(edge, -j)], axis=1))
            rows.append(jnp.concatenate([0.5 * (here + later), roll(half_edge, -j)], axis=1))
        value = exact_dot(jnp.concatenate(rows, axis=0), spread[...])
        for side in range(2):
            flat = ov.at[side].reshape(LEV * APAD, 128)
            for k in range(16):
                for h in range(2):
                    begin = k * 16 + h * 8
                    flat[pl.ds(h * 8 * APAD + block * 16 + k, 8, stride=APAD), :] = value[
                        begin : begin + 8, side * 128 : side * 128 + 128
                    ]
    copies = [
        pltpu.make_async_copy(
            ov.at[side, :, pl.ds(0, 64), :], out_hbm.at[:, :, pl.ds(side * 128, 128)], sem.at[side]
        )
        for side in range(2)
    ]
    for copy in copies:
        copy.start()
    for copy in copies:
        copy.wait()


def shards(nx, ny, gradient, members):
    filters, small, spread = constants()
    w1, w2, w4 = (jnp.asarray(value) for value in filters)
    any_space = pl.BlockSpec(memory_space=pltpu.HBM)
    in_vmem = pl.BlockSpec(memory_space=pltpu.VMEM)
    dma = pltpu.SemaphoreType.DMA

    def vmem(*shape, dtype=F32):
        return pltpu.VMEM(shape, dtype)

    comb, extra = pl.pallas_call(
        functools.partial(main_kernel, nx, ny),
        name="localise",
        out_shape=(jax.ShapeDtypeStruct((32, 16, 128), F32), jax.ShapeDtypeStruct((3, 16, 128), F32)),
        in_specs=[any_space] * 6,
        out_specs=(in_vmem, in_vmem),
        scratch_shapes=[
            vmem(2, LEV, 64, 128),
            vmem(MEM, LEV, MPAD, 128),
            vmem(2, 256, 128, dtype=BF16),
            vmem(2, 256, 256, dtype=BF16),
            vmem(2, 256, 512, dtype=BF16),
            vmem(2, 256, 128, dtype=BF16),
            vmem(LEV, APAD, 128),
            vmem(32, 16, 128),
            vmem(CHUNKS, 48, 32, 128),
            vmem(CHUNKS, 32, 16, 128),
            vmem(CHUNKS, 24, 8, 128),
            vmem(CHUNKS, 32, 32, 128),
            vmem(CHUNKS, 16, 16, 128),
            vmem(CHUNKS, 8, 8, 128),
            vmem(2, CHUNKS, 112, 128),
            vmem(2, CHUNKS, 112, 128),
            vmem(256, 256),
            vmem(64, 512),
            vmem(8, 128),
            vmem(8, 128),
            vmem(2, 16, 128),
            vmem(2, 16, 128),
            vmem(16, 128),
            vmem(16, 128),
            vmem(16, 128),
            vmem(16, 128),
            vmem(16, 128),
            dma((7,)),
            dma((3,)),
            dma((3,)),
            dma((2, CHUNKS, 4)),
            dma((2, CHUNKS, 4)),
            dma((2, CHUNKS)),
            dma((2, CHUNKS)),
            dma((3,)),
            dma((3,)),
        ],
        compiler_params=pltpu.CompilerParams(collective_id=0, has_side_effects=True, vmem_limit_bytes=48 << 20),
    )(*(pltpu.with_memory_space_constraint(value, pltpu.HBM) for value in (gradient, members, w1, w2, w4, jnp.asarray(small))))
    return pl.pallas_call(
        spread_kernel,
        name="spread",
        out_shape=jax.ShapeDtypeStruct((LEV, 64, 256), F32),
        in_specs=[in_vmem] * 3,
        out_specs=any_space,
        scratch_shapes=[vmem(2, LEV, APAD, 128), dma((2,))],
        compiler_params=pltpu.CompilerParams(vmem_limit_bytes=16 << 20),
    )(comb, extra, jnp.asarray(spread))


def solution(mesh):
    in_specs = (P(None, "gy", "gx"), P(None, None, "gy", "gx"))
    return jax.shard_map(
        functools.partial(shards, mesh.shape["gx"], mesh.shape["gy"]),
        mesh=mesh,
        in_specs=in_specs,
        out_specs=P(None, "gy", "gx"),
        check_vma=False,
    )
```

```python
import functools

import jax
import jax.numpy as jnp
import ml_dtypes
import numpy as np
from jax import lax
from jax.experimental import pallas as pl
from jax.experimental.pallas import tpu as pltpu
from jax.sharding import PartitionSpec as P

MESH = pl.DeviceIdType.MESH
F32, BF16 = jnp.float32, jnp.bfloat16
LEV, MEM = 16, 8
CHUNKS = 4
LAG = 2
MPAD = 40
APAD = 72

beta_raw = [(1.0 - (offset - 4) ** 2 / 25.0) ** 2 for offset in range(9)]
beta_taps = [value / sum(beta_raw) for value in beta_raw]
generations = ((1, 0.5), (2, 0.075), (4, 0.0125))
row_taps = [beta_taps[4 + k] / beta_taps[4] for k in range(5)]


def halves(matrix):
    hi = matrix.astype(ml_dtypes.bfloat16)
    lo = (matrix - hi.astype(np.float64)).astype(ml_dtypes.bfloat16)
    return np.stack([hi, lo])


def band(outputs):
    matrix = np.zeros((outputs + 8, outputs))
    for column in range(outputs):
        matrix[column : column + 9, column] = beta_taps
    return matrix


def column_filter(factor, weight, west_edge, east_edge):
    count = 128 // factor
    inside = np.ones(count + 8)
    if west_edge:
        inside[:4] = 0.0
    if east_edge:
        inside[-4:] = 0.0
    both = band(count + 8) @ (inside[:, None] * band(count))
    both = np.repeat(both, factor, axis=1) * (weight / (MEM - 1) * beta_taps[4] ** 2)
    result = np.zeros((256, 128 * factor))
    for part in range(factor):
        columns = slice(part * 128, part * 128 + 128)
        start = part * count
        result[start : start + count, columns] = both[8 : count + 8]
        result[128 + start : 136 + start, columns] = both[:8]
        result[136 + start : 144 + start, columns] = both[count + 8 :]
    return halves(result)


def row_filter(south_edge, north_edge):
    result = np.zeros((96, 128))
    start = 0
    for factor, _ in generations:
        count = 32 // factor
        inside = np.ones(count + 8)
        if south_edge:
            inside[:4] = 0.0
        if north_edge:
            inside[-4:] = 0.0
        both = band(count + 8) @ (inside[:, None] * band(count)) / beta_taps[4] ** 2
        for row in range(96):
            block = (row - 32) // factor + 8
            if 0 <= block < count + 16:
                result[row, start : start + count] = both[block]
        start += count
    return halves(result)


def constants():
    filters = []
    for factor, weight in generations:
        kinds = [column_filter(factor, weight, *edges) for edges in ((True, False), (False, False), (False, True))]
        filters.append(np.stack(kinds))
    filters[0] = np.concatenate([filters[0][:, 0], filters[0][:, 1]], axis=2)
    pairs = np.zeros((256, 128))
    reduce_columns = np.zeros((256, 128))
    for lane in range(128):
        pairs[2 * lane : 2 * lane + 2, lane] = 1.0
        reduce_columns[2 * lane, lane] = 1.0
        reduce_columns[2 * lane + 1, lane] = 0.5
        if lane:
            reduce_columns[2 * lane - 1, lane] = 0.5
    fours = np.zeros((2, 256, 128))
    for lane in range(256):
        fours[0, lane, lane // 4] = 1.0
        fours[1, lane, 64 + lane // 4] = 1.0
    border = np.zeros((256, 128))
    for chunk in range(CHUNKS):
        for j in range(32):
            border[2 * j, chunk * 32 + j] = 0.5
            border[2 * j + 1, chunk * 32 + j] = 0.25
            if j:
                border[2 * j - 1, chunk * 32 + j] = 0.25
    small = np.stack([pairs, reduce_columns, *fours, border]).astype(ml_dtypes.bfloat16)
    rows = np.stack([row_filter(*edges) for edges in ((True, False), (False, False), (False, True))])
    spread = np.zeros((256, 256))
    for lane in range(128):
        spread[lane, 2 * lane] = 1.0
        spread[lane, 2 * lane + 1] = 0.5
        spread[lane + 1, 2 * lane + 1] = 0.5
    return filters, rows, small, spread.astype(ml_dtypes.bfloat16)


def split(value):
    hi = value.astype(BF16)
    return hi, (value - hi.astype(F32)).astype(BF16)


def dot(a, b):
    return jnp.dot(a, b, preferred_element_type=F32)


def exact_dot(value, matrix):
    rows = value.shape[0]
    hi, lo = split(value)
    both = dot(jnp.concatenate([hi, lo], axis=0), matrix)
    return both[:rows] + both[rows:]


def full_dot(value, hi_matrix, lo_matrix):
    hi, lo = split(value)
    return dot(hi, hi_matrix) + dot(lo, hi_matrix) + dot(hi, lo_matrix)


def roll(value, shift):
    shift %= 128
    return value if shift == 0 else pltpu.roll(value, shift, 1)


def main_kernel(
    nx, ny,
    g_hbm, m_hbm, w1_hbm, w2_hbm, w4_hbm, wr_hbm, small_hbm,
    comb, extra,
    gv, mv, w1, w2, w4, wr, small,
    ac, cz, px, p2x, p4x, y1, y2, y4, sp, rp, o2, o4,
    col_out, col_in, row_out, row_in, corner_in, m_out, m_in, c_out, c_in, dp, dp_in, add_rows, a1, a2, a4,
    end_row_in, end_col_out, end_col_in, end_corner_in,
    local_sem, wr_sem, s1, r1, sf, rf, ys, yr, xs, xr, s3, r3,
):
    gx, gy = lax.axis_index("gx"), lax.axis_index("gy")
    has_w, has_e = gx > 0, gx < nx - 1
    has_s, has_n = gy > 0, gy < ny - 1

    kind = 1 - (gx == 0).astype(jnp.int32) + (gx == nx - 1).astype(jnp.int32)
    g_copies = [
        pltpu.make_async_copy(
            g_hbm.at[:, :, pl.ds(side * 128, 128)], gv.at[side, :, pl.ds(0, 64), :], local_sem.at[side * 6]
        )
        for side in range(2)
    ]
    m_copy = pltpu.make_async_copy(m_hbm, mv.at[:, :, pl.ds(0, 32), :], local_sem.at[1])
    small_copy = pltpu.make_async_copy(small_hbm, small, local_sem.at[2])
    w1_copy = pltpu.make_async_copy(w1_hbm.at[kind], w1, local_sem.at[3])
    w2_copy = pltpu.make_async_copy(w2_hbm.at[kind], w2, local_sem.at[4])
    w4_copy = pltpu.make_async_copy(w4_hbm.at[kind], w4, local_sem.at[5])
    row_kind = 1 - (gy == 0).astype(jnp.int32) + (gy == ny - 1).astype(jnp.int32)
    wr_copies = [
        pltpu.make_async_copy(
            wr_hbm.at[row_kind, part, pl.ds(tile * 32, 32), :],
            wr.at[part, tile, pl.ds(c * 32, 32), pl.ds(c * 128, 128)],
            wr_sem.at[part, tile, c],
        )
        for part in range(2) for tile in range(3) for c in range(CHUNKS)
    ]
    for copy in (g_copies[1], g_copies[0], small_copy, m_copy, *wr_copies, w1_copy, w2_copy, w4_copy):
        copy.start()

    barrier = pltpu.get_barrier_semaphore()
    around = [
        (has_w, -1, 0), (has_e, 1, 0), (has_s, 0, -1), (has_n, 0, 1),
        (has_w & has_s, -1, -1), (has_e & has_n, 1, 1),
    ]

    def at(dx, dy):
        return {"gx": gx + dx, "gy": gy + dy}

    for there, dx, dy in around:
        @pl.when(there)
        def _(dx=dx, dy=dy):
            pl.semaphore_signal(barrier, inc=1, device_id=at(dx, dy), device_id_type=MESH)

    for part in range(2):
        for tile in range(3):
            for c in range(CHUNKS):
                for other in range(CHUNKS):
                    if other != c:
                        wr[part, tile, pl.ds(c * 32, 32), pl.ds(other * 128, 128)] = jnp.zeros((32, 128), BF16)

    @pl.when(jnp.logical_not(has_s))
    def _():
        px[:, pl.ds(0, 8)] = jnp.zeros((CHUNKS, 8, 32, 128), F32)
        p2x[:, pl.ds(0, 4)] = jnp.zeros((CHUNKS, 4, 16, 128), F32)
        p4x[:, pl.ds(0, 4)] = jnp.zeros((CHUNKS, 4, 8, 128), F32)
        row_in[...] = jnp.zeros((2, 16, 128), F32)
        dp_in[0] = jnp.zeros((32, 128), F32)

    @pl.when(jnp.logical_not(has_n))
    def _():
        px[:, pl.ds(40, 8)] = jnp.zeros((CHUNKS, 8, 32, 128), F32)
        p2x[:, pl.ds(28, 4)] = jnp.zeros((CHUNKS, 4, 16, 128), F32)
        p4x[:, pl.ds(20, 4)] = jnp.zeros((CHUNKS, 4, 8, 128), F32)
        end_row_in[...] = jnp.zeros((16, 128), F32)
        dp_in[1] = jnp.zeros((32, 128), F32)

    @pl.when(jnp.logical_not(has_w))
    def _():
        rp[0] = jnp.zeros((CHUNKS, 112, 128), F32)
        col_in[...] = jnp.zeros((16, 128), F32)

    @pl.when(jnp.logical_not(has_e))
    def _():
        rp[1] = jnp.zeros((CHUNKS, 112, 128), F32)
        end_col_in[...] = jnp.zeros((16, 128), F32)

    @pl.when(jnp.logical_not(has_w & has_s))
    def _():
        corner_in[...] = jnp.zeros((16, 128), F32)

    @pl.when(jnp.logical_not(has_e & has_n))
    def _():
        end_corner_in[...] = jnp.zeros((16, 128), F32)

    def remote(src, dst, send, recv, dx, dy):
        return pltpu.make_async_remote_copy(
            src_ref=src, dst_ref=dst, send_sem=send, recv_sem=recv, device_id=at(dx, dy), device_id_type=MESH
        )

    col_copy = remote(col_out, col_in, s1.at[0], r1.at[0], 1, 0)
    row_copy = remote(row_out, row_in, s1.at[1], r1.at[1], 0, 1)
    corner_copy = remote(col_out, corner_in, s1.at[2], r1.at[2], 1, 1)
    end_row_copy = remote(comb.at[0], end_row_in, s3.at[0], r3.at[0], 0, -1)
    end_col_copy = remote(end_col_out, end_col_in, s3.at[1], r3.at[1], -1, 0)
    end_corner_copy = remote(comb.at[0], end_corner_in, s3.at[2], r3.at[2], -1, -1)

    def y_copies(c, direction, pieces=slice(0, 3)):
        if direction == 0:
            places = ((px, 32, 0, 8), (p2x, 16, 0, 4), (p4x, 8, 0, 4))
            dy = 1
        else:
            places = ((px, 9, 41, 7), (p2x, 12, 28, 4), (p4x, 12, 20, 4))
            dy = -1
        return [
            remote(ref.at[c, pl.ds(src, n)], ref.at[c, pl.ds(dst, n)], ys.at[direction, c, i], yr.at[direction, c, i], 0, dy)
            for i, (ref, src, dst, n) in list(enumerate(places))[pieces]
        ]

    first_members = remote(m_out, m_in, sf.at[0], rf.at[0], 0, -1)
    dp_north = remote(dp, dp_in.at[0], sf.at[2], rf.at[2], 0, 1)
    dp_south = remote(dp, dp_in.at[1], sf.at[3], rf.at[3], 0, -1)
    first_coarse = remote(c_out, c_in, sf.at[1], rf.at[1], 0, -1)

    def x_copy(c, direction):
        if direction == 0:
            return remote(sp.at[0, c], rp.at[0, c], xs.at[0, c], xr.at[0, c], 1, 0)
        return remote(sp.at[1, c], rp.at[1, c], xs.at[1, c], xr.at[1, c], -1, 0)

    lane = lax.broadcasted_iota(jnp.int32, (8, 128), 1)
    first_lane = lane == 0

    g_copies[1].wait()
    g0, g1 = gv.at[0].reshape(LEV * APAD, 128), gv.at[1].reshape(LEV * APAD, 128)

    def gradient_row(half, y, h):
        return half[pl.ds(h * 8 * APAD + y, 8, stride=APAD), :]

    for h in range(2):
        parts = []
        for quarter in range(2):
            packed = jnp.zeros((8, 128), F32)
            for y in range(quarter * 32, quarter * 32 + 32):
                packed = jnp.where(lane == y, roll(gradient_row(g1, y, h), y + 1), packed)
            parts.append(packed)
        col_out[pl.ds(h * 8, 8), :] = jnp.where(lane < 32, parts[0], parts[1])
    g_copies[0].wait()
    for h in range(2):
        row_out[0, pl.ds(h * 8, 8), :] = gradient_row(g0, 63, h)
        row_out[1, pl.ds(h * 8, 8), :] = gradient_row(g1, 63, h)

    small_copy.wait()
    for block in range(4):
        levels = pl.ds(block * 4, 4)
        value = jnp.concatenate(
            [gv[side, levels, pl.ds(0, 64), :].reshape(256, 128) for side in range(2)], axis=1
        )
        ac[levels, pl.ds(0, 64), :] = exact_dot(value, small[1]).reshape(4, 64, 128)
    ar = ac.reshape(LEV * APAD, 128)

    def across_row(y, h):
        return ar[pl.ds(h * 8 * APAD + y, 8, stride=APAD), :]

    for h in range(2):
        c_out[pl.ds(h * 8, 8), :] = across_row(0, h) + 0.5 * across_row(1, h)

    pl.semaphore_wait(barrier, sum(there.astype(jnp.int32) for there, _, _ in around))

    @pl.when(has_e)
    def _():
        col_copy.start()

    @pl.when(has_n)
    def _():
        row_copy.start()

    @pl.when(has_e & has_n)
    def _():
        corner_copy.start()

    @pl.when(has_s)
    def _():
        first_coarse.start()

    def reduce_rows(j, carry):
        odd_rows = []
        for h in range(2):
            odd = across_row(2 * j + 1, h)
            cz[j, pl.ds(h * 8, 8), :] = across_row(2 * j, h) + 0.5 * (odd + carry[h])
            odd_rows.append(odd)
        return tuple(odd_rows)

    lax.fori_loop(1, 32, reduce_rows, tuple(across_row(1, h) for h in range(2)))
    mr = mv.reshape(MEM * LEV * MPAD, 128)

    def member(c, m2, h, y):
        return mr[pl.ds(((2 * c + m2) * LEV + h * 8) * MPAD + y, 8, stride=MPAD), :]

    m_copy.wait()

    def half_blocks(places):
        rows = []
        for c, k in places:
            pair = px[c, 2 * k - 8] + px[c, 2 * k - 7]
            for m2 in range(2):
                rows.append(jnp.concatenate([pair[m2 * 16 : m2 * 16 + 8], pair[m2 * 16 + 8 : m2 * 16 + 16]], axis=1))
        value = exact_dot(jnp.concatenate(rows, axis=0), small[0])
        for i, (c, k) in enumerate(places):
            p2x[c, k] = value[i * 16 : i * 16 + 16]

    def quarter_blocks(places):
        rows = []
        for c, k in places:
            pair = p2x[c, 2 * k - 8] + p2x[c, 2 * k - 7]
            rows.append(jnp.concatenate([pair[:8], pair[8:]], axis=1))
        value = exact_dot(jnp.concatenate(rows, axis=0), small[0])
        for i, (c, k) in enumerate(places):
            p4x[c, k] = value[i * 8 : i * 8 + 8]

    def quarter_blocks_of_rows(places):
        rows = [[], []]
        for c, k, row in places:
            four = (px[c, row] + px[c, row + 1]) + (px[c, row + 2] + px[c, row + 3])
            for m2 in range(2):
                rows[m2].append(jnp.concatenate([four[m2 * 16 : m2 * 16 + 8], four[m2 * 16 + 8 : m2 * 16 + 16]], axis=1))
        value = sum(exact_dot(jnp.concatenate(rows[m2], axis=0), small[2 + m2]) for m2 in range(2))
        for i, (c, k, _) in enumerate(places):
            p4x[c, k] = value[i * 8 : i * 8 + 8]

    def product_row(c, y):
        for m2 in range(2):
            for h in range(2):
                px[c, 8 + y, pl.ds(m2 * 16 + h * 8, 8), :] = member(c, m2, h, y) * cz[y, pl.ds(h * 8, 8), :]

    def start_rows(c, north, south):
        @pl.when(has_n)
        def _():
            for copy in y_copies(c, 0, north):
                copy.start()

        @pl.when(has_s)
        def _():
            for copy in y_copies(c, 1, south):
                copy.start()

    everything, nothing = slice(0, 3), slice(0, 0)

    def later_rows(c):
        def row(y, carry):
            product_row(c, y)
            return carry

        lax.fori_loop(1, 32, row, 0, unroll=4)

    def first_columns():
        @pl.when(has_w)
        def _():
            col_copy.wait_recv()

        coarse = exact_dot(jnp.concatenate([col_in[...], jnp.zeros((16, 128), F32)], axis=1), small[4])

        for m2 in range(2):
            for h in range(2):
                columns = []
                for c in range(CHUNKS):
                    column = roll(member(c, m2, h, 0), c * 32)
                    for y in range(1, 32):
                        place = c * 32 + y
                        column = jnp.where(lane == place, roll(member(c, m2, h, y), place), column)
                    columns.append(column)
                column = columns[0]
                for c in range(1, CHUNKS):
                    column = jnp.where(lane >= c * 32, columns[c], column)
                dp[pl.ds(m2 * 16 + h * 8, 8), :] = column * coarse[h * 8 : h * 8 + 8]

        @pl.when(has_n)
        def _():
            dp_north.start()

        @pl.when(has_s)
        def _():
            dp_south.start()

    def without_first_row(c, carry):
        later_rows(c)
        half_blocks([(c, k) for k in range(12, 24)])
        quarter_blocks([(c, k) for k in range(12, 16)])
        start_rows(c, slice(0, 2), everything)
        return carry

    def first_row(c, carry):
        product_row(c, 0)
        half_blocks([(c, k) for k in range(8, 12)])
        quarter_blocks([(c, k) for k in range(8, 12)])
        start_rows(c, slice(2, 3), nothing)
        return carry

    def whole(c, carry):
        later_rows(c)
        product_row(c, 0)
        half_blocks([(c, k) for k in range(8, 24)])
        quarter_blocks([(c, k) for k in range(8, 16)])
        start_rows(c, everything, everything)
        return carry

    def first_coarse_row():
        @pl.when(has_s)
        def _():
            row_copy.wait_recv()

        @pl.when(has_w & has_s)
        def _():
            corner_copy.wait_recv()

        before = exact_dot(jnp.concatenate([row_in[0], row_in[1]], axis=1), small[1])
        for h in range(2):
            corner = jnp.where(first_lane, 0.5 * roll(corner_in[pl.ds(h * 8, 8), :], -63), 0.0)
            cz[0, pl.ds(h * 8, 8), :] = c_out[pl.ds(h * 8, 8), :] + 0.5 * (before[h * 8 : h * 8 + 8] + corner)

    far = (gy % 8 == 0) & has_s
    without_first_row(0, 0)

    @pl.when(has_s)
    def _():
        for c in range(CHUNKS):
            for m2 in range(2):
                for h in range(2):
                    m_out[c, pl.ds(m2 * 16 + h * 8, 8), :] = member(c, m2, h, 0)
        first_members.start()

    far_west = (gx % 4 == 0) & has_w

    @pl.when(far_west)
    def _():
        without_first_row(1, 0)

    first_columns()

    @pl.when(jnp.logical_not(far_west))
    def _():
        without_first_row(1, 0)

    @pl.when(far)
    def _():
        lax.fori_loop(2, CHUNKS, without_first_row, 0)

    first_coarse_row()

    @pl.when(far)
    def _():
        lax.fori_loop(0, CHUNKS, first_row, 0)

    @pl.when(jnp.logical_not(far))
    def _():
        lax.fori_loop(0, 2, first_row, 0)
        lax.fori_loop(2, CHUNKS, whole, 0)

    @pl.when(has_n)
    def _():
        first_members.wait_recv()
        first_coarse.wait_recv()
        for h in range(2):
            corner = jnp.where(first_lane, 0.5 * roll(col_in[pl.ds(h * 8, 8), :], -63), 0.0)
            coarse = c_in[pl.ds(h * 8, 8), :] + 0.5 * (across_row(63, h) + corner)
            for c in range(CHUNKS):
                for m2 in range(2):
                    at_f = pl.ds(m2 * 16 + h * 8, 8)
                    px[c, 40, at_f, :] = m_in[c, at_f, :] * coarse

    @pl.when(has_s)
    def _():
        dp_north.wait_recv()

    @pl.when(has_n)
    def _():
        dp_south.wait_recv()

    for copy in wr_copies:
        copy.wait()
    columns = jnp.concatenate([dp_in[0], dp[...], dp_in[1]], axis=1)
    hi, lo = split(columns)
    weights = [wr[part].reshape(384, 512) for part in range(2)]
    value = dot(jnp.concatenate([hi, lo], axis=0), weights[0])
    value = value[:32] + value[32:] + dot(hi, weights[1])
    for c in range(CHUNKS):
        add_rows[c] = value[:, c * 128 : c * 128 + 128]

    def spread_additions(c):
        for target, rows, width, first in ((a1, 32, 128, 0), (a2, 16, 64, 32), (a4, 8, 32, 48)):
            parts = 128 // width
            for f in range(4 // parts):
                fields = [add_rows[c, pl.ds((f * parts + part) * 8, 8), :] for part in range(parts)]
                for y in range(rows):
                    add = jnp.zeros((8, 128), F32)
                    for part in range(parts):
                        add = jnp.where(lane == part * width, roll(fields[part], part * width - first - y), add)
                    target[c, y, pl.ds(f * 8, 8), :] = add

    low = jnp.where(has_s, 1.0, 0.0).astype(F32)
    high = jnp.where(has_n, 1.0, 0.0).astype(F32)

    def one_pass(window):
        total = window[4]
        for k in range(1, 5):
            total = total + row_taps[k] * (window[4 - k] + window[4 + k])
        return total

    def filter_rows(c, source, target, rows, fields, width, base, additions):
        group = width // 8
        place = (lane % width) // 8

        def column(f, carry):
            at_f = pl.ds(f * 8, 8)
            window, passed = [], []
            east = west = None
            for row in range(rows):
                window.append(source[c, row, at_f, :])
                if row < 8:
                    continue
                once = one_pass(window[-9:])
                if row - 8 < 4:
                    once = once * low
                if row >= rows - 4:
                    once = once * high
                passed.append(once)
                if len(passed) < 9:
                    continue
                twice = one_pass(passed[-9:])
                y = row - 16
                twice = twice + additions[c, y, at_f, :]
                target[c, y, at_f, :] = twice
                r = y % group
                to_west, to_east = roll(twice, 8 * r), roll(twice, 8 * r + 8 - width)
                if r == 0:
                    west, east = to_west, to_east
                else:
                    west, east = jnp.where(place == r, to_west, west), jnp.where(place == r, to_east, east)
                if r == group - 1:
                    start = base + (y // group) * fields + f * 8
                    sp[0, c, pl.ds(start, 8), :] = east
                    sp[1, c, pl.ds(start, 8), :] = west
            return carry

        for f in range(fields // 8):
            column(f, 0)

    def rows_stage(c):
        spread_additions(c)

        @pl.when(has_s)
        def _():
            for copy in y_copies(c, 0):
                copy.wait_recv()

        @pl.when(has_n)
        def _():
            for copy in y_copies(c, 1):
                copy.wait_recv()

        quarter_blocks_of_rows([(c, 6, 0), (c, 7, 4), (c, 16, 40), (c, 17, 44)])
        half_blocks([(c, k) for k in (4, 5, 6, 7, 24, 25, 26, 27)])
        quarter_blocks([(c, k) for k in (4, 5, 18, 19)])
        filter_rows(c, px, y1, 48, 32, 128, 0, a1)
        filter_rows(c, p2x, y2, 32, 16, 64, 64, a2)
        filter_rows(c, p4x, y4, 24, 8, 32, 96, a4)

        @pl.when(has_e)
        def _():
            x_copy(c, 0).start()

        @pl.when(has_w)
        def _():
            x_copy(c, 1).start()

    comb[...] = jnp.zeros((32, 16, 128), F32)
    w1_copy.wait()
    w2_copy.wait()
    w4_copy.wait()

    def halo(c, start, fields, r, width):
        west, east = rp[0, c, pl.ds(start, fields), :], rp[1, c, pl.ds(start, fields), :]
        take_west = lax.broadcasted_iota(jnp.int32, (fields, 128), 1) % width < 8
        return jnp.where(take_west, roll(west, -8 * r), roll(east, 8 - 8 * r))

    def columns_stage(c):
        @pl.when(has_w)
        def _():
            x_copy(c, 0).wait_recv()

        @pl.when(has_e)
        def _():
            x_copy(c, 1).wait_recv()

        sides = [halo(c, 96 + (q // 4) * 8, 8, q % 4, 32) for q in range(8)]
        value = jnp.concatenate([y4[c].reshape(64, 128), jnp.concatenate(sides, axis=0)], axis=1)
        o4[...] = full_dot(value, w4[0], w4[1])
        sides = [halo(c, 64 + (q // 8) * 16, 16, q % 8, 64) for q in range(16)]
        value = jnp.concatenate([y2[c].reshape(256, 128), jnp.concatenate(sides, axis=0)], axis=1)
        o2[...] = full_dot(value, w2[0], w2[1])

        def block(b, carry):
            @pl.when((b == 1) & (c == CHUNKS - 1) & has_s)
            def _():
                end_row_copy.start()

            @pl.when((b == 1) & (c == CHUNKS - 1) & has_w & has_s)
            def _():
                end_corner_copy.start()

            for part in range(2):
                first = b * 16 + part * 8
                start = pl.multiple_of(b * 32, 32)
                sides = [halo(c, start, 32, part * 8 + r, 128) for r in range(8)]
                rows = y1[c, pl.ds(first, 8)].reshape(256, 128)
                both = exact_dot(jnp.concatenate([rows, jnp.concatenate(sides, axis=0)], axis=1), w1[...])
                value = both[:, :128] + both[:, 128:]
                for r in range(8):
                    y = first + r
                    at2 = pl.multiple_of((b * 8 + part * 4 + r // 2) * 16, 16)
                    at4 = pl.multiple_of((b * 4 + part * 2 + r // 4) * 8, 8)
                    for h in range(2):
                        total = comb[y, pl.ds(h * 8, 8), :]
                        for m2 in range(2):
                            begin = r * 32 + m2 * 16 + h * 8
                            local = value[begin : begin + 8]
                            local = local + o2[pl.ds(at2 + m2 * 8, 8), pl.ds(h * 128, 128)]
                            local = local + o4[pl.ds(at4, 8), pl.ds((m2 * 2 + h) * 128, 128)]
                            total = total + member(c, m2, h, y) * local
                        comb[y, pl.ds(h * 8, 8), :] = total
            return carry

        lax.fori_loop(0, 2, block, 0)

    def stages(step, carry):
        @pl.when(step < CHUNKS)
        def _():
            rows_stage(step)

        @pl.when(step >= LAG)
        def _():
            columns_stage(step - LAG)

        return carry

    lax.fori_loop(0, CHUNKS + LAG, stages, 0)

    for h in range(2):
        packed = comb[0, pl.ds(h * 8, 8), :]
        for y in range(1, 32):
            packed = jnp.where(lane == y, roll(comb[y, pl.ds(h * 8, 8), :], y), packed)
        end_col_out[pl.ds(h * 8, 8), :] = packed

    @pl.when(has_w)
    def _():
        end_col_copy.start()

    def send_waits(c, carry):
        @pl.when(has_n)
        def _():
            for copy in y_copies(c, 0):
                copy.wait_send()

        @pl.when(has_s)
        def _():
            for copy in y_copies(c, 1):
                copy.wait_send()

        @pl.when(has_e)
        def _():
            x_copy(c, 0).wait_send()

        @pl.when(has_w)
        def _():
            x_copy(c, 1).wait_send()

        return carry

    lax.fori_loop(0, CHUNKS, send_waits, 0)

    @pl.when(has_e)
    def _():
        col_copy.wait_send()
        end_col_copy.wait_recv()

    @pl.when(has_n)
    def _():
        row_copy.wait_send()
        dp_north.wait_send()
        end_row_copy.wait_recv()

    @pl.when(has_e & has_n)
    def _():
        corner_copy.wait_send()
        end_corner_copy.wait_recv()

    extra[0] = end_row_in[...]
    extra[1] = end_col_in[...]
    extra[2] = end_corner_in[...]

    @pl.when(has_s)
    def _():
        end_row_copy.wait_send()
        first_members.wait_send()
        first_coarse.wait_send()
        dp_south.wait_send()

    @pl.when(has_w)
    def _():
        end_col_copy.wait_send()

    @pl.when(has_w & has_s)
    def _():
        end_corner_copy.wait_send()


def spread_kernel(comb, extra, spread, out_hbm, ov, sem):
    lane = lax.broadcasted_iota(jnp.int32, (16, 128), 1)
    edge = jnp.where(lane == 32, roll(extra[2], 32), extra[1])
    half_edge = 0.5 * (edge + roll(edge, -1))
    copies = []
    for block in range(4):
        rows = []
        for j in range(block * 8, block * 8 + 8):
            here = comb[j]
            later = comb[j + 1] if j < 31 else extra[0]
            rows.append(jnp.concatenate([here, roll(edge, -j)], axis=1))
            rows.append(jnp.concatenate([0.5 * (here + later), roll(half_edge, -j)], axis=1))
        value = exact_dot(jnp.concatenate(rows, axis=0), spread[...])
        for side in range(2):
            flat = ov.at[side].reshape(LEV * APAD, 128)
            for k in range(16):
                for h in range(2):
                    begin = k * 16 + h * 8
                    flat[pl.ds(h * 8 * APAD + block * 16 + k, 8, stride=APAD), :] = value[
                        begin : begin + 8, side * 128 : side * 128 + 128
                    ]
    for side in range(2):
        copy = pltpu.make_async_copy(
            ov.at[side, :, pl.ds(0, 64), :], out_hbm.at[:, :, pl.ds(side * 128, 128)], sem.at[side, 0]
        )
        copy.start()
        copies.append(copy)
    for copy in copies:
        copy.wait()


def shards(nx, ny, gradient, members):
    filters, rows, small, spread = constants()
    w1, w2, w4 = (jnp.asarray(value) for value in filters)
    any_space = pl.BlockSpec(memory_space=pltpu.HBM)
    in_vmem = pl.BlockSpec(memory_space=pltpu.VMEM)
    dma = pltpu.SemaphoreType.DMA

    def vmem(*shape, dtype=F32):
        return pltpu.VMEM(shape, dtype)

    comb, extra = pl.pallas_call(
        functools.partial(main_kernel, nx, ny),
        name="localise",
        out_shape=(jax.ShapeDtypeStruct((32, 16, 128), F32), jax.ShapeDtypeStruct((3, 16, 128), F32)),
        in_specs=[any_space] * 7,
        out_specs=(in_vmem, in_vmem),
        scratch_shapes=[
            vmem(2, LEV, APAD, 128),
            vmem(MEM, LEV, MPAD, 128),
            vmem(256, 256, dtype=BF16),
            vmem(2, 256, 256, dtype=BF16),
            vmem(2, 256, 512, dtype=BF16),
            vmem(2, 3, 128, 512, dtype=BF16),
            vmem(5, 256, 128, dtype=BF16),
            vmem(LEV, APAD, 128),
            vmem(32, 16, 128),
            vmem(CHUNKS, 48, 32, 128),
            vmem(CHUNKS, 32, 16, 128),
            vmem(CHUNKS, 24, 8, 128),
            vmem(CHUNKS, 32, 32, 128),
            vmem(CHUNKS, 16, 16, 128),
            vmem(CHUNKS, 8, 8, 128),
            vmem(2, CHUNKS, 112, 128),
            vmem(2, CHUNKS, 112, 128),
            vmem(256, 256),
            vmem(64, 512),
            vmem(16, 128),
            vmem(16, 128),
            vmem(2, 16, 128),
            vmem(2, 16, 128),
            vmem(16, 128),
            vmem(CHUNKS, 32, 128),
            vmem(CHUNKS, 32, 128),
            vmem(16, 128),
            vmem(16, 128),
            vmem(32, 128),
            vmem(2, 32, 128),
            vmem(CHUNKS, 32, 128),
            vmem(CHUNKS, 32, 32, 128),
            vmem(CHUNKS, 16, 16, 128),
            vmem(CHUNKS, 8, 8, 128),
            vmem(16, 128),
            vmem(16, 128),
            vmem(16, 128),
            vmem(16, 128),
            dma((7,)),
            dma((2, 3, CHUNKS)),
            dma((3,)),
            dma((3,)),
            dma((4,)),
            dma((4,)),
            dma((2, CHUNKS, 3)),
            dma((2, CHUNKS, 3)),
            dma((2, CHUNKS)),
            dma((2, CHUNKS)),
            dma((3,)),
            dma((3,)),
        ],
        compiler_params=pltpu.CompilerParams(collective_id=0, has_side_effects=True, vmem_limit_bytes=48 << 20),
    )(*(pltpu.with_memory_space_constraint(value, pltpu.HBM) for value in (gradient, members, w1, w2, w4, jnp.asarray(rows), jnp.asarray(small))))
    return pl.pallas_call(
        spread_kernel,
        name="spread",
        out_shape=jax.ShapeDtypeStruct((LEV, 64, 256), F32),
        in_specs=[in_vmem] * 3,
        out_specs=any_space,
        scratch_shapes=[vmem(2, LEV, APAD, 128), dma((2, 4))],
        compiler_params=pltpu.CompilerParams(vmem_limit_bytes=16 << 20),
    )(comb, extra, jnp.asarray(spread))


def solution(mesh):
    in_specs = (P(None, "gy", "gx"), P(None, None, "gy", "gx"))
    return jax.shard_map(
        functools.partial(shards, mesh.shape["gx"], mesh.shape["gy"]),
        mesh=mesh,
        in_specs=in_specs,
        out_specs=P(None, "gy", "gx"),
        check_vma=False,
    )
```

```python
import functools

import jax
import jax.numpy as jnp
import ml_dtypes
import numpy as np
from jax import lax
from jax.experimental import pallas as pl
from jax.experimental.pallas import tpu as pltpu
from jax.sharding import PartitionSpec as P

MESH = pl.DeviceIdType.MESH
F32, BF16 = jnp.float32, jnp.bfloat16
LEV, MEM = 16, 8
CHUNKS = 4
LAG = 3
DEFER = 2
MPAD = 40
APAD = 72

beta_raw = [(1.0 - (offset - 4) ** 2 / 25.0) ** 2 for offset in range(9)]
beta_taps = [value / sum(beta_raw) for value in beta_raw]
generations = ((1, 0.5), (2, 0.075), (4, 0.0125))
row_taps = [beta_taps[4 + k] / beta_taps[4] for k in range(5)]


def halves(matrix):
    hi = matrix.astype(ml_dtypes.bfloat16)
    lo = (matrix - hi.astype(np.float64)).astype(ml_dtypes.bfloat16)
    return np.stack([hi, lo])


def band(outputs):
    matrix = np.zeros((outputs + 8, outputs))
    for column in range(outputs):
        matrix[column : column + 9, column] = beta_taps
    return matrix


def column_filter(factor, weight, west_edge, east_edge):
    count = 128 // factor
    inside = np.ones(count + 8)
    if west_edge:
        inside[:4] = 0.0
    if east_edge:
        inside[-4:] = 0.0
    both = band(count + 8) @ (inside[:, None] * band(count))
    both = np.repeat(both, factor, axis=1) * (weight / (MEM - 1) * beta_taps[4] ** 2)
    result = np.zeros((256, 128 * factor))
    for part in range(factor):
        columns = slice(part * 128, part * 128 + 128)
        start = part * count
        result[start : start + count, columns] = both[8 : count + 8]
        result[128 + start : 136 + start, columns] = both[:8]
        result[136 + start : 144 + start, columns] = both[count + 8 :]
    return halves(result)


def row_filter(south_edge, north_edge):
    result = np.zeros((96, 128))
    start = 0
    for factor, _ in generations:
        count = 32 // factor
        inside = np.ones(count + 8)
        if south_edge:
            inside[:4] = 0.0
        if north_edge:
            inside[-4:] = 0.0
        both = band(count + 8) @ (inside[:, None] * band(count)) / beta_taps[4] ** 2
        for row in range(96):
            block = (row - 32) // factor + 8
            if 0 <= block < count + 16:
                result[row, start : start + count] = both[block]
        start += count
    return halves(result)


def constants():
    filters = []
    for factor, weight in generations:
        kinds = [column_filter(factor, weight, *edges) for edges in ((True, False), (False, False), (False, True))]
        filters.append(np.stack(kinds))
    filters[0] = np.concatenate([filters[0][:, 0], filters[0][:, 1]], axis=2)
    pairs = np.zeros((256, 128))
    reduce_columns = np.zeros((256, 128))
    for lane in range(128):
        pairs[2 * lane : 2 * lane + 2, lane] = 1.0
        reduce_columns[2 * lane, lane] = 1.0
        reduce_columns[2 * lane + 1, lane] = 0.5
        if lane:
            reduce_columns[2 * lane - 1, lane] = 0.5
    fours = np.zeros((2, 256, 128))
    for lane in range(256):
        fours[0, lane, lane // 4] = 1.0
        fours[1, lane, 64 + lane // 4] = 1.0
    border = np.zeros((256, 128))
    for chunk in range(CHUNKS):
        for j in range(32):
            border[2 * j, chunk * 32 + j] = 0.5
            border[2 * j + 1, chunk * 32 + j] = 0.25
            if j:
                border[2 * j - 1, chunk * 32 + j] = 0.25
    small = np.stack([pairs, reduce_columns, *fours, border]).astype(ml_dtypes.bfloat16)
    rows = np.stack([row_filter(*edges) for edges in ((True, False), (False, False), (False, True))])
    spread = np.zeros((256, 256))
    for lane in range(128):
        spread[lane, 2 * lane] = 1.0
        spread[lane, 2 * lane + 1] = 0.5
        spread[lane + 1, 2 * lane + 1] = 0.5
    return filters, rows, small, spread.astype(ml_dtypes.bfloat16)


def split(value):
    hi = value.astype(BF16)
    return hi, (value - hi.astype(F32)).astype(BF16)


def dot(a, b):
    return jnp.dot(a, b, preferred_element_type=F32)


def exact_dot(value, matrix):
    rows = value.shape[0]
    hi, lo = split(value)
    both = dot(jnp.concatenate([hi, lo], axis=0), matrix)
    return both[:rows] + both[rows:]


def full_dot(value, hi_matrix, lo_matrix):
    hi, lo = split(value)
    return dot(hi, hi_matrix) + dot(lo, hi_matrix) + dot(hi, lo_matrix)


def roll(value, shift):
    shift %= 128
    return value if shift == 0 else pltpu.roll(value, shift, 1)


def main_kernel(
    nx, ny,
    g_hbm, m_hbm, w1_hbm, w2_hbm, w4_hbm, wr_hbm, small_hbm, spread_hbm,
    out,
    gv, mv, w1, w2, w4, wr, small, spread, comb,
    ac, cz, px, p2x, p4x, y1, y2, y4, sp, rp, o2, o4,
    col_out, col_in, row_out, row_in, corner_in, m_out, m_in, c_out, c_in, c_next, dp, dp_in, add_rows, a1, a2, a4,
    end_row_in, end_col_out, end_col_in, end_corner_in,
    local_sem, wr_sem, s1, r1, sf, rf, ys, yr, xs, xr, s3, r3,
):
    gx, gy = lax.axis_index("gx"), lax.axis_index("gy")
    has_w, has_e = gx > 0, gx < nx - 1
    has_s, has_n = gy > 0, gy < ny - 1

    kind = 1 - (gx == 0).astype(jnp.int32) + (gx == nx - 1).astype(jnp.int32)
    g_copies = [
        pltpu.make_async_copy(
            g_hbm.at[:, :, pl.ds(side * 128, 128)], gv.at[side, :, pl.ds(0, 64), :], local_sem.at[side * 6]
        )
        for side in range(2)
    ]
    m_copy = pltpu.make_async_copy(m_hbm, mv.at[:, :, pl.ds(0, 32), :], local_sem.at[1])
    small_copy = pltpu.make_async_copy(small_hbm, small, local_sem.at[2])
    w1_copy = pltpu.make_async_copy(w1_hbm.at[kind], w1, local_sem.at[3])
    w2_copy = pltpu.make_async_copy(w2_hbm.at[kind], w2, local_sem.at[4])
    w4_copy = pltpu.make_async_copy(w4_hbm.at[kind], w4, local_sem.at[5])
    spread_copy = pltpu.make_async_copy(spread_hbm, spread, local_sem.at[7])
    row_kind = 1 - (gy == 0).astype(jnp.int32) + (gy == ny - 1).astype(jnp.int32)
    wr_copies = [
        pltpu.make_async_copy(
            wr_hbm.at[row_kind, part, pl.ds(tile * 32, 32), :],
            wr.at[part, tile, pl.ds(c * 32, 32), pl.ds(c * 128, 128)],
            wr_sem.at[part, tile, c],
        )
        for part in range(2) for tile in range(3) for c in range(CHUNKS)
    ]
    for copy in (g_copies[1], g_copies[0], small_copy, m_copy, *wr_copies, w1_copy, w2_copy, w4_copy, spread_copy):
        copy.start()

    barrier = pltpu.get_barrier_semaphore()
    around = [
        (has_w, -1, 0), (has_e, 1, 0), (has_s, 0, -1), (has_n, 0, 1),
        (has_w & has_s, -1, -1), (has_e & has_n, 1, 1),
    ]

    def at(dx, dy):
        return {"gx": gx + dx, "gy": gy + dy}

    for there, dx, dy in around:
        @pl.when(there)
        def _(dx=dx, dy=dy):
            pl.semaphore_signal(barrier, inc=1, device_id=at(dx, dy), device_id_type=MESH)

    for part in range(2):
        for tile in range(3):
            for c in range(CHUNKS):
                for other in range(CHUNKS):
                    if other != c:
                        wr[part, tile, pl.ds(c * 32, 32), pl.ds(other * 128, 128)] = jnp.zeros((32, 128), BF16)

    @pl.when(jnp.logical_not(has_s))
    def _():
        px[:, pl.ds(0, 8)] = jnp.zeros((CHUNKS, 8, 32, 128), F32)
        p2x[:, pl.ds(0, 4)] = jnp.zeros((CHUNKS, 4, 16, 128), F32)
        p4x[:, pl.ds(0, 4)] = jnp.zeros((CHUNKS, 4, 8, 128), F32)
        row_in[...] = jnp.zeros((2, 16, 128), F32)
        dp_in[0] = jnp.zeros((32, 128), F32)

    @pl.when(jnp.logical_not(has_n))
    def _():
        px[:, pl.ds(40, 8)] = jnp.zeros((CHUNKS, 8, 32, 128), F32)
        p2x[:, pl.ds(28, 4)] = jnp.zeros((CHUNKS, 4, 16, 128), F32)
        p4x[:, pl.ds(20, 4)] = jnp.zeros((CHUNKS, 4, 8, 128), F32)
        end_row_in[...] = jnp.zeros((16, 128), F32)
        dp_in[1] = jnp.zeros((32, 128), F32)

    @pl.when(jnp.logical_not(has_w))
    def _():
        rp[0] = jnp.zeros((CHUNKS, 112, 128), F32)
        col_in[...] = jnp.zeros((16, 128), F32)

    @pl.when(jnp.logical_not(has_e))
    def _():
        rp[1] = jnp.zeros((CHUNKS, 112, 128), F32)
        end_col_in[...] = jnp.zeros((16, 128), F32)

    @pl.when(jnp.logical_not(has_w & has_s))
    def _():
        corner_in[...] = jnp.zeros((16, 128), F32)

    @pl.when(jnp.logical_not(has_e & has_n))
    def _():
        end_corner_in[...] = jnp.zeros((16, 128), F32)

    def remote(src, dst, send, recv, dx, dy):
        return pltpu.make_async_remote_copy(
            src_ref=src, dst_ref=dst, send_sem=send, recv_sem=recv, device_id=at(dx, dy), device_id_type=MESH
        )

    col_copy = remote(col_out, col_in, s1.at[0], r1.at[0], 1, 0)
    row_copy = remote(row_out, row_in, s1.at[1], r1.at[1], 0, 1)
    corner_copy = remote(col_out, corner_in, s1.at[2], r1.at[2], 1, 1)
    end_row_copy = remote(comb.at[0], end_row_in, s3.at[0], r3.at[0], 0, -1)
    end_col_copy = remote(end_col_out, end_col_in, s3.at[1], r3.at[1], -1, 0)
    end_corner_copy = remote(comb.at[0], end_corner_in, s3.at[2], r3.at[2], -1, -1)

    def y_copies(c, direction, pieces=slice(0, 4)):
        if direction == 0:
            places = ((px, 32, 0, 8), (p2x, 16, 0, 4), (p4x, 8, 0, 4))
            dy = 1
        else:
            places = ((px, 9, 41, 7), (p2x, 12, 28, 4), (p4x, 12, 20, 4))
            dy = -1
        ends = [(ref.at[c, pl.ds(src, n)], ref.at[c, pl.ds(dst, n)]) for ref, src, dst, n in places]
        if direction == 1:
            ends.append((m_out.at[c], m_in.at[c]))
        return [
            remote(src, dst, ys.at[direction, c, i], yr.at[direction, c, i], 0, dy)
            for i, (src, dst) in list(enumerate(ends))[pieces]
        ]

    dp_north = remote(dp, dp_in.at[0], sf.at[2], rf.at[2], 0, 1)
    dp_south = remote(dp, dp_in.at[1], sf.at[3], rf.at[3], 0, -1)
    first_coarse = remote(c_out, c_in, sf.at[1], rf.at[1], 0, -1)

    def x_copy(c, direction):
        if direction == 0:
            return remote(sp.at[0, c], rp.at[0, c], xs.at[0, c], xr.at[0, c], 1, 0)
        return remote(sp.at[1, c], rp.at[1, c], xs.at[1, c], xr.at[1, c], -1, 0)

    lane = lax.broadcasted_iota(jnp.int32, (8, 128), 1)
    first_lane = lane == 0

    g_copies[1].wait()
    g0, g1 = gv.at[0].reshape(LEV * APAD, 128), gv.at[1].reshape(LEV * APAD, 128)

    def gradient_row(half, y, h):
        return half[pl.ds(h * 8 * APAD + y, 8, stride=APAD), :]

    for h in range(2):
        parts = []
        for quarter in range(2):
            packed = jnp.zeros((8, 128), F32)
            for y in range(quarter * 32, quarter * 32 + 32):
                packed = jnp.where(lane == y, roll(gradient_row(g1, y, h), y + 1), packed)
            parts.append(packed)
        col_out[pl.ds(h * 8, 8), :] = jnp.where(lane < 32, parts[0], parts[1])
    g_copies[0].wait()
    for h in range(2):
        row_out[0, pl.ds(h * 8, 8), :] = gradient_row(g0, 63, h)
        row_out[1, pl.ds(h * 8, 8), :] = gradient_row(g1, 63, h)

    small_copy.wait()
    for block in range(4):
        levels = pl.ds(block * 4, 4)
        value = jnp.concatenate(
            [gv[side, levels, pl.ds(0, 64), :].reshape(256, 128) for side in range(2)], axis=1
        )
        ac[levels, pl.ds(0, 64), :] = exact_dot(value, small[1]).reshape(4, 64, 128)
    ar = ac.reshape(LEV * APAD, 128)

    def across_row(y, h):
        return ar[pl.ds(h * 8 * APAD + y, 8, stride=APAD), :]

    for h in range(2):
        c_out[pl.ds(h * 8, 8), :] = across_row(0, h) + 0.5 * across_row(1, h)

    def reduce_rows(j, carry):
        odd_rows = []
        for h in range(2):
            odd = across_row(2 * j + 1, h)
            cz[j, pl.ds(h * 8, 8), :] = across_row(2 * j, h) + 0.5 * (odd + carry[h])
            odd_rows.append(odd)
        return tuple(odd_rows)

    lax.fori_loop(1, 32, reduce_rows, tuple(across_row(1, h) for h in range(2)))
    mr = mv.reshape(MEM * LEV * MPAD, 128)

    def member(c, m2, h, y):
        return mr[pl.ds(((2 * c + m2) * LEV + h * 8) * MPAD + y, 8, stride=MPAD), :]

    m_copy.wait()

    for c in range(CHUNKS):
        for m2 in range(2):
            for h in range(2):
                m_out[c, pl.ds(m2 * 16 + h * 8, 8), :] = member(c, m2, h, 0)

    def half_blocks(places):
        rows = []
        for c, k in places:
            pair = px[c, 2 * k - 8] + px[c, 2 * k - 7]
            for m2 in range(2):
                rows.append(jnp.concatenate([pair[m2 * 16 : m2 * 16 + 8], pair[m2 * 16 + 8 : m2 * 16 + 16]], axis=1))
        value = exact_dot(jnp.concatenate(rows, axis=0), small[0])
        for i, (c, k) in enumerate(places):
            p2x[c, k] = value[i * 16 : i * 16 + 16]

    def quarter_blocks(places):
        rows = []
        for c, k in places:
            pair = p2x[c, 2 * k - 8] + p2x[c, 2 * k - 7]
            rows.append(jnp.concatenate([pair[:8], pair[8:]], axis=1))
        value = exact_dot(jnp.concatenate(rows, axis=0), small[0])
        for i, (c, k) in enumerate(places):
            p4x[c, k] = value[i * 8 : i * 8 + 8]

    def quarter_blocks_of_rows(places):
        rows = [[], []]
        for c, k, row in places:
            four = (px[c, row] + px[c, row + 1]) + (px[c, row + 2] + px[c, row + 3])
            for m2 in range(2):
                rows[m2].append(jnp.concatenate([four[m2 * 16 : m2 * 16 + 8], four[m2 * 16 + 8 : m2 * 16 + 16]], axis=1))
        value = sum(exact_dot(jnp.concatenate(rows[m2], axis=0), small[2 + m2]) for m2 in range(2))
        for i, (c, k, _) in enumerate(places):
            p4x[c, k] = value[i * 8 : i * 8 + 8]

    def product_row(c, y):
        for m2 in range(2):
            for h in range(2):
                px[c, 8 + y, pl.ds(m2 * 16 + h * 8, 8), :] = member(c, m2, h, y) * cz[y, pl.ds(h * 8, 8), :]

    def start_rows(c, north, south):
        @pl.when(has_n)
        def _():
            for copy in y_copies(c, 0, north):
                copy.start()

        @pl.when(has_s)
        def _():
            for copy in y_copies(c, 1, south):
                copy.start()

    everything, nothing = slice(0, 4), slice(0, 0)

    def later_rows(c):
        def row(y, carry):
            product_row(c, y)
            return carry

        lax.fori_loop(1, 32, row, 0, unroll=4)

    def first_columns():
        @pl.when(has_w)
        def _():
            col_copy.wait_recv()

        coarse = exact_dot(jnp.concatenate([col_in[...], jnp.zeros((16, 128), F32)], axis=1), small[4])

        for m2 in range(2):
            for h in range(2):
                columns = []
                for c in range(CHUNKS):
                    column = roll(member(c, m2, h, 0), c * 32)
                    for y in range(1, 32):
                        place = c * 32 + y
                        column = jnp.where(lane == place, roll(member(c, m2, h, y), place), column)
                    columns.append(column)
                column = columns[0]
                for c in range(1, CHUNKS):
                    column = jnp.where(lane >= c * 32, columns[c], column)
                dp[pl.ds(m2 * 16 + h * 8, 8), :] = column * coarse[h * 8 : h * 8 + 8]

        @pl.when(has_n)
        def _():
            dp_north.start()

        @pl.when(has_s)
        def _():
            dp_south.start()

    def own_rows(c):
        later_rows(c)
        half_blocks([(c, k) for k in range(12, 24)])
        quarter_blocks([(c, k) for k in range(12, 16)])

    def without_first_row(c, carry):
        own_rows(c)
        start_rows(c, slice(0, 2), everything)
        return carry

    def first_row(c, carry):
        product_row(c, 0)
        half_blocks([(c, k) for k in range(8, 12)])
        quarter_blocks([(c, k) for k in range(8, 12)])
        start_rows(c, slice(2, 3), nothing)
        return carry

    def whole(c, carry):
        later_rows(c)
        product_row(c, 0)
        half_blocks([(c, k) for k in range(8, 24)])
        quarter_blocks([(c, k) for k in range(8, 16)])
        start_rows(c, everything, everything)
        return carry

    def first_coarse_row():
        @pl.when(has_s)
        def _():
            row_copy.wait_recv()

        @pl.when(has_w & has_s)
        def _():
            corner_copy.wait_recv()

        before = exact_dot(jnp.concatenate([row_in[0], row_in[1]], axis=1), small[1])
        for h in range(2):
            corner = jnp.where(first_lane, 0.5 * roll(corner_in[pl.ds(h * 8, 8), :], -63), 0.0)
            cz[0, pl.ds(h * 8, 8), :] = c_out[pl.ds(h * 8, 8), :] + 0.5 * (before[h * 8 : h * 8 + 8] + corner)

    far = (gy % 8 == 0) & has_s
    own_rows(0)
    pl.semaphore_wait(barrier, sum(there.astype(jnp.int32) for there, _, _ in around))

    @pl.when(has_e)
    def _():
        col_copy.start()

    @pl.when(has_n)
    def _():
        row_copy.start()

    @pl.when(has_e & has_n)
    def _():
        corner_copy.start()

    @pl.when(has_s)
    def _():
        first_coarse.start()

    start_rows(0, slice(0, 2), everything)

    far_west = (gx % 4 == 0) & has_w
    near_south = gy % 2 == 1
    second = 1 + far_west.astype(jnp.int32)

    @pl.when(far_west)
    def _():
        without_first_row(1, 0)

    @pl.when(near_south)
    def _():
        first_coarse_row()
        first_row(0, 0)

    first_columns()

    @pl.when(far)
    def _():
        lax.fori_loop(second, CHUNKS, without_first_row, 0)

    @pl.when(jnp.logical_not(near_south))
    def _():
        first_coarse_row()
        first_row(0, 0)

    @pl.when(far)
    def _():
        lax.fori_loop(1, CHUNKS, first_row, 0)

    @pl.when(jnp.logical_not(far) & far_west)
    def _():
        first_row(1, 0)

    @pl.when(jnp.logical_not(far))
    def _():
        lax.fori_loop(second, CHUNKS, whole, 0)

    @pl.when(has_n)
    def _():
        first_coarse.wait_recv()
        for h in range(2):
            corner = jnp.where(first_lane, 0.5 * roll(col_in[pl.ds(h * 8, 8), :], -63), 0.0)
            c_next[pl.ds(h * 8, 8), :] = c_in[pl.ds(h * 8, 8), :] + 0.5 * (across_row(63, h) + corner)

    @pl.when(has_s)
    def _():
        dp_north.wait_recv()

    @pl.when(has_n)
    def _():
        dp_south.wait_recv()

    for copy in wr_copies:
        copy.wait()
    columns = jnp.concatenate([dp_in[0], dp[...], dp_in[1]], axis=1)
    hi, lo = split(columns)
    weights = [wr[part].reshape(384, 512) for part in range(2)]
    value = dot(jnp.concatenate([hi, lo], axis=0), weights[0])
    value = value[:32] + value[32:] + dot(hi, weights[1])
    for c in range(CHUNKS):
        add_rows[c] = value[:, c * 128 : c * 128 + 128]

    def spread_additions(c):
        for target, rows, width, first in ((a1, 32, 128, 0), (a2, 16, 64, 32), (a4, 8, 32, 48)):
            parts = 128 // width
            for f in range(4 // parts):
                fields = [add_rows[c, pl.ds((f * parts + part) * 8, 8), :] for part in range(parts)]
                for y in range(rows):
                    add = jnp.zeros((8, 128), F32)
                    for part in range(parts):
                        add = jnp.where(lane == part * width, roll(fields[part], part * width - first - y), add)
                    target[c, y, pl.ds(f * 8, 8), :] = add

    low = jnp.where(has_s, 1.0, 0.0).astype(F32)
    high = jnp.where(has_n, 1.0, 0.0).astype(F32)

    def one_pass(window):
        total = window[4]
        for k in range(1, 5):
            total = total + row_taps[k] * (window[4 - k] + window[4 + k])
        return total

    def filter_rows(c, source, target, rows, fields, width, base, additions):
        group = width // 8
        place = (lane % width) // 8

        def column(f, carry):
            at_f = pl.ds(f * 8, 8)
            window, passed = [], []
            east = west = None
            for row in range(rows):
                window.append(source[c, row, at_f, :])
                if row < 8:
                    continue
                once = one_pass(window[-9:])
                if row - 8 < 4:
                    once = once * low
                if row >= rows - 4:
                    once = once * high
                passed.append(once)
                if len(passed) < 9:
                    continue
                twice = one_pass(passed[-9:])
                y = row - 16
                twice = twice + additions[c, y, at_f, :]
                target[c, y, at_f, :] = twice
                r = y % group
                to_west, to_east = roll(twice, 8 * r), roll(twice, 8 * r + 8 - width)
                if r == 0:
                    west, east = to_west, to_east
                else:
                    west, east = jnp.where(place == r, to_west, west), jnp.where(place == r, to_east, east)
                if r == group - 1:
                    start = base + (y // group) * fields + f * 8
                    sp[0, c, pl.ds(start, 8), :] = east
                    sp[1, c, pl.ds(start, 8), :] = west
            return carry

        for f in range(fields // 8):
            column(f, 0)

    outer = (gy < 2) | (gy >= ny - 2)
    defer_e = outer & has_e & (gx == nx // 2 - 1)
    defer_w = outer & has_w & (gx == nx // 2)

    def rows_stage(c):
        spread_additions(c)

        @pl.when(has_s)
        def _():
            for copy in y_copies(c, 0):
                copy.wait_recv()

        @pl.when(has_n)
        def _():
            for copy in y_copies(c, 1):
                copy.wait_recv()

        @pl.when(has_n)
        def _():
            for m2 in range(2):
                for h in range(2):
                    at_f = pl.ds(m2 * 16 + h * 8, 8)
                    px[c, 40, at_f, :] = m_in[c, at_f, :] * c_next[pl.ds(h * 8, 8), :]

        quarter_blocks_of_rows([(c, 6, 0), (c, 7, 4), (c, 16, 40), (c, 17, 44)])
        half_blocks([(c, k) for k in (4, 5, 6, 7, 24, 25, 26, 27)])
        quarter_blocks([(c, k) for k in (4, 5, 18, 19)])
        filter_rows(c, px, y1, 48, 32, 128, 0, a1)
        filter_rows(c, p2x, y2, 32, 16, 64, 64, a2)
        filter_rows(c, p4x, y4, 24, 8, 32, 96, a4)

        @pl.when(has_e & (jnp.logical_not(defer_e) | (c > DEFER)))
        def _():
            x_copy(c, 0).start()

        @pl.when(has_w & (jnp.logical_not(defer_w) | (c > DEFER)))
        def _():
            x_copy(c, 1).start()

        @pl.when(defer_e & (c == DEFER))
        def _():
            for chunk in range(DEFER + 1):
                x_copy(chunk, 0).start()

        @pl.when(defer_w & (c == DEFER))
        def _():
            for chunk in range(DEFER + 1):
                x_copy(chunk, 1).start()

    comb[...] = jnp.zeros((32, 16, 128), F32)
    w1_copy.wait()
    w2_copy.wait()
    w4_copy.wait()

    def halo(c, start, fields, r, width):
        west, east = rp[0, c, pl.ds(start, fields), :], rp[1, c, pl.ds(start, fields), :]
        take_west = lax.broadcasted_iota(jnp.int32, (fields, 128), 1) % width < 8
        return jnp.where(take_west, roll(west, -8 * r), roll(east, 8 - 8 * r))

    def columns_stage(c):
        @pl.when(has_w)
        def _():
            x_copy(c, 0).wait_recv()

        @pl.when(has_e)
        def _():
            x_copy(c, 1).wait_recv()

        sides = [halo(c, 96 + (q // 4) * 8, 8, q % 4, 32) for q in range(8)]
        value = jnp.concatenate([y4[c].reshape(64, 128), jnp.concatenate(sides, axis=0)], axis=1)
        o4[...] = full_dot(value, w4[0], w4[1])
        sides = [halo(c, 64 + (q // 8) * 16, 16, q % 8, 64) for q in range(16)]
        value = jnp.concatenate([y2[c].reshape(256, 128), jnp.concatenate(sides, axis=0)], axis=1)
        o2[...] = full_dot(value, w2[0], w2[1])

        def block(b, carry):
            @pl.when((b == 1) & (c == CHUNKS - 1) & has_s)
            def _():
                end_row_copy.start()

            @pl.when((b == 1) & (c == CHUNKS - 1) & has_w & has_s)
            def _():
                end_corner_copy.start()

            for part in range(2):
                first = b * 16 + part * 8
                start = pl.multiple_of(b * 32, 32)
                sides = [halo(c, start, 32, part * 8 + r, 128) for r in range(8)]
                rows = y1[c, pl.ds(first, 8)].reshape(256, 128)
                both = exact_dot(jnp.concatenate([rows, jnp.concatenate(sides, axis=0)], axis=1), w1[...])
                value = both[:, :128] + both[:, 128:]
                for r in range(8):
                    y = first + r
                    at2 = pl.multiple_of((b * 8 + part * 4 + r // 2) * 16, 16)
                    at4 = pl.multiple_of((b * 4 + part * 2 + r // 4) * 8, 8)
                    for h in range(2):
                        total = comb[y, pl.ds(h * 8, 8), :]
                        for m2 in range(2):
                            begin = r * 32 + m2 * 16 + h * 8
                            local = value[begin : begin + 8]
                            local = local + o2[pl.ds(at2 + m2 * 8, 8), pl.ds(h * 128, 128)]
                            local = local + o4[pl.ds(at4, 8), pl.ds((m2 * 2 + h) * 128, 128)]
                            total = total + member(c, m2, h, y) * local
                        comb[y, pl.ds(h * 8, 8), :] = total
            return carry

        lax.fori_loop(0, 2, block, 0)

    def stages(step, carry):
        @pl.when(step < CHUNKS)
        def _():
            rows_stage(step)

        @pl.when(step >= LAG)
        def _():
            columns_stage(step - LAG)

        return carry

    lax.fori_loop(0, CHUNKS + LAG, stages, 0)

    for h in range(2):
        packed = comb[0, pl.ds(h * 8, 8), :]
        for y in range(1, 32):
            packed = jnp.where(lane == y, roll(comb[y, pl.ds(h * 8, 8), :], y), packed)
        end_col_out[pl.ds(h * 8, 8), :] = packed

    @pl.when(has_w)
    def _():
        end_col_copy.start()

    def send_waits(c, carry):
        @pl.when(has_n)
        def _():
            for copy in y_copies(c, 0):
                copy.wait_send()

        @pl.when(has_s)
        def _():
            for copy in y_copies(c, 1):
                copy.wait_send()

        @pl.when(has_e)
        def _():
            x_copy(c, 0).wait_send()

        @pl.when(has_w)
        def _():
            x_copy(c, 1).wait_send()

        return carry

    spread_copy.wait()
    flats = [out.at[side].reshape(LEV * APAD, 128) for side in range(2)]

    def store_row(y, side, h, value):
        flats[side][pl.ds(h * 8 * APAD + y, 8, stride=APAD), :] = value

    def row_of(y, h):
        return flats[1][pl.ds(h * 8 * APAD + y, 8, stride=APAD), :]

    for block in range(4):
        rows = []
        for j in range(block * 8, block * 8 + 8):
            rows += [comb[j], 0.5 * (comb[j] + comb[j + 1])] if j < 31 else [comb[j]]
        value = exact_dot(jnp.concatenate(rows, axis=0), spread[pl.ds(0, 128), :])
        for k in range(len(rows)):
            for h in range(2):
                for side in range(2):
                    begin = k * 16 + h * 8
                    store_row(block * 16 + k, side, h, value[begin : begin + 8, side * 128 : side * 128 + 128])

    lax.fori_loop(0, CHUNKS, send_waits, 0)

    @pl.when(has_e)
    def _():
        col_copy.wait_send()
        end_col_copy.wait_recv()

    @pl.when(has_n)
    def _():
        row_copy.wait_send()
        dp_north.wait_send()
        end_row_copy.wait_recv()

    @pl.when(has_e & has_n)
    def _():
        corner_copy.wait_send()
        end_corner_copy.wait_recv()

    for h in range(2):
        levels = pl.ds(h * 8, 8)
        edge = jnp.where(lane == 32, roll(end_corner_in[levels, :], 32), end_col_in[levels, :])
        half_edge = 0.5 * (edge + roll(edge, -1))
        for y in range(63):
            add = roll((half_edge, edge)[y % 2 == 0], 127 - y // 2)
            store_row(y, 1, h, row_of(y, h) + jnp.where(lane == 127, 0.5 * add, 0.0))
        last = 0.5 * (comb[31, levels, :] + end_row_in[levels, :])
        value = exact_dot(jnp.concatenate([last, roll(half_edge, -31)], axis=1), spread[...])
        for side in range(2):
            store_row(63, side, h, value[:, side * 128 : side * 128 + 128])

    @pl.when(has_s)
    def _():
        end_row_copy.wait_send()
        first_coarse.wait_send()
        dp_south.wait_send()

    @pl.when(has_w)
    def _():
        end_col_copy.wait_send()

    @pl.when(has_w & has_s)
    def _():
        end_corner_copy.wait_send()


def output_kernel(padded, out_hbm, sem):
    copies = [
        pltpu.make_async_copy(
            padded.at[side, :, pl.ds(0, 64), :], out_hbm.at[:, :, pl.ds(side * 128, 128)], sem.at[side]
        )
        for side in range(2)
    ]
    for copy in copies:
        copy.start()
    for copy in copies:
        copy.wait()


def shards(nx, ny, gradient, members):
    filters, rows, small, spread = constants()
    w1, w2, w4 = (jnp.asarray(value) for value in filters)
    any_space = pl.BlockSpec(memory_space=pltpu.HBM)
    in_vmem = pl.BlockSpec(memory_space=pltpu.VMEM)
    dma = pltpu.SemaphoreType.DMA

    def vmem(*shape, dtype=F32):
        return pltpu.VMEM(shape, dtype)

    padded = pl.pallas_call(
        functools.partial(main_kernel, nx, ny),
        name="localise",
        out_shape=jax.ShapeDtypeStruct((2, LEV, APAD, 128), F32),
        in_specs=[any_space] * 8,
        out_specs=in_vmem,
        scratch_shapes=[
            vmem(2, LEV, APAD, 128),
            vmem(MEM, LEV, MPAD, 128),
            vmem(256, 256, dtype=BF16),
            vmem(2, 256, 256, dtype=BF16),
            vmem(2, 256, 512, dtype=BF16),
            vmem(2, 3, 128, 512, dtype=BF16),
            vmem(5, 256, 128, dtype=BF16),
            vmem(256, 256, dtype=BF16),
            vmem(32, 16, 128),
            vmem(LEV, APAD, 128),
            vmem(32, 16, 128),
            vmem(CHUNKS, 48, 32, 128),
            vmem(CHUNKS, 32, 16, 128),
            vmem(CHUNKS, 24, 8, 128),
            vmem(CHUNKS, 32, 32, 128),
            vmem(CHUNKS, 16, 16, 128),
            vmem(CHUNKS, 8, 8, 128),
            vmem(2, CHUNKS, 112, 128),
            vmem(2, CHUNKS, 112, 128),
            vmem(256, 256),
            vmem(64, 512),
            vmem(16, 128),
            vmem(16, 128),
            vmem(2, 16, 128),
            vmem(2, 16, 128),
            vmem(16, 128),
            vmem(CHUNKS, 32, 128),
            vmem(CHUNKS, 32, 128),
            vmem(16, 128),
            vmem(16, 128),
            vmem(16, 128),
            vmem(32, 128),
            vmem(2, 32, 128),
            vmem(CHUNKS, 32, 128),
            vmem(CHUNKS, 32, 32, 128),
            vmem(CHUNKS, 16, 16, 128),
            vmem(CHUNKS, 8, 8, 128),
            vmem(16, 128),
            vmem(16, 128),
            vmem(16, 128),
            vmem(16, 128),
            dma((8,)),
            dma((2, 3, CHUNKS)),
            dma((3,)),
            dma((3,)),
            dma((4,)),
            dma((4,)),
            dma((2, CHUNKS, 4)),
            dma((2, CHUNKS, 4)),
            dma((2, CHUNKS)),
            dma((2, CHUNKS)),
            dma((3,)),
            dma((3,)),
        ],
        compiler_params=pltpu.CompilerParams(collective_id=0, has_side_effects=True, vmem_limit_bytes=48 << 20),
    )(*(pltpu.with_memory_space_constraint(value, pltpu.HBM) for value in (gradient, members, w1, w2, w4, jnp.asarray(rows), jnp.asarray(small), jnp.asarray(spread))))
    return pl.pallas_call(
        output_kernel,
        name="output",
        out_shape=jax.ShapeDtypeStruct((LEV, 64, 256), F32),
        in_specs=[in_vmem],
        out_specs=any_space,
        scratch_shapes=[dma((2,))],
        compiler_params=pltpu.CompilerParams(vmem_limit_bytes=8 << 20),
    )(padded)


def solution(mesh):
    in_specs = (P(None, "gy", "gx"), P(None, None, "gy", "gx"))
    return jax.shard_map(
        functools.partial(shards, mesh.shape["gx"], mesh.shape["gy"]),
        mesh=mesh,
        in_specs=in_specs,
        out_specs=P(None, "gy", "gx"),
        check_vma=False,
    )
```

```python
import functools

import jax
import jax.numpy as jnp
import ml_dtypes
import numpy as np
from jax import lax
from jax.experimental import pallas as pl
from jax.experimental.pallas import tpu as pltpu
from jax.sharding import PartitionSpec as P

MESH = pl.DeviceIdType.MESH
F32, BF16 = jnp.float32, jnp.bfloat16
LEV, MEM = 16, 8
CHUNKS = 4
LAG = 3
DEFER = 2
MPAD = 40
APAD = 72

beta_raw = [(1.0 - (offset - 4) ** 2 / 25.0) ** 2 for offset in range(9)]
beta_taps = [value / sum(beta_raw) for value in beta_raw]
generations = ((1, 0.5), (2, 0.075), (4, 0.0125))
row_taps = [beta_taps[4 + k] / beta_taps[4] for k in range(5)]


def halves(matrix):
    hi = matrix.astype(ml_dtypes.bfloat16)
    lo = (matrix - hi.astype(np.float64)).astype(ml_dtypes.bfloat16)
    return np.stack([hi, lo])


def band(outputs):
    matrix = np.zeros((outputs + 8, outputs))
    for column in range(outputs):
        matrix[column : column + 9, column] = beta_taps
    return matrix


def column_filter(factor, weight, west_edge, east_edge):
    count = 128 // factor
    inside = np.ones(count + 8)
    if west_edge:
        inside[:4] = 0.0
    if east_edge:
        inside[-4:] = 0.0
    both = band(count + 8) @ (inside[:, None] * band(count))
    both = np.repeat(both, factor, axis=1) * (weight / (MEM - 1) * beta_taps[4] ** 2)
    result = np.zeros((256, 128 * factor))
    for part in range(factor):
        columns = slice(part * 128, part * 128 + 128)
        start = part * count
        result[start : start + count, columns] = both[8 : count + 8]
        result[128 + start : 136 + start, columns] = both[:8]
        result[136 + start : 144 + start, columns] = both[count + 8 :]
    return halves(result)


def row_filter(south_edge, north_edge):
    result = np.zeros((96, 128))
    start = 0
    for factor, _ in generations:
        count = 32 // factor
        inside = np.ones(count + 8)
        if south_edge:
            inside[:4] = 0.0
        if north_edge:
            inside[-4:] = 0.0
        both = band(count + 8) @ (inside[:, None] * band(count)) / beta_taps[4] ** 2
        for row in range(96):
            block = (row - 32) // factor + 8
            if 0 <= block < count + 16:
                result[row, start : start + count] = both[block]
        start += count
    return halves(result)


def constants():
    filters = []
    for factor, weight in generations:
        kinds = [column_filter(factor, weight, *edges) for edges in ((True, False), (False, False), (False, True))]
        filters.append(np.stack(kinds))
    filters[0] = np.concatenate([filters[0][:, 0], filters[0][:, 1]], axis=2)
    pairs = np.zeros((256, 128))
    reduce_columns = np.zeros((256, 128))
    for lane in range(128):
        pairs[2 * lane : 2 * lane + 2, lane] = 1.0
        reduce_columns[2 * lane, lane] = 1.0
        reduce_columns[2 * lane + 1, lane] = 0.5
        if lane:
            reduce_columns[2 * lane - 1, lane] = 0.5
    fours = np.zeros((2, 256, 128))
    for lane in range(256):
        fours[0, lane, lane // 4] = 1.0
        fours[1, lane, 64 + lane // 4] = 1.0
    border = np.zeros((256, 128))
    for chunk in range(CHUNKS):
        for j in range(32):
            border[2 * j, chunk * 32 + j] = 0.5
            border[2 * j + 1, chunk * 32 + j] = 0.25
            if j:
                border[2 * j - 1, chunk * 32 + j] = 0.25
    small = np.stack([pairs, reduce_columns, *fours, border]).astype(ml_dtypes.bfloat16)
    rows = np.stack([row_filter(*edges) for edges in ((True, False), (False, False), (False, True))])
    spread = np.zeros((256, 256))
    for lane in range(128):
        spread[lane, 2 * lane] = 1.0
        spread[lane, 2 * lane + 1] = 0.5
        spread[lane + 1, 2 * lane + 1] = 0.5
    return filters, rows, small, spread.astype(ml_dtypes.bfloat16)


def split(value):
    hi = value.astype(BF16)
    return hi, (value - hi.astype(F32)).astype(BF16)


def dot(a, b):
    return jnp.dot(a, b, preferred_element_type=F32)


def exact_dot(value, matrix):
    rows = value.shape[0]
    hi, lo = split(value)
    both = dot(jnp.concatenate([hi, lo], axis=0), matrix)
    return both[:rows] + both[rows:]


def full_dot(value, hi_matrix, lo_matrix):
    hi, lo = split(value)
    return dot(hi, hi_matrix) + dot(lo, hi_matrix) + dot(hi, lo_matrix)


def roll(value, shift):
    shift %= 128
    return value if shift == 0 else pltpu.roll(value, shift, 1)


def main_kernel(
    nx, ny,
    g_hbm, m_hbm, w1_hbm, w2_hbm, w4_hbm, wr_hbm, small_hbm, spread_hbm,
    out,
    gv, mv, w1, w2, w4, wr, small, spread, comb,
    ac, cz, px, p2x, p4x, y1, y2, y4, sp, rp, o2, o4,
    col_out, col_in, row_out, row_in, corner_in, m_out, m_in, c_out, c_in, c_next, dp, dp_in, add_rows, a1, a2, a4,
    end_row_in, end_col_out, end_col_in, end_corner_in,
    local_sem, wr_sem, s1, r1, sf, rf, ys, yr, xs, xr, s3, r3,
):
    gx, gy = lax.axis_index("gx"), lax.axis_index("gy")
    has_w, has_e = gx > 0, gx < nx - 1
    has_s, has_n = gy > 0, gy < ny - 1

    kind = 1 - (gx == 0).astype(jnp.int32) + (gx == nx - 1).astype(jnp.int32)
    g_copies = [
        pltpu.make_async_copy(
            g_hbm.at[:, :, pl.ds(side * 128, 128)], gv.at[side, :, pl.ds(0, 64), :], local_sem.at[side * 6]
        )
        for side in range(2)
    ]
    m_copy = pltpu.make_async_copy(m_hbm, mv.at[:, :, pl.ds(0, 32), :], local_sem.at[1])
    small_copy = pltpu.make_async_copy(small_hbm, small, local_sem.at[2])
    w1_copy = pltpu.make_async_copy(w1_hbm.at[kind], w1, local_sem.at[3])
    w2_copy = pltpu.make_async_copy(w2_hbm.at[kind], w2, local_sem.at[4])
    w4_copy = pltpu.make_async_copy(w4_hbm.at[kind], w4, local_sem.at[5])
    spread_copy = pltpu.make_async_copy(spread_hbm, spread, local_sem.at[7])
    row_kind = 1 - (gy == 0).astype(jnp.int32) + (gy == ny - 1).astype(jnp.int32)
    wr_copies = [
        pltpu.make_async_copy(
            wr_hbm.at[row_kind, part, pl.ds(tile * 32, 32), :],
            wr.at[part, tile, pl.ds(c * 32, 32), pl.ds(c * 128, 128)],
            wr_sem.at[part, tile, c],
        )
        for part in range(2) for tile in range(3) for c in range(CHUNKS)
    ]
    for copy in (g_copies[1], g_copies[0], small_copy, m_copy, *wr_copies, w1_copy, w2_copy, w4_copy, spread_copy):
        copy.start()

    barrier = pltpu.get_barrier_semaphore()
    around = [
        (has_w, -1, 0), (has_e, 1, 0), (has_s, 0, -1), (has_n, 0, 1),
        (has_w & has_s, -1, -1), (has_e & has_n, 1, 1),
    ]

    def at(dx, dy):
        return {"gx": gx + dx, "gy": gy + dy}

    for there, dx, dy in around:
        @pl.when(there)
        def _(dx=dx, dy=dy):
            pl.semaphore_signal(barrier, inc=1, device_id=at(dx, dy), device_id_type=MESH)

    for part in range(2):
        for tile in range(3):
            for c in range(CHUNKS):
                for other in range(CHUNKS):
                    if other != c:
                        wr[part, tile, pl.ds(c * 32, 32), pl.ds(other * 128, 128)] = jnp.zeros((32, 128), BF16)

    @pl.when(jnp.logical_not(has_s))
    def _():
        px[:, pl.ds(0, 8)] = jnp.zeros((CHUNKS, 8, 32, 128), F32)
        p2x[:, pl.ds(0, 4)] = jnp.zeros((CHUNKS, 4, 16, 128), F32)
        p4x[:, pl.ds(0, 4)] = jnp.zeros((CHUNKS, 4, 8, 128), F32)
        row_in[...] = jnp.zeros((2, 16, 128), F32)
        dp_in[0] = jnp.zeros((32, 128), F32)

    @pl.when(jnp.logical_not(has_n))
    def _():
        px[:, pl.ds(40, 8)] = jnp.zeros((CHUNKS, 8, 32, 128), F32)
        p2x[:, pl.ds(28, 4)] = jnp.zeros((CHUNKS, 4, 16, 128), F32)
        p4x[:, pl.ds(20, 4)] = jnp.zeros((CHUNKS, 4, 8, 128), F32)
        end_row_in[...] = jnp.zeros((16, 128), F32)
        dp_in[1] = jnp.zeros((32, 128), F32)

    @pl.when(jnp.logical_not(has_w))
    def _():
        rp[0] = jnp.zeros((CHUNKS, 112, 128), F32)
        col_in[...] = jnp.zeros((16, 128), F32)

    @pl.when(jnp.logical_not(has_e))
    def _():
        rp[1] = jnp.zeros((CHUNKS, 112, 128), F32)
        end_col_in[...] = jnp.zeros((16, 128), F32)

    @pl.when(jnp.logical_not(has_w & has_s))
    def _():
        corner_in[...] = jnp.zeros((16, 128), F32)

    @pl.when(jnp.logical_not(has_e & has_n))
    def _():
        end_corner_in[...] = jnp.zeros((16, 128), F32)

    def remote(src, dst, send, recv, dx, dy):
        return pltpu.make_async_remote_copy(
            src_ref=src, dst_ref=dst, send_sem=send, recv_sem=recv, device_id=at(dx, dy), device_id_type=MESH
        )

    col_copy = remote(col_out, col_in, s1.at[0], r1.at[0], 1, 0)
    row_copy = remote(row_out, row_in, s1.at[1], r1.at[1], 0, 1)
    corner_copy = remote(col_out, corner_in, s1.at[2], r1.at[2], 1, 1)
    end_row_copy = remote(comb.at[0], end_row_in, s3.at[0], r3.at[0], 0, -1)
    end_col_copy = remote(end_col_out, end_col_in, s3.at[1], r3.at[1], -1, 0)
    end_corner_copy = remote(comb.at[0], end_corner_in, s3.at[2], r3.at[2], -1, -1)

    def y_copies(c, direction, pieces=slice(0, 4)):
        if direction == 0:
            places = ((px, 32, 0, 8), (p2x, 16, 0, 4), (p4x, 8, 0, 4))
            dy = 1
        else:
            places = ((px, 9, 41, 7), (p2x, 12, 28, 4), (p4x, 12, 20, 4))
            dy = -1
        ends = [(ref.at[c, pl.ds(src, n)], ref.at[c, pl.ds(dst, n)]) for ref, src, dst, n in places]
        if direction == 1:
            ends.append((m_out.at[c], m_in.at[c]))
        return [
            remote(src, dst, ys.at[direction, c, i], yr.at[direction, c, i], 0, dy)
            for i, (src, dst) in list(enumerate(ends))[pieces]
        ]

    dp_north = remote(dp, dp_in.at[0], sf.at[2], rf.at[2], 0, 1)
    dp_south = remote(dp, dp_in.at[1], sf.at[3], rf.at[3], 0, -1)
    first_coarse = remote(c_out, c_in, sf.at[1], rf.at[1], 0, -1)

    def x_copy(c, direction):
        if direction == 0:
            return remote(sp.at[0, c], rp.at[0, c], xs.at[0, c], xr.at[0, c], 1, 0)
        return remote(sp.at[1, c], rp.at[1, c], xs.at[1, c], xr.at[1, c], -1, 0)

    lane = lax.broadcasted_iota(jnp.int32, (8, 128), 1)
    first_lane = lane == 0

    g_copies[1].wait()
    g0, g1 = gv.at[0].reshape(LEV * APAD, 128), gv.at[1].reshape(LEV * APAD, 128)

    def gradient_row(half, y, h):
        return half[pl.ds(h * 8 * APAD + y, 8, stride=APAD), :]

    for h in range(2):
        parts = []
        for quarter in range(2):
            packed = jnp.zeros((8, 128), F32)
            for y in range(quarter * 32, quarter * 32 + 32):
                packed = jnp.where(lane == y, roll(gradient_row(g1, y, h), y + 1), packed)
            parts.append(packed)
        col_out[pl.ds(h * 8, 8), :] = jnp.where(lane < 32, parts[0], parts[1])
    g_copies[0].wait()
    for h in range(2):
        row_out[0, pl.ds(h * 8, 8), :] = gradient_row(g0, 63, h)
        row_out[1, pl.ds(h * 8, 8), :] = gradient_row(g1, 63, h)

    small_copy.wait()
    for block in range(4):
        levels = pl.ds(block * 4, 4)
        value = jnp.concatenate(
            [gv[side, levels, pl.ds(0, 64), :].reshape(256, 128) for side in range(2)], axis=1
        )
        ac[levels, pl.ds(0, 64), :] = exact_dot(value, small[1]).reshape(4, 64, 128)
    ar = ac.reshape(LEV * APAD, 128)

    def across_row(y, h):
        return ar[pl.ds(h * 8 * APAD + y, 8, stride=APAD), :]

    for h in range(2):
        c_out[pl.ds(h * 8, 8), :] = across_row(0, h) + 0.5 * across_row(1, h)

    def reduce_rows(j, carry):
        odd_rows = []
        for h in range(2):
            odd = across_row(2 * j + 1, h)
            cz[j, pl.ds(h * 8, 8), :] = across_row(2 * j, h) + 0.5 * (odd + carry[h])
            odd_rows.append(odd)
        return tuple(odd_rows)

    lax.fori_loop(1, 32, reduce_rows, tuple(across_row(1, h) for h in range(2)))
    mr = mv.reshape(MEM * LEV * MPAD, 128)

    def member(c, m2, h, y):
        return mr[pl.ds(((2 * c + m2) * LEV + h * 8) * MPAD + y, 8, stride=MPAD), :]

    m_copy.wait()

    for c in range(CHUNKS):
        for m2 in range(2):
            for h in range(2):
                m_out[c, pl.ds(m2 * 16 + h * 8, 8), :] = member(c, m2, h, 0)

    def half_blocks(places):
        rows = []
        for c, k in places:
            pair = px[c, 2 * k - 8] + px[c, 2 * k - 7]
            for m2 in range(2):
                rows.append(jnp.concatenate([pair[m2 * 16 : m2 * 16 + 8], pair[m2 * 16 + 8 : m2 * 16 + 16]], axis=1))
        value = exact_dot(jnp.concatenate(rows, axis=0), small[0])
        for i, (c, k) in enumerate(places):
            p2x[c, k] = value[i * 16 : i * 16 + 16]

    def quarter_blocks(places):
        rows = []
        for c, k in places:
            pair = p2x[c, 2 * k - 8] + p2x[c, 2 * k - 7]
            rows.append(jnp.concatenate([pair[:8], pair[8:]], axis=1))
        value = exact_dot(jnp.concatenate(rows, axis=0), small[0])
        for i, (c, k) in enumerate(places):
            p4x[c, k] = value[i * 8 : i * 8 + 8]

    def quarter_blocks_of_rows(places):
        rows = [[], []]
        for c, k, row in places:
            four = (px[c, row] + px[c, row + 1]) + (px[c, row + 2] + px[c, row + 3])
            for m2 in range(2):
                rows[m2].append(jnp.concatenate([four[m2 * 16 : m2 * 16 + 8], four[m2 * 16 + 8 : m2 * 16 + 16]], axis=1))
        value = sum(exact_dot(jnp.concatenate(rows[m2], axis=0), small[2 + m2]) for m2 in range(2))
        for i, (c, k, _) in enumerate(places):
            p4x[c, k] = value[i * 8 : i * 8 + 8]

    def product_row(c, y):
        for m2 in range(2):
            for h in range(2):
                px[c, 8 + y, pl.ds(m2 * 16 + h * 8, 8), :] = member(c, m2, h, y) * cz[y, pl.ds(h * 8, 8), :]

    def start_rows(c, north, south):
        @pl.when(has_n)
        def _():
            for copy in y_copies(c, 0, north):
                copy.start()

        @pl.when(has_s)
        def _():
            for copy in y_copies(c, 1, south):
                copy.start()

    everything, nothing = slice(0, 4), slice(0, 0)

    def later_rows(c):
        def row(y, carry):
            product_row(c, y)
            return carry

        lax.fori_loop(1, 32, row, 0, unroll=4)

    def first_columns():
        @pl.when(has_w)
        def _():
            col_copy.wait_recv()

        coarse = exact_dot(jnp.concatenate([col_in[...], jnp.zeros((16, 128), F32)], axis=1), small[4])

        for m2 in range(2):
            for h in range(2):
                columns = []
                for c in range(CHUNKS):
                    column = roll(member(c, m2, h, 0), c * 32)
                    for y in range(1, 32):
                        place = c * 32 + y
                        column = jnp.where(lane == place, roll(member(c, m2, h, y), place), column)
                    columns.append(column)
                column = columns[0]
                for c in range(1, CHUNKS):
                    column = jnp.where(lane >= c * 32, columns[c], column)
                dp[pl.ds(m2 * 16 + h * 8, 8), :] = column * coarse[h * 8 : h * 8 + 8]

        @pl.when(has_n)
        def _():
            dp_north.start()

        @pl.when(has_s)
        def _():
            dp_south.start()

    def own_rows(c):
        later_rows(c)
        half_blocks([(c, k) for k in range(12, 24)])
        quarter_blocks([(c, k) for k in range(12, 16)])

    def without_first_row(c, carry):
        own_rows(c)
        start_rows(c, slice(0, 2), everything)
        return carry

    def first_row(c, carry):
        product_row(c, 0)
        half_blocks([(c, k) for k in range(8, 12)])
        quarter_blocks([(c, k) for k in range(8, 12)])
        start_rows(c, slice(2, 3), nothing)
        return carry

    def whole(c, carry):
        later_rows(c)
        product_row(c, 0)
        half_blocks([(c, k) for k in range(8, 24)])
        quarter_blocks([(c, k) for k in range(8, 16)])
        start_rows(c, everything, everything)
        return carry

    def first_coarse_row():
        @pl.when(has_s)
        def _():
            row_copy.wait_recv()

        @pl.when(has_w & has_s)
        def _():
            corner_copy.wait_recv()

        before = exact_dot(jnp.concatenate([row_in[0], row_in[1]], axis=1), small[1])
        for h in range(2):
            corner = jnp.where(first_lane, 0.5 * roll(corner_in[pl.ds(h * 8, 8), :], -63), 0.0)
            cz[0, pl.ds(h * 8, 8), :] = c_out[pl.ds(h * 8, 8), :] + 0.5 * (before[h * 8 : h * 8 + 8] + corner)

    far = (gy % 8 == 0) & has_s
    own_rows(0)
    pl.semaphore_wait(barrier, sum(there.astype(jnp.int32) for there, _, _ in around))

    @pl.when(has_e)
    def _():
        col_copy.start()

    @pl.when(has_n)
    def _():
        row_copy.start()

    @pl.when(has_e & has_n)
    def _():
        corner_copy.start()

    @pl.when(has_s)
    def _():
        first_coarse.start()

    start_rows(0, slice(0, 2), everything)

    far_west = (gx % 4 == 0) & has_w
    near_south = gy % 2 == 1
    second = 1 + far_west.astype(jnp.int32)

    @pl.when(far_west)
    def _():
        without_first_row(1, 0)

    @pl.when(near_south)
    def _():
        first_coarse_row()
        first_row(0, 0)

    first_columns()

    @pl.when(far)
    def _():
        lax.fori_loop(second, CHUNKS, without_first_row, 0)

    @pl.when(jnp.logical_not(near_south))
    def _():
        first_coarse_row()
        first_row(0, 0)

    @pl.when(far)
    def _():
        lax.fori_loop(1, CHUNKS, first_row, 0)

    @pl.when(jnp.logical_not(far) & far_west)
    def _():
        first_row(1, 0)

    @pl.when(jnp.logical_not(far))
    def _():
        lax.fori_loop(second, CHUNKS, whole, 0)

    @pl.when(has_n)
    def _():
        first_coarse.wait_recv()
        for h in range(2):
            corner = jnp.where(first_lane, 0.5 * roll(col_in[pl.ds(h * 8, 8), :], -63), 0.0)
            c_next[pl.ds(h * 8, 8), :] = c_in[pl.ds(h * 8, 8), :] + 0.5 * (across_row(63, h) + corner)

    @pl.when(has_s)
    def _():
        dp_north.wait_recv()

    @pl.when(has_n)
    def _():
        dp_south.wait_recv()

    for copy in wr_copies:
        copy.wait()
    columns = jnp.concatenate([dp_in[0], dp[...], dp_in[1]], axis=1)
    hi, lo = split(columns)
    weights = [wr[part].reshape(384, 512) for part in range(2)]
    value = dot(jnp.concatenate([hi, lo], axis=0), weights[0])
    value = value[:32] + value[32:] + dot(hi, weights[1])
    for c in range(CHUNKS):
        add_rows[c] = value[:, c * 128 : c * 128 + 128]

    def spread_additions(c):
        for target, rows, width, first in ((a1, 32, 128, 0), (a2, 16, 64, 32), (a4, 8, 32, 48)):
            parts = 128 // width
            for f in range(4 // parts):
                fields = [add_rows[c, pl.ds((f * parts + part) * 8, 8), :] for part in range(parts)]
                for y in range(rows):
                    add = jnp.zeros((8, 128), F32)
                    for part in range(parts):
                        add = jnp.where(lane == part * width, roll(fields[part], part * width - first - y), add)
                    target[c, y, pl.ds(f * 8, 8), :] = add

    low = jnp.where(has_s, 1.0, 0.0).astype(F32)
    high = jnp.where(has_n, 1.0, 0.0).astype(F32)

    def one_pass(window):
        total = window[4]
        for k in range(1, 5):
            total = total + row_taps[k] * (window[4 - k] + window[4 + k])
        return total

    def filter_rows(c, source, target, rows, fields, width, base, additions):
        group = width // 8
        place = (lane % width) // 8

        def column(f, carry):
            at_f = pl.ds(f * 8, 8)
            window, passed = [], []
            east = west = None
            for row in range(rows):
                window.append(source[c, row, at_f, :])
                if row < 8:
                    continue
                once = one_pass(window[-9:])
                if row - 8 < 4:
                    once = once * low
                if row >= rows - 4:
                    once = once * high
                passed.append(once)
                if len(passed) < 9:
                    continue
                twice = one_pass(passed[-9:])
                y = row - 16
                twice = twice + additions[c, y, at_f, :]
                target[c, y, at_f, :] = twice
                r = y % group
                to_west, to_east = roll(twice, 8 * r), roll(twice, 8 * r + 8 - width)
                if r == 0:
                    west, east = to_west, to_east
                else:
                    west, east = jnp.where(place == r, to_west, west), jnp.where(place == r, to_east, east)
                if r == group - 1:
                    start = base + (y // group) * fields + f * 8
                    sp[0, c, pl.ds(start, 8), :] = east
                    sp[1, c, pl.ds(start, 8), :] = west
            return carry

        for f in range(fields // 8):
            column(f, 0)

    outer = (gy < 2) | (gy >= ny - 2)
    defer_e = outer & has_e & (gx == nx // 2 - 1)
    defer_w = outer & has_w & (gx == nx // 2)

    def rows_stage(c):
        spread_additions(c)

        @pl.when(has_s)
        def _():
            for copy in y_copies(c, 0):
                copy.wait_recv()

        @pl.when(has_n)
        def _():
            for copy in y_copies(c, 1):
                copy.wait_recv()

        @pl.when(defer_e & (c == DEFER + 1))
        def _():
            for chunk in range(DEFER + 1):
                x_copy(chunk, 0).start()

        @pl.when(defer_w & (c == DEFER + 1))
        def _():
            for chunk in range(DEFER + 1):
                x_copy(chunk, 1).start()

        @pl.when(has_n)
        def _():
            for m2 in range(2):
                for h in range(2):
                    at_f = pl.ds(m2 * 16 + h * 8, 8)
                    px[c, 40, at_f, :] = m_in[c, at_f, :] * c_next[pl.ds(h * 8, 8), :]

        quarter_blocks_of_rows([(c, 6, 0), (c, 7, 4), (c, 16, 40), (c, 17, 44)])
        half_blocks([(c, k) for k in (4, 5, 6, 7, 24, 25, 26, 27)])
        quarter_blocks([(c, k) for k in (4, 5, 18, 19)])
        filter_rows(c, px, y1, 48, 32, 128, 0, a1)
        filter_rows(c, p2x, y2, 32, 16, 64, 64, a2)
        filter_rows(c, p4x, y4, 24, 8, 32, 96, a4)

        @pl.when(has_e & (jnp.logical_not(defer_e) | (c > DEFER)))
        def _():
            x_copy(c, 0).start()

        @pl.when(has_w & (jnp.logical_not(defer_w) | (c > DEFER)))
        def _():
            x_copy(c, 1).start()

    comb[...] = jnp.zeros((32, 16, 128), F32)
    w1_copy.wait()
    w2_copy.wait()
    w4_copy.wait()

    def halo(c, start, fields, r, width):
        west, east = rp[0, c, pl.ds(start, fields), :], rp[1, c, pl.ds(start, fields), :]
        take_west = lax.broadcasted_iota(jnp.int32, (fields, 128), 1) % width < 8
        return jnp.where(take_west, roll(west, -8 * r), roll(east, 8 - 8 * r))

    def columns_stage(c):
        @pl.when(has_w)
        def _():
            x_copy(c, 0).wait_recv()

        @pl.when(has_e)
        def _():
            x_copy(c, 1).wait_recv()

        sides = [halo(c, 96 + (q // 4) * 8, 8, q % 4, 32) for q in range(8)]
        value = jnp.concatenate([y4[c].reshape(64, 128), jnp.concatenate(sides, axis=0)], axis=1)
        o4[...] = full_dot(value, w4[0], w4[1])
        sides = [halo(c, 64 + (q // 8) * 16, 16, q % 8, 64) for q in range(16)]
        value = jnp.concatenate([y2[c].reshape(256, 128), jnp.concatenate(sides, axis=0)], axis=1)
        o2[...] = full_dot(value, w2[0], w2[1])

        def block(b, carry):
            for part in range(2):
                if part == 1:
                    @pl.when((b == 0) & (c == CHUNKS - 1) & has_s)
                    def _():
                        end_row_copy.start()

                    @pl.when((b == 0) & (c == CHUNKS - 1) & has_w & has_s)
                    def _():
                        end_corner_copy.start()

                first = b * 16 + part * 8
                start = pl.multiple_of(b * 32, 32)
                sides = [halo(c, start, 32, part * 8 + r, 128) for r in range(8)]
                rows = y1[c, pl.ds(first, 8)].reshape(256, 128)
                both = exact_dot(jnp.concatenate([rows, jnp.concatenate(sides, axis=0)], axis=1), w1[...])
                value = both[:, :128] + both[:, 128:]
                for r in range(8):
                    y = first + r
                    at2 = pl.multiple_of((b * 8 + part * 4 + r // 2) * 16, 16)
                    at4 = pl.multiple_of((b * 4 + part * 2 + r // 4) * 8, 8)
                    for h in range(2):
                        total = comb[y, pl.ds(h * 8, 8), :]
                        for m2 in range(2):
                            begin = r * 32 + m2 * 16 + h * 8
                            local = value[begin : begin + 8]
                            local = local + o2[pl.ds(at2 + m2 * 8, 8), pl.ds(h * 128, 128)]
                            local = local + o4[pl.ds(at4, 8), pl.ds((m2 * 2 + h) * 128, 128)]
                            total = total + member(c, m2, h, y) * local
                        comb[y, pl.ds(h * 8, 8), :] = total
            return carry

        lax.fori_loop(0, 2, block, 0)

    def stages(step, carry):
        @pl.when(step < CHUNKS)
        def _():
            rows_stage(step)

        @pl.when(step >= LAG)
        def _():
            columns_stage(step - LAG)

        return carry

    lax.fori_loop(0, CHUNKS + LAG, stages, 0)

    for h in range(2):
        packed = comb[0, pl.ds(h * 8, 8), :]
        for y in range(1, 32):
            packed = jnp.where(lane == y, roll(comb[y, pl.ds(h * 8, 8), :], y), packed)
        end_col_out[pl.ds(h * 8, 8), :] = packed

    @pl.when(has_w)
    def _():
        end_col_copy.start()

    def send_waits(c, carry):
        @pl.when(has_n)
        def _():
            for copy in y_copies(c, 0):
                copy.wait_send()

        @pl.when(has_s)
        def _():
            for copy in y_copies(c, 1):
                copy.wait_send()

        @pl.when(has_e)
        def _():
            x_copy(c, 0).wait_send()

        @pl.when(has_w)
        def _():
            x_copy(c, 1).wait_send()

        return carry

    spread_copy.wait()
    flats = [out.at[side].reshape(LEV * APAD, 128) for side in range(2)]

    def store_row(y, side, h, value):
        flats[side][pl.ds(h * 8 * APAD + y, 8, stride=APAD), :] = value

    def row_of(y, h):
        return flats[1][pl.ds(h * 8 * APAD + y, 8, stride=APAD), :]

    for block in range(4):
        rows = []
        for j in range(block * 8, block * 8 + 8):
            rows += [comb[j], 0.5 * (comb[j] + comb[j + 1])] if j < 31 else [comb[j]]
        value = exact_dot(jnp.concatenate(rows, axis=0), spread[pl.ds(0, 128), :])
        for k in range(len(rows)):
            for h in range(2):
                for side in range(2):
                    begin = k * 16 + h * 8
                    store_row(block * 16 + k, side, h, value[begin : begin + 8, side * 128 : side * 128 + 128])

    lax.fori_loop(0, CHUNKS, send_waits, 0)

    @pl.when(has_e)
    def _():
        col_copy.wait_send()
        end_col_copy.wait_recv()

    @pl.when(has_n)
    def _():
        row_copy.wait_send()
        dp_north.wait_send()
        end_row_copy.wait_recv()

    @pl.when(has_e & has_n)
    def _():
        corner_copy.wait_send()
        end_corner_copy.wait_recv()

    for h in range(2):
        levels = pl.ds(h * 8, 8)
        edge = jnp.where(lane == 32, roll(end_corner_in[levels, :], 32), end_col_in[levels, :])
        half_edge = 0.5 * (edge + roll(edge, -1))
        for y in range(63):
            add = roll((half_edge, edge)[y % 2 == 0], 127 - y // 2)
            store_row(y, 1, h, row_of(y, h) + jnp.where(lane == 127, 0.5 * add, 0.0))
        last = 0.5 * (comb[31, levels, :] + end_row_in[levels, :])
        value = exact_dot(jnp.concatenate([last, roll(half_edge, -31)], axis=1), spread[...])
        for side in range(2):
            store_row(63, side, h, value[:, side * 128 : side * 128 + 128])

    @pl.when(has_s)
    def _():
        end_row_copy.wait_send()
        first_coarse.wait_send()
        dp_south.wait_send()

    @pl.when(has_w)
    def _():
        end_col_copy.wait_send()

    @pl.when(has_w & has_s)
    def _():
        end_corner_copy.wait_send()


def output_kernel(padded, out_hbm, sem):
    copies = [
        pltpu.make_async_copy(
            padded.at[side, :, pl.ds(0, 64), :], out_hbm.at[:, :, pl.ds(side * 128, 128)], sem.at[side]
        )
        for side in range(2)
    ]
    for copy in copies:
        copy.start()
    for copy in copies:
        copy.wait()


def shards(nx, ny, gradient, members):
    filters, rows, small, spread = constants()
    w1, w2, w4 = (jnp.asarray(value) for value in filters)
    any_space = pl.BlockSpec(memory_space=pltpu.HBM)
    in_vmem = pl.BlockSpec(memory_space=pltpu.VMEM)
    dma = pltpu.SemaphoreType.DMA

    def vmem(*shape, dtype=F32):
        return pltpu.VMEM(shape, dtype)

    padded = pl.pallas_call(
        functools.partial(main_kernel, nx, ny),
        name="localise",
        out_shape=jax.ShapeDtypeStruct((2, LEV, APAD, 128), F32),
        in_specs=[any_space] * 8,
        out_specs=in_vmem,
        scratch_shapes=[
            vmem(2, LEV, APAD, 128),
            vmem(MEM, LEV, MPAD, 128),
            vmem(256, 256, dtype=BF16),
            vmem(2, 256, 256, dtype=BF16),
            vmem(2, 256, 512, dtype=BF16),
            vmem(2, 3, 128, 512, dtype=BF16),
            vmem(5, 256, 128, dtype=BF16),
            vmem(256, 256, dtype=BF16),
            vmem(32, 16, 128),
            vmem(LEV, APAD, 128),
            vmem(32, 16, 128),
            vmem(CHUNKS, 48, 32, 128),
            vmem(CHUNKS, 32, 16, 128),
            vmem(CHUNKS, 24, 8, 128),
            vmem(CHUNKS, 32, 32, 128),
            vmem(CHUNKS, 16, 16, 128),
            vmem(CHUNKS, 8, 8, 128),
            vmem(2, CHUNKS, 112, 128),
            vmem(2, CHUNKS, 112, 128),
            vmem(256, 256),
            vmem(64, 512),
            vmem(16, 128),
            vmem(16, 128),
            vmem(2, 16, 128),
            vmem(2, 16, 128),
            vmem(16, 128),
            vmem(CHUNKS, 32, 128),
            vmem(CHUNKS, 32, 128),
            vmem(16, 128),
            vmem(16, 128),
            vmem(16, 128),
            vmem(32, 128),
            vmem(2, 32, 128),
            vmem(CHUNKS, 32, 128),
            vmem(CHUNKS, 32, 32, 128),
            vmem(CHUNKS, 16, 16, 128),
            vmem(CHUNKS, 8, 8, 128),
            vmem(16, 128),
            vmem(16, 128),
            vmem(16, 128),
            vmem(16, 128),
            dma((8,)),
            dma((2, 3, CHUNKS)),
            dma((3,)),
            dma((3,)),
            dma((4,)),
            dma((4,)),
            dma((2, CHUNKS, 4)),
            dma((2, CHUNKS, 4)),
            dma((2, CHUNKS)),
            dma((2, CHUNKS)),
            dma((3,)),
            dma((3,)),
        ],
        compiler_params=pltpu.CompilerParams(collective_id=0, has_side_effects=True, vmem_limit_bytes=48 << 20),
    )(*(pltpu.with_memory_space_constraint(value, pltpu.HBM) for value in (gradient, members, w1, w2, w4, jnp.asarray(rows), jnp.asarray(small), jnp.asarray(spread))))
    return pl.pallas_call(
        output_kernel,
        name="output",
        out_shape=jax.ShapeDtypeStruct((LEV, 64, 256), F32),
        in_specs=[in_vmem],
        out_specs=any_space,
        scratch_shapes=[dma((2,))],
        compiler_params=pltpu.CompilerParams(vmem_limit_bytes=8 << 20),
    )(padded)


def solution(mesh):
    in_specs = (P(None, "gy", "gx"), P(None, None, "gy", "gx"))
    return jax.shard_map(
        functools.partial(shards, mesh.shape["gx"], mesh.shape["gy"]),
        mesh=mesh,
        in_specs=in_specs,
        out_specs=P(None, "gy", "gx"),
        check_vma=False,
    )
```

```python
import functools

import jax
import jax.numpy as jnp
import ml_dtypes
import numpy as np
from jax import lax
from jax.experimental import pallas as pl
from jax.experimental.pallas import tpu as pltpu
from jax.sharding import PartitionSpec as P

MESH = pl.DeviceIdType.MESH
F32, BF16 = jnp.float32, jnp.bfloat16
LEV, MEM = 16, 8
CHUNKS = 4
LAG = 3
DEFER = 3
MPAD = 40
APAD = 72

beta_raw = [(1.0 - (offset - 4) ** 2 / 25.0) ** 2 for offset in range(9)]
beta_taps = [value / sum(beta_raw) for value in beta_raw]
generations = ((1, 0.5), (2, 0.075), (4, 0.0125))
row_taps = [beta_taps[4 + k] / beta_taps[4] for k in range(5)]


def halves(matrix):
    hi = matrix.astype(ml_dtypes.bfloat16)
    lo = (matrix - hi.astype(np.float64)).astype(ml_dtypes.bfloat16)
    return np.stack([hi, lo])


def band(outputs):
    matrix = np.zeros((outputs + 8, outputs))
    for column in range(outputs):
        matrix[column : column + 9, column] = beta_taps
    return matrix


def column_filter(factor, weight, west_edge, east_edge):
    count = 128 // factor
    inside = np.ones(count + 8)
    if west_edge:
        inside[:4] = 0.0
    if east_edge:
        inside[-4:] = 0.0
    both = band(count + 8) @ (inside[:, None] * band(count))
    both = np.repeat(both, factor, axis=1) * (weight / (MEM - 1) * beta_taps[4] ** 2)
    result = np.zeros((256, 128 * factor))
    for part in range(factor):
        columns = slice(part * 128, part * 128 + 128)
        start = part * count
        result[start : start + count, columns] = both[8 : count + 8]
        result[128 + start : 136 + start, columns] = both[:8]
        result[136 + start : 144 + start, columns] = both[count + 8 :]
    return halves(result)


def row_filter(south_edge, north_edge):
    result = np.zeros((96, 128))
    start = 0
    for factor, _ in generations:
        count = 32 // factor
        inside = np.ones(count + 8)
        if south_edge:
            inside[:4] = 0.0
        if north_edge:
            inside[-4:] = 0.0
        both = band(count + 8) @ (inside[:, None] * band(count)) / beta_taps[4] ** 2
        for row in range(96):
            block = (row - 32) // factor + 8
            if 0 <= block < count + 16:
                result[row, start : start + count] = both[block]
        start += count
    return halves(result)


def constants():
    filters = []
    for factor, weight in generations:
        kinds = [column_filter(factor, weight, *edges) for edges in ((True, False), (False, False), (False, True))]
        filters.append(np.stack(kinds))
    filters[0] = np.concatenate([filters[0][:, 0], filters[0][:, 1]], axis=2)
    pairs = np.zeros((256, 128))
    reduce_columns = np.zeros((256, 128))
    for lane in range(128):
        pairs[2 * lane : 2 * lane + 2, lane] = 1.0
        reduce_columns[2 * lane, lane] = 1.0
        reduce_columns[2 * lane + 1, lane] = 0.5
        if lane:
            reduce_columns[2 * lane - 1, lane] = 0.5
    fours = np.zeros((2, 256, 128))
    for lane in range(256):
        fours[0, lane, lane // 4] = 1.0
        fours[1, lane, 64 + lane // 4] = 1.0
    border = np.zeros((256, 128))
    for chunk in range(CHUNKS):
        for j in range(32):
            border[2 * j, chunk * 32 + j] = 0.5
            border[2 * j + 1, chunk * 32 + j] = 0.25
            if j:
                border[2 * j - 1, chunk * 32 + j] = 0.25
    small = np.stack([pairs, reduce_columns, *fours, border]).astype(ml_dtypes.bfloat16)
    rows = np.stack([row_filter(*edges) for edges in ((True, False), (False, False), (False, True))])
    spread = np.zeros((256, 256))
    for lane in range(128):
        spread[lane, 2 * lane] = 1.0
        spread[lane, 2 * lane + 1] = 0.5
        spread[lane + 1, 2 * lane + 1] = 0.5
    return filters, rows, small, spread.astype(ml_dtypes.bfloat16)


def split(value):
    hi = value.astype(BF16)
    return hi, (value - hi.astype(F32)).astype(BF16)


def dot(a, b):
    return jnp.dot(a, b, preferred_element_type=F32)


def exact_dot(value, matrix):
    rows = value.shape[0]
    hi, lo = split(value)
    both = dot(jnp.concatenate([hi, lo], axis=0), matrix)
    return both[:rows] + both[rows:]


def full_dot(value, hi_matrix, lo_matrix):
    hi, lo = split(value)
    return dot(hi, hi_matrix) + dot(lo, hi_matrix) + dot(hi, lo_matrix)


def roll(value, shift):
    shift %= 128
    return value if shift == 0 else pltpu.roll(value, shift, 1)


def main_kernel(
    nx, ny,
    g_hbm, m_hbm, w1_hbm, w2_hbm, w4_hbm, wr_hbm, small_hbm, spread_hbm,
    out,
    gv, mv, w1, w2, w4, wr, small, spread, comb,
    ac, cz, px, p2x, p4x, y1, y2, y4, sp, rp, o2, o4,
    col_out, col_in, row_out, row_in, corner_in, m_out, m_in, c_out, c_in, c_next, dp, dp_in, add_rows, a1, a2, a4,
    end_row_in, end_col_out, end_col_in, end_corner_in,
    local_sem, wr_sem, s1, r1, sf, rf, ys, yr, xs, xr, s3, r3,
):
    gx, gy = lax.axis_index("gx"), lax.axis_index("gy")
    has_w, has_e = gx > 0, gx < nx - 1
    has_s, has_n = gy > 0, gy < ny - 1

    kind = 1 - (gx == 0).astype(jnp.int32) + (gx == nx - 1).astype(jnp.int32)
    g_copies = [
        pltpu.make_async_copy(
            g_hbm.at[:, :, pl.ds(side * 128, 128)], gv.at[side, :, pl.ds(0, 64), :], local_sem.at[side * 6]
        )
        for side in range(2)
    ]
    m_copy = pltpu.make_async_copy(m_hbm, mv.at[:, :, pl.ds(0, 32), :], local_sem.at[1])
    small_copy = pltpu.make_async_copy(small_hbm, small, local_sem.at[2])
    w1_copy = pltpu.make_async_copy(w1_hbm.at[kind], w1, local_sem.at[3])
    w2_copy = pltpu.make_async_copy(w2_hbm.at[kind], w2, local_sem.at[4])
    w4_copy = pltpu.make_async_copy(w4_hbm.at[kind], w4, local_sem.at[5])
    spread_copy = pltpu.make_async_copy(spread_hbm, spread, local_sem.at[7])
    row_kind = 1 - (gy == 0).astype(jnp.int32) + (gy == ny - 1).astype(jnp.int32)
    wr_copies = [
        pltpu.make_async_copy(
            wr_hbm.at[row_kind, part, pl.ds(tile * 32, 32), :],
            wr.at[part, tile, pl.ds(c * 32, 32), pl.ds(c * 128, 128)],
            wr_sem.at[part, tile, c],
        )
        for part in range(2) for tile in range(3) for c in range(CHUNKS)
    ]
    for copy in (g_copies[1], g_copies[0], small_copy, m_copy, *wr_copies, w1_copy, w2_copy, w4_copy, spread_copy):
        copy.start()

    barrier = pltpu.get_barrier_semaphore()
    around = [
        (has_w, -1, 0), (has_e, 1, 0), (has_s, 0, -1), (has_n, 0, 1),
        (has_w & has_s, -1, -1), (has_e & has_n, 1, 1),
    ]

    def at(dx, dy):
        return {"gx": gx + dx, "gy": gy + dy}

    for there, dx, dy in around:
        @pl.when(there)
        def _(dx=dx, dy=dy):
            pl.semaphore_signal(barrier, inc=1, device_id=at(dx, dy), device_id_type=MESH)

    for part in range(2):
        for tile in range(3):
            for c in range(CHUNKS):
                for other in range(CHUNKS):
                    if other != c:
                        wr[part, tile, pl.ds(c * 32, 32), pl.ds(other * 128, 128)] = jnp.zeros((32, 128), BF16)

    @pl.when(jnp.logical_not(has_s))
    def _():
        px[:, pl.ds(0, 8)] = jnp.zeros((CHUNKS, 8, 32, 128), F32)
        p2x[:, pl.ds(0, 4)] = jnp.zeros((CHUNKS, 4, 16, 128), F32)
        p4x[:, pl.ds(0, 4)] = jnp.zeros((CHUNKS, 4, 8, 128), F32)
        row_in[...] = jnp.zeros((2, 16, 128), F32)
        dp_in[0] = jnp.zeros((32, 128), F32)

    @pl.when(jnp.logical_not(has_n))
    def _():
        px[:, pl.ds(40, 8)] = jnp.zeros((CHUNKS, 8, 32, 128), F32)
        p2x[:, pl.ds(28, 4)] = jnp.zeros((CHUNKS, 4, 16, 128), F32)
        p4x[:, pl.ds(20, 4)] = jnp.zeros((CHUNKS, 4, 8, 128), F32)
        end_row_in[...] = jnp.zeros((16, 128), F32)
        dp_in[1] = jnp.zeros((32, 128), F32)

    @pl.when(jnp.logical_not(has_w))
    def _():
        rp[0] = jnp.zeros((CHUNKS, 112, 128), F32)
        col_in[...] = jnp.zeros((16, 128), F32)

    @pl.when(jnp.logical_not(has_e))
    def _():
        rp[1] = jnp.zeros((CHUNKS, 112, 128), F32)
        end_col_in[...] = jnp.zeros((16, 128), F32)

    @pl.when(jnp.logical_not(has_w & has_s))
    def _():
        corner_in[...] = jnp.zeros((16, 128), F32)

    @pl.when(jnp.logical_not(has_e & has_n))
    def _():
        end_corner_in[...] = jnp.zeros((16, 128), F32)

    def remote(src, dst, send, recv, dx, dy):
        return pltpu.make_async_remote_copy(
            src_ref=src, dst_ref=dst, send_sem=send, recv_sem=recv, device_id=at(dx, dy), device_id_type=MESH
        )

    col_copy = remote(col_out, col_in, s1.at[0], r1.at[0], 1, 0)
    row_copy = remote(row_out, row_in, s1.at[1], r1.at[1], 0, 1)
    corner_copy = remote(col_out, corner_in, s1.at[2], r1.at[2], 1, 1)
    end_row_copy = remote(comb.at[0], end_row_in, s3.at[0], r3.at[0], 0, -1)
    end_col_copy = remote(end_col_out, end_col_in, s3.at[1], r3.at[1], -1, 0)
    end_corner_copy = remote(comb.at[0], end_corner_in, s3.at[2], r3.at[2], -1, -1)

    def y_copies(c, direction, pieces=slice(0, 4)):
        if direction == 0:
            places = ((px, 32, 0, 8), (p2x, 16, 0, 4), (p4x, 8, 0, 4))
            dy = 1
        else:
            places = ((px, 9, 41, 7), (p2x, 12, 28, 4), (p4x, 12, 20, 4))
            dy = -1
        ends = [(ref.at[c, pl.ds(src, n)], ref.at[c, pl.ds(dst, n)]) for ref, src, dst, n in places]
        if direction == 1:
            ends.append((m_out.at[c], m_in.at[c]))
        return [
            remote(src, dst, ys.at[direction, c, i], yr.at[direction, c, i], 0, dy)
            for i, (src, dst) in list(enumerate(ends))[pieces]
        ]

    dp_north = remote(dp, dp_in.at[0], sf.at[2], rf.at[2], 0, 1)
    dp_south = remote(dp, dp_in.at[1], sf.at[3], rf.at[3], 0, -1)
    first_coarse = remote(c_out, c_in, sf.at[1], rf.at[1], 0, -1)

    def x_copy(c, direction):
        if direction == 0:
            return remote(sp.at[0, c], rp.at[0, c], xs.at[0, c], xr.at[0, c], 1, 0)
        return remote(sp.at[1, c], rp.at[1, c], xs.at[1, c], xr.at[1, c], -1, 0)

    lane = lax.broadcasted_iota(jnp.int32, (8, 128), 1)
    first_lane = lane == 0

    g_copies[1].wait()
    g0, g1 = gv.at[0].reshape(LEV * APAD, 128), gv.at[1].reshape(LEV * APAD, 128)

    def gradient_row(half, y, h):
        return half[pl.ds(h * 8 * APAD + y, 8, stride=APAD), :]

    for h in range(2):
        parts = []
        for quarter in range(2):
            packed = jnp.zeros((8, 128), F32)
            for y in range(quarter * 32, quarter * 32 + 32):
                packed = jnp.where(lane == y, roll(gradient_row(g1, y, h), y + 1), packed)
            parts.append(packed)
        col_out[pl.ds(h * 8, 8), :] = jnp.where(lane < 32, parts[0], parts[1])
    g_copies[0].wait()
    for h in range(2):
        row_out[0, pl.ds(h * 8, 8), :] = gradient_row(g0, 63, h)
        row_out[1, pl.ds(h * 8, 8), :] = gradient_row(g1, 63, h)

    small_copy.wait()
    for block in range(4):
        levels = pl.ds(block * 4, 4)
        value = jnp.concatenate(
            [gv[side, levels, pl.ds(0, 64), :].reshape(256, 128) for side in range(2)], axis=1
        )
        ac[levels, pl.ds(0, 64), :] = exact_dot(value, small[1]).reshape(4, 64, 128)
    ar = ac.reshape(LEV * APAD, 128)

    def across_row(y, h):
        return ar[pl.ds(h * 8 * APAD + y, 8, stride=APAD), :]

    for h in range(2):
        c_out[pl.ds(h * 8, 8), :] = across_row(0, h) + 0.5 * across_row(1, h)

    def reduce_rows(j, carry):
        odd_rows = []
        for h in range(2):
            odd = across_row(2 * j + 1, h)
            cz[j, pl.ds(h * 8, 8), :] = across_row(2 * j, h) + 0.5 * (odd + carry[h])
            odd_rows.append(odd)
        return tuple(odd_rows)

    lax.fori_loop(1, 32, reduce_rows, tuple(across_row(1, h) for h in range(2)))
    mr = mv.reshape(MEM * LEV * MPAD, 128)

    def member(c, m2, h, y):
        return mr[pl.ds(((2 * c + m2) * LEV + h * 8) * MPAD + y, 8, stride=MPAD), :]

    m_copy.wait()

    for c in range(CHUNKS):
        for m2 in range(2):
            for h in range(2):
                m_out[c, pl.ds(m2 * 16 + h * 8, 8), :] = member(c, m2, h, 0)

    def half_blocks(places):
        rows = []
        for c, k in places:
            pair = px[c, 2 * k - 8] + px[c, 2 * k - 7]
            for m2 in range(2):
                rows.append(jnp.concatenate([pair[m2 * 16 : m2 * 16 + 8], pair[m2 * 16 + 8 : m2 * 16 + 16]], axis=1))
        value = exact_dot(jnp.concatenate(rows, axis=0), small[0])
        for i, (c, k) in enumerate(places):
            p2x[c, k] = value[i * 16 : i * 16 + 16]

    def quarter_blocks(places):
        rows = []
        for c, k in places:
            pair = p2x[c, 2 * k - 8] + p2x[c, 2 * k - 7]
            rows.append(jnp.concatenate([pair[:8], pair[8:]], axis=1))
        value = exact_dot(jnp.concatenate(rows, axis=0), small[0])
        for i, (c, k) in enumerate(places):
            p4x[c, k] = value[i * 8 : i * 8 + 8]

    def quarter_blocks_of_rows(places):
        rows = [[], []]
        for c, k, row in places:
            four = (px[c, row] + px[c, row + 1]) + (px[c, row + 2] + px[c, row + 3])
            for m2 in range(2):
                rows[m2].append(jnp.concatenate([four[m2 * 16 : m2 * 16 + 8], four[m2 * 16 + 8 : m2 * 16 + 16]], axis=1))
        value = sum(exact_dot(jnp.concatenate(rows[m2], axis=0), small[2 + m2]) for m2 in range(2))
        for i, (c, k, _) in enumerate(places):
            p4x[c, k] = value[i * 8 : i * 8 + 8]

    def product_row(c, y):
        for m2 in range(2):
            for h in range(2):
                px[c, 8 + y, pl.ds(m2 * 16 + h * 8, 8), :] = member(c, m2, h, y) * cz[y, pl.ds(h * 8, 8), :]

    def start_rows(c, north, south):
        @pl.when(has_n)
        def _():
            for copy in y_copies(c, 0, north):
                copy.start()

        @pl.when(has_s)
        def _():
            for copy in y_copies(c, 1, south):
                copy.start()

    everything, nothing = slice(0, 4), slice(0, 0)

    def later_rows(c):
        def row(y, carry):
            product_row(c, y)
            return carry

        lax.fori_loop(1, 32, row, 0, unroll=4)

    def first_columns():
        @pl.when(has_w)
        def _():
            col_copy.wait_recv()

        coarse = exact_dot(jnp.concatenate([col_in[...], jnp.zeros((16, 128), F32)], axis=1), small[4])

        for m2 in range(2):
            for h in range(2):
                columns = []
                for c in range(CHUNKS):
                    column = roll(member(c, m2, h, 0), c * 32)
                    for y in range(1, 32):
                        place = c * 32 + y
                        column = jnp.where(lane == place, roll(member(c, m2, h, y), place), column)
                    columns.append(column)
                column = columns[0]
                for c in range(1, CHUNKS):
                    column = jnp.where(lane >= c * 32, columns[c], column)
                dp[pl.ds(m2 * 16 + h * 8, 8), :] = column * coarse[h * 8 : h * 8 + 8]

        @pl.when(has_n)
        def _():
            dp_north.start()

        @pl.when(has_s)
        def _():
            dp_south.start()

    def own_rows(c):
        later_rows(c)
        half_blocks([(c, k) for k in range(12, 24)])
        quarter_blocks([(c, k) for k in range(12, 16)])

    def without_first_row(c, carry):
        own_rows(c)
        start_rows(c, slice(0, 2), everything)
        return carry

    def first_row(c, carry):
        product_row(c, 0)
        half_blocks([(c, k) for k in range(8, 12)])
        quarter_blocks([(c, k) for k in range(8, 12)])
        start_rows(c, slice(2, 3), nothing)
        return carry

    def whole(c, carry):
        later_rows(c)
        product_row(c, 0)
        half_blocks([(c, k) for k in range(8, 24)])
        quarter_blocks([(c, k) for k in range(8, 16)])
        start_rows(c, everything, everything)
        return carry

    def first_coarse_row():
        @pl.when(has_s)
        def _():
            row_copy.wait_recv()

        @pl.when(has_w & has_s)
        def _():
            corner_copy.wait_recv()

        before = exact_dot(jnp.concatenate([row_in[0], row_in[1]], axis=1), small[1])
        for h in range(2):
            corner = jnp.where(first_lane, 0.5 * roll(corner_in[pl.ds(h * 8, 8), :], -63), 0.0)
            cz[0, pl.ds(h * 8, 8), :] = c_out[pl.ds(h * 8, 8), :] + 0.5 * (before[h * 8 : h * 8 + 8] + corner)

    far = (gy % 8 == 0) & has_s
    own_rows(0)
    pl.semaphore_wait(barrier, sum(there.astype(jnp.int32) for there, _, _ in around))

    @pl.when(has_e)
    def _():
        col_copy.start()

    @pl.when(has_n)
    def _():
        row_copy.start()

    @pl.when(has_e & has_n)
    def _():
        corner_copy.start()

    @pl.when(has_s)
    def _():
        first_coarse.start()

    start_rows(0, slice(0, 2), everything)

    far_west = (gx % 4 == 0) & has_w
    near_south = gy % 2 == 1
    second = 1 + far_west.astype(jnp.int32)

    @pl.when(far_west)
    def _():
        without_first_row(1, 0)

    @pl.when(near_south)
    def _():
        first_coarse_row()
        first_row(0, 0)

    first_columns()

    @pl.when(far)
    def _():
        lax.fori_loop(second, CHUNKS, without_first_row, 0)

    @pl.when(jnp.logical_not(near_south))
    def _():
        first_coarse_row()
        first_row(0, 0)

    @pl.when(far)
    def _():
        lax.fori_loop(1, CHUNKS, first_row, 0)

    @pl.when(jnp.logical_not(far) & far_west)
    def _():
        first_row(1, 0)

    @pl.when(jnp.logical_not(far))
    def _():
        lax.fori_loop(second, CHUNKS, whole, 0)

    @pl.when(has_n)
    def _():
        first_coarse.wait_recv()
        for h in range(2):
            corner = jnp.where(first_lane, 0.5 * roll(col_in[pl.ds(h * 8, 8), :], -63), 0.0)
            c_next[pl.ds(h * 8, 8), :] = c_in[pl.ds(h * 8, 8), :] + 0.5 * (across_row(63, h) + corner)

    @pl.when(has_s)
    def _():
        dp_north.wait_recv()

    @pl.when(has_n)
    def _():
        dp_south.wait_recv()

    for copy in wr_copies:
        copy.wait()
    columns = jnp.concatenate([dp_in[0], dp[...], dp_in[1]], axis=1)
    hi, lo = split(columns)
    weights = [wr[part].reshape(384, 512) for part in range(2)]
    value = dot(jnp.concatenate([hi, lo], axis=0), weights[0])
    value = value[:32] + value[32:] + dot(hi, weights[1])
    for c in range(CHUNKS):
        add_rows[c] = value[:, c * 128 : c * 128 + 128]

    def spread_additions(c):
        for target, rows, width, first in ((a1, 32, 128, 0), (a2, 16, 64, 32), (a4, 8, 32, 48)):
            parts = 128 // width
            for f in range(4 // parts):
                fields = [add_rows[c, pl.ds((f * parts + part) * 8, 8), :] for part in range(parts)]
                for y in range(rows):
                    add = jnp.zeros((8, 128), F32)
                    for part in range(parts):
                        add = jnp.where(lane == part * width, roll(fields[part], part * width - first - y), add)
                    target[c, y, pl.ds(f * 8, 8), :] = add

    low = jnp.where(has_s, 1.0, 0.0).astype(F32)
    high = jnp.where(has_n, 1.0, 0.0).astype(F32)

    def one_pass(window):
        total = window[4]
        for k in range(1, 5):
            total = total + row_taps[k] * (window[4 - k] + window[4 + k])
        return total

    def filter_rows(c, source, target, rows, fields, width, base, additions):
        group = width // 8
        place = (lane % width) // 8

        def column(f, carry):
            at_f = pl.ds(f * 8, 8)
            window, passed = [], []
            east = west = None
            for row in range(rows):
                window.append(source[c, row, at_f, :])
                if row < 8:
                    continue
                once = one_pass(window[-9:])
                if row - 8 < 4:
                    once = once * low
                if row >= rows - 4:
                    once = once * high
                passed.append(once)
                if len(passed) < 9:
                    continue
                twice = one_pass(passed[-9:])
                y = row - 16
                twice = twice + additions[c, y, at_f, :]
                target[c, y, at_f, :] = twice
                r = y % group
                to_west, to_east = roll(twice, 8 * r), roll(twice, 8 * r + 8 - width)
                if r == 0:
                    west, east = to_west, to_east
                else:
                    west, east = jnp.where(place == r, to_west, west), jnp.where(place == r, to_east, east)
                if r == group - 1:
                    start = base + (y // group) * fields + f * 8
                    sp[0, c, pl.ds(start, 8), :] = east
                    sp[1, c, pl.ds(start, 8), :] = west
            return carry

        for f in range(fields // 8):
            column(f, 0)

    outer = (gy < 2) | (gy >= ny - 2)
    defer_e = outer & has_e & (gx == nx // 2 - 1)
    defer_w = outer & has_w & (gx == nx // 2)

    def rows_stage(c):
        spread_additions(c)

        @pl.when(has_s)
        def _():
            for copy in y_copies(c, 0):
                copy.wait_recv()

        @pl.when(has_n)
        def _():
            for copy in y_copies(c, 1):
                copy.wait_recv()

        @pl.when(has_n)
        def _():
            for m2 in range(2):
                for h in range(2):
                    at_f = pl.ds(m2 * 16 + h * 8, 8)
                    px[c, 40, at_f, :] = m_in[c, at_f, :] * c_next[pl.ds(h * 8, 8), :]

        quarter_blocks_of_rows([(c, 6, 0), (c, 7, 4), (c, 16, 40), (c, 17, 44)])
        half_blocks([(c, k) for k in (4, 5, 6, 7, 24, 25, 26, 27)])
        quarter_blocks([(c, k) for k in (4, 5, 18, 19)])
        filter_rows(c, px, y1, 48, 32, 128, 0, a1)
        filter_rows(c, p2x, y2, 32, 16, 64, 64, a2)
        filter_rows(c, p4x, y4, 24, 8, 32, 96, a4)

        @pl.when(has_e & (jnp.logical_not(defer_e) | (c > DEFER)))
        def _():
            x_copy(c, 0).start()

        @pl.when(has_w & (jnp.logical_not(defer_w) | (c > DEFER)))
        def _():
            x_copy(c, 1).start()

        @pl.when(defer_e & (c == DEFER))
        def _():
            for chunk in range(DEFER + 1):
                x_copy(chunk, 0).start()

        @pl.when(defer_w & (c == DEFER))
        def _():
            for chunk in range(DEFER + 1):
                x_copy(chunk, 1).start()

    comb[...] = jnp.zeros((32, 16, 128), F32)
    w1_copy.wait()
    w2_copy.wait()
    w4_copy.wait()

    def halo(c, start, fields, r, width):
        west, east = rp[0, c, pl.ds(start, fields), :], rp[1, c, pl.ds(start, fields), :]
        take_west = lax.broadcasted_iota(jnp.int32, (fields, 128), 1) % width < 8
        return jnp.where(take_west, roll(west, -8 * r), roll(east, 8 - 8 * r))

    def columns_stage(c):
        @pl.when(has_w)
        def _():
            x_copy(c, 0).wait_recv()

        @pl.when(has_e)
        def _():
            x_copy(c, 1).wait_recv()

        sides = [halo(c, 96 + (q // 4) * 8, 8, q % 4, 32) for q in range(8)]
        value = jnp.concatenate([y4[c].reshape(64, 128), jnp.concatenate(sides, axis=0)], axis=1)
        o4[...] = full_dot(value, w4[0], w4[1])
        sides = [halo(c, 64 + (q // 8) * 16, 16, q % 8, 64) for q in range(16)]
        value = jnp.concatenate([y2[c].reshape(256, 128), jnp.concatenate(sides, axis=0)], axis=1)
        o2[...] = full_dot(value, w2[0], w2[1])

        def block(b, carry):
            @pl.when((b == 1) & (c == CHUNKS - 1) & has_s)
            def _():
                end_row_copy.start()

            @pl.when((b == 1) & (c == CHUNKS - 1) & has_w & has_s)
            def _():
                end_corner_copy.start()

            for part in range(2):
                first = b * 16 + part * 8
                start = pl.multiple_of(b * 32, 32)
                sides = [halo(c, start, 32, part * 8 + r, 128) for r in range(8)]
                rows = y1[c, pl.ds(first, 8)].reshape(256, 128)
                both = exact_dot(jnp.concatenate([rows, jnp.concatenate(sides, axis=0)], axis=1), w1[...])
                value = both[:, :128] + both[:, 128:]
                for r in range(8):
                    y = first + r
                    at2 = pl.multiple_of((b * 8 + part * 4 + r // 2) * 16, 16)
                    at4 = pl.multiple_of((b * 4 + part * 2 + r // 4) * 8, 8)
                    for h in range(2):
                        total = comb[y, pl.ds(h * 8, 8), :]
                        for m2 in range(2):
                            begin = r * 32 + m2 * 16 + h * 8
                            local = value[begin : begin + 8]
                            local = local + o2[pl.ds(at2 + m2 * 8, 8), pl.ds(h * 128, 128)]
                            local = local + o4[pl.ds(at4, 8), pl.ds((m2 * 2 + h) * 128, 128)]
                            total = total + member(c, m2, h, y) * local
                        comb[y, pl.ds(h * 8, 8), :] = total
            return carry

        lax.fori_loop(0, 2, block, 0)

    def stages(step, carry):
        @pl.when(step < CHUNKS)
        def _():
            rows_stage(step)

        @pl.when(step >= LAG)
        def _():
            columns_stage(step - LAG)

        return carry

    lax.fori_loop(0, CHUNKS + LAG, stages, 0)

    for h in range(2):
        packed = comb[0, pl.ds(h * 8, 8), :]
        for y in range(1, 32):
            packed = jnp.where(lane == y, roll(comb[y, pl.ds(h * 8, 8), :], y), packed)
        end_col_out[pl.ds(h * 8, 8), :] = packed

    @pl.when(has_w)
    def _():
        end_col_copy.start()

    def send_waits(c, carry):
        @pl.when(has_n)
        def _():
            for copy in y_copies(c, 0):
                copy.wait_send()

        @pl.when(has_s)
        def _():
            for copy in y_copies(c, 1):
                copy.wait_send()

        @pl.when(has_e)
        def _():
            x_copy(c, 0).wait_send()

        @pl.when(has_w)
        def _():
            x_copy(c, 1).wait_send()

        return carry

    spread_copy.wait()
    flats = [out.at[side].reshape(LEV * APAD, 128) for side in range(2)]

    def store_row(y, side, h, value):
        flats[side][pl.ds(h * 8 * APAD + y, 8, stride=APAD), :] = value

    def row_of(y, h):
        return flats[1][pl.ds(h * 8 * APAD + y, 8, stride=APAD), :]

    for block in range(4):
        rows = []
        for j in range(block * 8, block * 8 + 8):
            rows += [comb[j], 0.5 * (comb[j] + comb[j + 1])] if j < 31 else [comb[j]]
        value = exact_dot(jnp.concatenate(rows, axis=0), spread[pl.ds(0, 128), :])
        for k in range(len(rows)):
            for h in range(2):
                for side in range(2):
                    begin = k * 16 + h * 8
                    store_row(block * 16 + k, side, h, value[begin : begin + 8, side * 128 : side * 128 + 128])

    lax.fori_loop(0, CHUNKS, send_waits, 0)

    @pl.when(has_e)
    def _():
        col_copy.wait_send()
        end_col_copy.wait_recv()

    @pl.when(has_n)
    def _():
        row_copy.wait_send()
        dp_north.wait_send()
        end_row_copy.wait_recv()

    @pl.when(has_e & has_n)
    def _():
        corner_copy.wait_send()
        end_corner_copy.wait_recv()

    for h in range(2):
        levels = pl.ds(h * 8, 8)
        edge = jnp.where(lane == 32, roll(end_corner_in[levels, :], 32), end_col_in[levels, :])
        half_edge = 0.5 * (edge + roll(edge, -1))
        for y in range(63):
            add = roll((half_edge, edge)[y % 2 == 0], 127 - y // 2)
            store_row(y, 1, h, row_of(y, h) + jnp.where(lane == 127, 0.5 * add, 0.0))
        last = 0.5 * (comb[31, levels, :] + end_row_in[levels, :])
        value = exact_dot(jnp.concatenate([last, roll(half_edge, -31)], axis=1), spread[...])
        for side in range(2):
            store_row(63, side, h, value[:, side * 128 : side * 128 + 128])

    @pl.when(has_s)
    def _():
        end_row_copy.wait_send()
        first_coarse.wait_send()
        dp_south.wait_send()

    @pl.when(has_w)
    def _():
        end_col_copy.wait_send()

    @pl.when(has_w & has_s)
    def _():
        end_corner_copy.wait_send()


def output_kernel(padded, out_hbm, sem):
    copies = [
        pltpu.make_async_copy(
            padded.at[side, :, pl.ds(0, 64), :], out_hbm.at[:, :, pl.ds(side * 128, 128)], sem.at[side]
        )
        for side in range(2)
    ]
    for copy in copies:
        copy.start()
    for copy in copies:
        copy.wait()


def shards(nx, ny, gradient, members):
    filters, rows, small, spread = constants()
    w1, w2, w4 = (jnp.asarray(value) for value in filters)
    any_space = pl.BlockSpec(memory_space=pltpu.HBM)
    in_vmem = pl.BlockSpec(memory_space=pltpu.VMEM)
    dma = pltpu.SemaphoreType.DMA

    def vmem(*shape, dtype=F32):
        return pltpu.VMEM(shape, dtype)

    padded = pl.pallas_call(
        functools.partial(main_kernel, nx, ny),
        name="localise",
        out_shape=jax.ShapeDtypeStruct((2, LEV, APAD, 128), F32),
        in_specs=[any_space] * 8,
        out_specs=in_vmem,
        scratch_shapes=[
            vmem(2, LEV, APAD, 128),
            vmem(MEM, LEV, MPAD, 128),
            vmem(256, 256, dtype=BF16),
            vmem(2, 256, 256, dtype=BF16),
            vmem(2, 256, 512, dtype=BF16),
            vmem(2, 3, 128, 512, dtype=BF16),
            vmem(5, 256, 128, dtype=BF16),
            vmem(256, 256, dtype=BF16),
            vmem(32, 16, 128),
            vmem(LEV, APAD, 128),
            vmem(32, 16, 128),
            vmem(CHUNKS, 48, 32, 128),
            vmem(CHUNKS, 32, 16, 128),
            vmem(CHUNKS, 24, 8, 128),
            vmem(CHUNKS, 32, 32, 128),
            vmem(CHUNKS, 16, 16, 128),
            vmem(CHUNKS, 8, 8, 128),
            vmem(2, CHUNKS, 112, 128),
            vmem(2, CHUNKS, 112, 128),
            vmem(256, 256),
            vmem(64, 512),
            vmem(16, 128),
            vmem(16, 128),
            vmem(2, 16, 128),
            vmem(2, 16, 128),
            vmem(16, 128),
            vmem(CHUNKS, 32, 128),
            vmem(CHUNKS, 32, 128),
            vmem(16, 128),
            vmem(16, 128),
            vmem(16, 128),
            vmem(32, 128),
            vmem(2, 32, 128),
            vmem(CHUNKS, 32, 128),
            vmem(CHUNKS, 32, 32, 128),
            vmem(CHUNKS, 16, 16, 128),
            vmem(CHUNKS, 8, 8, 128),
            vmem(16, 128),
            vmem(16, 128),
            vmem(16, 128),
            vmem(16, 128),
            dma((8,)),
            dma((2, 3, CHUNKS)),
            dma((3,)),
            dma((3,)),
            dma((4,)),
            dma((4,)),
            dma((2, CHUNKS, 4)),
            dma((2, CHUNKS, 4)),
            dma((2, CHUNKS)),
            dma((2, CHUNKS)),
            dma((3,)),
            dma((3,)),
        ],
        compiler_params=pltpu.CompilerParams(collective_id=0, has_side_effects=True, vmem_limit_bytes=48 << 20),
    )(*(pltpu.with_memory_space_constraint(value, pltpu.HBM) for value in (gradient, members, w1, w2, w4, jnp.asarray(rows), jnp.asarray(small), jnp.asarray(spread))))
    return pl.pallas_call(
        output_kernel,
        name="output",
        out_shape=jax.ShapeDtypeStruct((LEV, 64, 256), F32),
        in_specs=[in_vmem],
        out_specs=any_space,
        scratch_shapes=[dma((2,))],
        compiler_params=pltpu.CompilerParams(vmem_limit_bytes=8 << 20),
    )(padded)


def solution(mesh):
    in_specs = (P(None, "gy", "gx"), P(None, None, "gy", "gx"))
    return jax.shard_map(
        functools.partial(shards, mesh.shape["gx"], mesh.shape["gy"]),
        mesh=mesh,
        in_specs=in_specs,
        out_specs=P(None, "gy", "gx"),
        check_vma=False,
    )
```

```python
import functools

import jax
import jax.numpy as jnp
import ml_dtypes
import numpy as np
from jax import lax
from jax.experimental import pallas as pl
from jax.experimental.pallas import tpu as pltpu
from jax.sharding import PartitionSpec as P

MESH = pl.DeviceIdType.MESH
F32, BF16 = jnp.float32, jnp.bfloat16
LEV, MEM = 16, 8
CHUNKS = 4
LAG = 3
DEFER = 2
MPAD = 40
APAD = 72

beta_raw = [(1.0 - (offset - 4) ** 2 / 25.0) ** 2 for offset in range(9)]
beta_taps = [value / sum(beta_raw) for value in beta_raw]
generations = ((1, 0.5), (2, 0.075), (4, 0.0125))
row_taps = [beta_taps[4 + k] / beta_taps[4] for k in range(5)]


def halves(matrix):
    hi = matrix.astype(ml_dtypes.bfloat16)
    lo = (matrix - hi.astype(np.float64)).astype(ml_dtypes.bfloat16)
    return np.stack([hi, lo])


def band(outputs):
    matrix = np.zeros((outputs + 8, outputs))
    for column in range(outputs):
        matrix[column : column + 9, column] = beta_taps
    return matrix


def column_filter(factor, weight, west_edge, east_edge):
    count = 128 // factor
    inside = np.ones(count + 8)
    if west_edge:
        inside[:4] = 0.0
    if east_edge:
        inside[-4:] = 0.0
    both = band(count + 8) @ (inside[:, None] * band(count))
    both = np.repeat(both, factor, axis=1) * (weight / (MEM - 1) * beta_taps[4] ** 2)
    result = np.zeros((256, 128 * factor))
    for part in range(factor):
        columns = slice(part * 128, part * 128 + 128)
        start = part * count
        result[start : start + count, columns] = both[8 : count + 8]
        result[128 + start : 136 + start, columns] = both[:8]
        result[136 + start : 144 + start, columns] = both[count + 8 :]
    return halves(result)


def row_filter(south_edge, north_edge):
    result = np.zeros((96, 128))
    start = 0
    for factor, _ in generations:
        count = 32 // factor
        inside = np.ones(count + 8)
        if south_edge:
            inside[:4] = 0.0
        if north_edge:
            inside[-4:] = 0.0
        both = band(count + 8) @ (inside[:, None] * band(count)) / beta_taps[4] ** 2
        for row in range(96):
            block = (row - 32) // factor + 8
            if 0 <= block < count + 16:
                result[row, start : start + count] = both[block]
        start += count
    return halves(result)


def constants():
    filters = []
    for factor, weight in generations:
        kinds = [column_filter(factor, weight, *edges) for edges in ((True, False), (False, False), (False, True))]
        filters.append(np.stack(kinds))
    filters[0] = np.concatenate([filters[0][:, 0], filters[0][:, 1]], axis=2)
    pairs = np.zeros((256, 128))
    reduce_columns = np.zeros((256, 128))
    for lane in range(128):
        pairs[2 * lane : 2 * lane + 2, lane] = 1.0
        reduce_columns[2 * lane, lane] = 1.0
        reduce_columns[2 * lane + 1, lane] = 0.5
        if lane:
            reduce_columns[2 * lane - 1, lane] = 0.5
    fours = np.zeros((2, 256, 128))
    for lane in range(256):
        fours[0, lane, lane // 4] = 1.0
        fours[1, lane, 64 + lane // 4] = 1.0
    border = np.zeros((256, 128))
    for chunk in range(CHUNKS):
        for j in range(32):
            border[2 * j, chunk * 32 + j] = 0.5
            border[2 * j + 1, chunk * 32 + j] = 0.25
            if j:
                border[2 * j - 1, chunk * 32 + j] = 0.25
    small = np.stack([pairs, reduce_columns, *fours, border]).astype(ml_dtypes.bfloat16)
    rows = np.stack([row_filter(*edges) for edges in ((True, False), (False, False), (False, True))])
    spread = np.zeros((256, 256))
    for lane in range(128):
        spread[lane, 2 * lane] = 1.0
        spread[lane, 2 * lane + 1] = 0.5
        spread[lane + 1, 2 * lane + 1] = 0.5
    return filters, rows, small, spread.astype(ml_dtypes.bfloat16)


def split(value):
    hi = value.astype(BF16)
    return hi, (value - hi.astype(F32)).astype(BF16)


def dot(a, b):
    return jnp.dot(a, b, preferred_element_type=F32)


def exact_dot(value, matrix):
    rows = value.shape[0]
    hi, lo = split(value)
    both = dot(jnp.concatenate([hi, lo], axis=0), matrix)
    return both[:rows] + both[rows:]


def full_dot(value, hi_matrix, lo_matrix):
    hi, lo = split(value)
    return dot(hi, hi_matrix) + dot(lo, hi_matrix) + dot(hi, lo_matrix)


def roll(value, shift):
    shift %= 128
    return value if shift == 0 else pltpu.roll(value, shift, 1)


def main_kernel(
    nx, ny,
    g_hbm, m_hbm, w1_hbm, w2_hbm, w4_hbm, wr_hbm, small_hbm, spread_hbm,
    out,
    gv, mv, w1, w2, w4, wr, small, spread, comb,
    ac, cz, px, p2x, p4x, y1, y2, y4, sp, rp, o2, o4,
    col_out, col_in, row_out, row_in, corner_in, m_out, m_in, c_out, c_in, c_next, dp, dp_in, add_rows, a1, a2, a4,
    end_row_in, end_col_out, end_col_in, end_corner_in,
    local_sem, wr_sem, s1, r1, sf, rf, ys, yr, xs, xr, s3, r3,
):
    gx, gy = lax.axis_index("gx"), lax.axis_index("gy")
    has_w, has_e = gx > 0, gx < nx - 1
    has_s, has_n = gy > 0, gy < ny - 1

    kind = 1 - (gx == 0).astype(jnp.int32) + (gx == nx - 1).astype(jnp.int32)
    g_copies = [
        pltpu.make_async_copy(
            g_hbm.at[:, :, pl.ds(side * 128, 128)], gv.at[side, :, pl.ds(0, 64), :], local_sem.at[side * 6]
        )
        for side in range(2)
    ]
    m_copy = pltpu.make_async_copy(m_hbm, mv.at[:, :, pl.ds(0, 32), :], local_sem.at[1])
    small_copy = pltpu.make_async_copy(small_hbm, small, local_sem.at[2])
    w1_copy = pltpu.make_async_copy(w1_hbm.at[kind], w1, local_sem.at[3])
    w2_copy = pltpu.make_async_copy(w2_hbm.at[kind], w2, local_sem.at[4])
    w4_copy = pltpu.make_async_copy(w4_hbm.at[kind], w4, local_sem.at[5])
    spread_copy = pltpu.make_async_copy(spread_hbm, spread, local_sem.at[7])
    row_kind = 1 - (gy == 0).astype(jnp.int32) + (gy == ny - 1).astype(jnp.int32)
    wr_copies = [
        pltpu.make_async_copy(
            wr_hbm.at[row_kind, part, pl.ds(tile * 32, 32), :],
            wr.at[part, tile, pl.ds(c * 32, 32), pl.ds(c * 128, 128)],
            wr_sem.at[part, tile, c],
        )
        for part in range(2) for tile in range(3) for c in range(CHUNKS)
    ]
    for copy in (g_copies[1], g_copies[0], small_copy, m_copy, *wr_copies, w1_copy, w2_copy, w4_copy, spread_copy):
        copy.start()

    barrier = pltpu.get_barrier_semaphore()
    around = [
        (has_w, -1, 0), (has_e, 1, 0), (has_s, 0, -1), (has_n, 0, 1),
        (has_w & has_s, -1, -1), (has_e & has_n, 1, 1),
    ]

    def at(dx, dy):
        return {"gx": gx + dx, "gy": gy + dy}

    for there, dx, dy in around:
        @pl.when(there)
        def _(dx=dx, dy=dy):
            pl.semaphore_signal(barrier, inc=1, device_id=at(dx, dy), device_id_type=MESH)

    for part in range(2):
        for tile in range(3):
            for c in range(CHUNKS):
                for other in range(CHUNKS):
                    if other != c:
                        wr[part, tile, pl.ds(c * 32, 32), pl.ds(other * 128, 128)] = jnp.zeros((32, 128), BF16)

    @pl.when(jnp.logical_not(has_s))
    def _():
        px[:, pl.ds(0, 8)] = jnp.zeros((CHUNKS, 8, 32, 128), F32)
        p2x[:, pl.ds(0, 4)] = jnp.zeros((CHUNKS, 4, 16, 128), F32)
        p4x[:, pl.ds(0, 4)] = jnp.zeros((CHUNKS, 4, 8, 128), F32)
        row_in[...] = jnp.zeros((2, 16, 128), F32)
        dp_in[0] = jnp.zeros((32, 128), F32)

    @pl.when(jnp.logical_not(has_n))
    def _():
        px[:, pl.ds(40, 8)] = jnp.zeros((CHUNKS, 8, 32, 128), F32)
        p2x[:, pl.ds(28, 4)] = jnp.zeros((CHUNKS, 4, 16, 128), F32)
        p4x[:, pl.ds(20, 4)] = jnp.zeros((CHUNKS, 4, 8, 128), F32)
        end_row_in[...] = jnp.zeros((16, 128), F32)
        dp_in[1] = jnp.zeros((32, 128), F32)

    @pl.when(jnp.logical_not(has_w))
    def _():
        rp[0] = jnp.zeros((CHUNKS, 112, 128), F32)
        col_in[...] = jnp.zeros((16, 128), F32)

    @pl.when(jnp.logical_not(has_e))
    def _():
        rp[1] = jnp.zeros((CHUNKS, 112, 128), F32)
        end_col_in[...] = jnp.zeros((16, 128), F32)

    @pl.when(jnp.logical_not(has_w & has_s))
    def _():
        corner_in[...] = jnp.zeros((16, 128), F32)

    @pl.when(jnp.logical_not(has_e & has_n))
    def _():
        end_corner_in[...] = jnp.zeros((16, 128), F32)

    def remote(src, dst, send, recv, dx, dy):
        return pltpu.make_async_remote_copy(
            src_ref=src, dst_ref=dst, send_sem=send, recv_sem=recv, device_id=at(dx, dy), device_id_type=MESH
        )

    col_copy = remote(col_out, col_in, s1.at[0], r1.at[0], 1, 0)
    row_copy = remote(row_out, row_in, s1.at[1], r1.at[1], 0, 1)
    corner_copy = remote(col_out, corner_in, s1.at[2], r1.at[2], 1, 1)
    end_row_copy = remote(comb.at[0], end_row_in, s3.at[0], r3.at[0], 0, -1)
    end_col_copy = remote(end_col_out, end_col_in, s3.at[1], r3.at[1], -1, 0)
    end_corner_copy = remote(comb.at[0], end_corner_in, s3.at[2], r3.at[2], -1, -1)

    def y_copies(c, direction, pieces=slice(0, 4)):
        if direction == 0:
            places = ((px, 32, 0, 8), (p2x, 16, 0, 4), (p4x, 8, 0, 4))
            dy = 1
        else:
            places = ((px, 9, 41, 7), (p2x, 12, 28, 4), (p4x, 12, 20, 4))
            dy = -1
        ends = [(ref.at[c, pl.ds(src, n)], ref.at[c, pl.ds(dst, n)]) for ref, src, dst, n in places]
        if direction == 1:
            ends.append((m_out.at[c], m_in.at[c]))
        return [
            remote(src, dst, ys.at[direction, c, i], yr.at[direction, c, i], 0, dy)
            for i, (src, dst) in list(enumerate(ends))[pieces]
        ]

    dp_north = remote(dp, dp_in.at[0], sf.at[2], rf.at[2], 0, 1)
    dp_south = remote(dp, dp_in.at[1], sf.at[3], rf.at[3], 0, -1)
    first_coarse = remote(c_out, c_in, sf.at[1], rf.at[1], 0, -1)

    def x_copy(c, direction):
        if direction == 0:
            return remote(sp.at[0, c], rp.at[0, c], xs.at[0, c], xr.at[0, c], 1, 0)
        return remote(sp.at[1, c], rp.at[1, c], xs.at[1, c], xr.at[1, c], -1, 0)

    lane = lax.broadcasted_iota(jnp.int32, (8, 128), 1)
    first_lane = lane == 0

    g_copies[1].wait()
    g0, g1 = gv.at[0].reshape(LEV * APAD, 128), gv.at[1].reshape(LEV * APAD, 128)

    def gradient_row(half, y, h):
        return half[pl.ds(h * 8 * APAD + y, 8, stride=APAD), :]

    for h in range(2):
        parts = []
        for quarter in range(2):
            packed = jnp.zeros((8, 128), F32)
            for y in range(quarter * 32, quarter * 32 + 32):
                packed = jnp.where(lane == y, roll(gradient_row(g1, y, h), y + 1), packed)
            parts.append(packed)
        col_out[pl.ds(h * 8, 8), :] = jnp.where(lane < 32, parts[0], parts[1])
    g_copies[0].wait()
    for h in range(2):
        row_out[0, pl.ds(h * 8, 8), :] = gradient_row(g0, 63, h)
        row_out[1, pl.ds(h * 8, 8), :] = gradient_row(g1, 63, h)

    small_copy.wait()
    for block in range(4):
        levels = pl.ds(block * 4, 4)
        value = jnp.concatenate(
            [gv[side, levels, pl.ds(0, 64), :].reshape(256, 128) for side in range(2)], axis=1
        )
        ac[levels, pl.ds(0, 64), :] = exact_dot(value, small[1]).reshape(4, 64, 128)
    ar = ac.reshape(LEV * APAD, 128)

    def across_row(y, h):
        return ar[pl.ds(h * 8 * APAD + y, 8, stride=APAD), :]

    for h in range(2):
        c_out[pl.ds(h * 8, 8), :] = across_row(0, h) + 0.5 * across_row(1, h)

    def reduce_rows(j, carry):
        odd_rows = []
        for h in range(2):
            odd = across_row(2 * j + 1, h)
            cz[j, pl.ds(h * 8, 8), :] = across_row(2 * j, h) + 0.5 * (odd + carry[h])
            odd_rows.append(odd)
        return tuple(odd_rows)

    lax.fori_loop(1, 32, reduce_rows, tuple(across_row(1, h) for h in range(2)))
    mr = mv.reshape(MEM * LEV * MPAD, 128)

    def member(c, m2, h, y):
        return mr[pl.ds(((2 * c + m2) * LEV + h * 8) * MPAD + y, 8, stride=MPAD), :]

    m_copy.wait()

    for c in range(CHUNKS):
        for m2 in range(2):
            for h in range(2):
                m_out[c, pl.ds(m2 * 16 + h * 8, 8), :] = member(c, m2, h, 0)

    def half_blocks(places):
        rows = []
        for c, k in places:
            pair = px[c, 2 * k - 8] + px[c, 2 * k - 7]
            for m2 in range(2):
                rows.append(jnp.concatenate([pair[m2 * 16 : m2 * 16 + 8], pair[m2 * 16 + 8 : m2 * 16 + 16]], axis=1))
        value = exact_dot(jnp.concatenate(rows, axis=0), small[0])
        for i, (c, k) in enumerate(places):
            p2x[c, k] = value[i * 16 : i * 16 + 16]

    def quarter_blocks(places):
        rows = []
        for c, k in places:
            pair = p2x[c, 2 * k - 8] + p2x[c, 2 * k - 7]
            rows.append(jnp.concatenate([pair[:8], pair[8:]], axis=1))
        value = exact_dot(jnp.concatenate(rows, axis=0), small[0])
        for i, (c, k) in enumerate(places):
            p4x[c, k] = value[i * 8 : i * 8 + 8]

    def quarter_blocks_of_rows(places):
        rows = [[], []]
        for c, k, row in places:
            four = (px[c, row] + px[c, row + 1]) + (px[c, row + 2] + px[c, row + 3])
            for m2 in range(2):
                rows[m2].append(jnp.concatenate([four[m2 * 16 : m2 * 16 + 8], four[m2 * 16 + 8 : m2 * 16 + 16]], axis=1))
        value = sum(exact_dot(jnp.concatenate(rows[m2], axis=0), small[2 + m2]) for m2 in range(2))
        for i, (c, k, _) in enumerate(places):
            p4x[c, k] = value[i * 8 : i * 8 + 8]

    def product_row(c, y):
        for m2 in range(2):
            for h in range(2):
                px[c, 8 + y, pl.ds(m2 * 16 + h * 8, 8), :] = member(c, m2, h, y) * cz[y, pl.ds(h * 8, 8), :]

    def start_rows(c, north, south):
        @pl.when(has_n)
        def _():
            for copy in y_copies(c, 0, north):
                copy.start()

        @pl.when(has_s)
        def _():
            for copy in y_copies(c, 1, south):
                copy.start()

    everything, nothing = slice(0, 4), slice(0, 0)

    def later_rows(c):
        def row(y, carry):
            product_row(c, y)
            return carry

        lax.fori_loop(1, 32, row, 0, unroll=4)

    def first_columns():
        @pl.when(has_w)
        def _():
            col_copy.wait_recv()

        coarse = exact_dot(jnp.concatenate([col_in[...], jnp.zeros((16, 128), F32)], axis=1), small[4])

        for m2 in range(2):
            for h in range(2):
                columns = []
                for c in range(CHUNKS):
                    column = roll(member(c, m2, h, 0), c * 32)
                    for y in range(1, 32):
                        place = c * 32 + y
                        column = jnp.where(lane == place, roll(member(c, m2, h, y), place), column)
                    columns.append(column)
                column = columns[0]
                for c in range(1, CHUNKS):
                    column = jnp.where(lane >= c * 32, columns[c], column)
                dp[pl.ds(m2 * 16 + h * 8, 8), :] = column * coarse[h * 8 : h * 8 + 8]

        @pl.when(has_n)
        def _():
            dp_north.start()

        @pl.when(has_s)
        def _():
            dp_south.start()

    def own_rows(c):
        later_rows(c)
        half_blocks([(c, k) for k in range(12, 24)])
        quarter_blocks([(c, k) for k in range(12, 16)])

    def without_first_row(c, carry):
        own_rows(c)
        start_rows(c, slice(0, 2), everything)
        return carry

    def first_row(c, carry):
        product_row(c, 0)
        half_blocks([(c, k) for k in range(8, 12)])
        quarter_blocks([(c, k) for k in range(8, 12)])
        start_rows(c, slice(2, 3), nothing)
        return carry

    def whole(c, carry):
        later_rows(c)
        product_row(c, 0)
        half_blocks([(c, k) for k in range(8, 24)])
        quarter_blocks([(c, k) for k in range(8, 16)])
        start_rows(c, everything, everything)
        return carry

    def first_coarse_row():
        @pl.when(has_s)
        def _():
            row_copy.wait_recv()

        @pl.when(has_w & has_s)
        def _():
            corner_copy.wait_recv()

        before = exact_dot(jnp.concatenate([row_in[0], row_in[1]], axis=1), small[1])
        for h in range(2):
            corner = jnp.where(first_lane, 0.5 * roll(corner_in[pl.ds(h * 8, 8), :], -63), 0.0)
            cz[0, pl.ds(h * 8, 8), :] = c_out[pl.ds(h * 8, 8), :] + 0.5 * (before[h * 8 : h * 8 + 8] + corner)

    far = (gy % 8 == 0) & has_s
    own_rows(0)
    pl.semaphore_wait(barrier, sum(there.astype(jnp.int32) for there, _, _ in around))

    @pl.when(has_e)
    def _():
        col_copy.start()

    @pl.when(has_n)
    def _():
        row_copy.start()

    @pl.when(has_e & has_n)
    def _():
        corner_copy.start()

    @pl.when(has_s)
    def _():
        first_coarse.start()

    start_rows(0, slice(0, 2), everything)

    far_west = (gx % 4 == 0) & has_w
    near_south = gy % 2 == 1
    second = 1 + far_west.astype(jnp.int32)

    @pl.when(far_west)
    def _():
        without_first_row(1, 0)

    @pl.when(near_south)
    def _():
        first_coarse_row()
        first_row(0, 0)

    first_columns()

    @pl.when(far)
    def _():
        lax.fori_loop(second, CHUNKS, without_first_row, 0)

    @pl.when(jnp.logical_not(near_south))
    def _():
        first_coarse_row()
        first_row(0, 0)

    @pl.when(far)
    def _():
        lax.fori_loop(1, CHUNKS, first_row, 0)

    @pl.when(jnp.logical_not(far) & far_west)
    def _():
        first_row(1, 0)

    @pl.when(jnp.logical_not(far))
    def _():
        lax.fori_loop(second, CHUNKS, whole, 0)

    @pl.when(has_n)
    def _():
        first_coarse.wait_recv()
        for h in range(2):
            corner = jnp.where(first_lane, 0.5 * roll(col_in[pl.ds(h * 8, 8), :], -63), 0.0)
            c_next[pl.ds(h * 8, 8), :] = c_in[pl.ds(h * 8, 8), :] + 0.5 * (across_row(63, h) + corner)

    @pl.when(has_s)
    def _():
        dp_north.wait_recv()

    @pl.when(has_n)
    def _():
        dp_south.wait_recv()

    for copy in wr_copies:
        copy.wait()
    columns = jnp.concatenate([dp_in[0], dp[...], dp_in[1]], axis=1)
    hi, lo = split(columns)
    weights = [wr[part].reshape(384, 512) for part in range(2)]
    value = dot(jnp.concatenate([hi, lo], axis=0), weights[0])
    value = value[:32] + value[32:] + dot(hi, weights[1])
    for c in range(CHUNKS):
        add_rows[c] = value[:, c * 128 : c * 128 + 128]

    def spread_additions(c):
        for target, rows, width, first in ((a1, 32, 128, 0), (a2, 16, 64, 32), (a4, 8, 32, 48)):
            parts = 128 // width
            for f in range(4 // parts):
                fields = [add_rows[c, pl.ds((f * parts + part) * 8, 8), :] for part in range(parts)]
                for y in range(rows):
                    add = jnp.zeros((8, 128), F32)
                    for part in range(parts):
                        add = jnp.where(lane == part * width, roll(fields[part], part * width - first - y), add)
                    target[c, y, pl.ds(f * 8, 8), :] = add

    low = jnp.where(has_s, 1.0, 0.0).astype(F32)
    high = jnp.where(has_n, 1.0, 0.0).astype(F32)

    def one_pass(window):
        total = window[4]
        for k in range(1, 5):
            total = total + row_taps[k] * (window[4 - k] + window[4 + k])
        return total

    def filter_rows(c, source, target, rows, fields, width, base, additions):
        group = width // 8
        place = (lane % width) // 8

        def column(f, carry):
            at_f = pl.ds(f * 8, 8)
            window, passed = [], []
            east = west = None
            for row in range(rows):
                window.append(source[c, row, at_f, :])
                if row < 8:
                    continue
                once = one_pass(window[-9:])
                if row - 8 < 4:
                    once = once * low
                if row >= rows - 4:
                    once = once * high
                passed.append(once)
                if len(passed) < 9:
                    continue
                twice = one_pass(passed[-9:])
                y = row - 16
                twice = twice + additions[c, y, at_f, :]
                target[c, y, at_f, :] = twice
                r = y % group
                to_west, to_east = roll(twice, 8 * r), roll(twice, 8 * r + 8 - width)
                if r == 0:
                    west, east = to_west, to_east
                else:
                    west, east = jnp.where(place == r, to_west, west), jnp.where(place == r, to_east, east)
                if r == group - 1:
                    start = base + (y // group) * fields + f * 8
                    sp[0, c, pl.ds(start, 8), :] = east
                    sp[1, c, pl.ds(start, 8), :] = west
            return carry

        for f in range(fields // 8):
            column(f, 0)

    outer = (gy < 2) | (gy >= ny - 2)
    defer_e = outer & has_e & (gx == nx // 2 - 1)
    defer_w = outer & has_w & (gx == nx // 2)

    def rows_stage(c):
        spread_additions(c)

        @pl.when(has_s)
        def _():
            for copy in y_copies(c, 0):
                copy.wait_recv()

        @pl.when(has_n)
        def _():
            for copy in y_copies(c, 1):
                copy.wait_recv()

        @pl.when(defer_e & (c == DEFER + 1))
        def _():
            for chunk in range(DEFER + 1):
                x_copy(chunk, 0).start()

        @pl.when(defer_w & (c == DEFER + 1))
        def _():
            for chunk in range(DEFER + 1):
                x_copy(chunk, 1).start()

        @pl.when(has_n)
        def _():
            for m2 in range(2):
                for h in range(2):
                    at_f = pl.ds(m2 * 16 + h * 8, 8)
                    px[c, 40, at_f, :] = m_in[c, at_f, :] * c_next[pl.ds(h * 8, 8), :]

        quarter_blocks_of_rows([(c, 6, 0), (c, 7, 4), (c, 16, 40), (c, 17, 44)])
        half_blocks([(c, k) for k in (4, 5, 6, 7, 24, 25, 26, 27)])
        quarter_blocks([(c, k) for k in (4, 5, 18, 19)])
        filter_rows(c, px, y1, 48, 32, 128, 0, a1)
        filter_rows(c, p2x, y2, 32, 16, 64, 64, a2)
        filter_rows(c, p4x, y4, 24, 8, 32, 96, a4)

        @pl.when(has_e & (jnp.logical_not(defer_e) | (c > DEFER)))
        def _():
            x_copy(c, 0).start()

        @pl.when(has_w & (jnp.logical_not(defer_w) | (c > DEFER)))
        def _():
            x_copy(c, 1).start()

    comb[...] = jnp.zeros((32, 16, 128), F32)
    w1_copy.wait()
    w2_copy.wait()
    w4_copy.wait()

    def halo(c, start, fields, r, width):
        west, east = rp[0, c, pl.ds(start, fields), :], rp[1, c, pl.ds(start, fields), :]
        take_west = lax.broadcasted_iota(jnp.int32, (fields, 128), 1) % width < 8
        return jnp.where(take_west, roll(west, -8 * r), roll(east, 8 - 8 * r))

    def columns_stage(c):
        @pl.when(has_w)
        def _():
            x_copy(c, 0).wait_recv()

        @pl.when(has_e)
        def _():
            x_copy(c, 1).wait_recv()

        sides = [halo(c, 96 + (q // 4) * 8, 8, q % 4, 32) for q in range(8)]
        value = jnp.concatenate([y4[c].reshape(64, 128), jnp.concatenate(sides, axis=0)], axis=1)
        o4[...] = full_dot(value, w4[0], w4[1])
        sides = [halo(c, 64 + (q // 8) * 16, 16, q % 8, 64) for q in range(16)]
        value = jnp.concatenate([y2[c].reshape(256, 128), jnp.concatenate(sides, axis=0)], axis=1)
        o2[...] = full_dot(value, w2[0], w2[1])

        def block(b, carry):
            @pl.when((b == 1) & (c == CHUNKS - 1) & has_s)
            def _():
                end_row_copy.start()

            @pl.when((b == 1) & (c == CHUNKS - 1) & has_w & has_s)
            def _():
                end_corner_copy.start()

            for part in range(2):
                first = b * 16 + part * 8
                start = pl.multiple_of(b * 32, 32)
                sides = [halo(c, start, 32, part * 8 + r, 128) for r in range(8)]
                rows = y1[c, pl.ds(first, 8)].reshape(256, 128)
                both = exact_dot(jnp.concatenate([rows, jnp.concatenate(sides, axis=0)], axis=1), w1[...])
                value = both[:, :128] + both[:, 128:]
                for r in range(8):
                    y = first + r
                    at2 = pl.multiple_of((b * 8 + part * 4 + r // 2) * 16, 16)
                    at4 = pl.multiple_of((b * 4 + part * 2 + r // 4) * 8, 8)
                    for h in range(2):
                        total = comb[y, pl.ds(h * 8, 8), :]
                        for m2 in range(2):
                            begin = r * 32 + m2 * 16 + h * 8
                            local = value[begin : begin + 8]
                            local = local + o2[pl.ds(at2 + m2 * 8, 8), pl.ds(h * 128, 128)]
                            local = local + o4[pl.ds(at4, 8), pl.ds((m2 * 2 + h) * 128, 128)]
                            total = total + member(c, m2, h, y) * local
                        comb[y, pl.ds(h * 8, 8), :] = total
            return carry

        lax.fori_loop(0, 2, block, 0)

    def stages(step, carry):
        @pl.when(step < CHUNKS)
        def _():
            rows_stage(step)

        @pl.when(step >= LAG)
        def _():
            columns_stage(step - LAG)

        return carry

    lax.fori_loop(0, CHUNKS + LAG, stages, 0)

    for h in range(2):
        packed = comb[0, pl.ds(h * 8, 8), :]
        for y in range(1, 32):
            packed = jnp.where(lane == y, roll(comb[y, pl.ds(h * 8, 8), :], y), packed)
        end_col_out[pl.ds(h * 8, 8), :] = packed

    @pl.when(has_w)
    def _():
        end_col_copy.start()

    def send_waits(c, carry):
        @pl.when(has_n)
        def _():
            for copy in y_copies(c, 0):
                copy.wait_send()

        @pl.when(has_s)
        def _():
            for copy in y_copies(c, 1):
                copy.wait_send()

        @pl.when(has_e)
        def _():
            x_copy(c, 0).wait_send()

        @pl.when(has_w)
        def _():
            x_copy(c, 1).wait_send()

        return carry

    spread_copy.wait()
    flats = [out.at[side].reshape(LEV * APAD, 128) for side in range(2)]

    def store_row(y, side, h, value):
        flats[side][pl.ds(h * 8 * APAD + y, 8, stride=APAD), :] = value

    def row_of(y, h):
        return flats[1][pl.ds(h * 8 * APAD + y, 8, stride=APAD), :]

    for block in range(4):
        rows = []
        for j in range(block * 8, block * 8 + 8):
            rows += [comb[j], 0.5 * (comb[j] + comb[j + 1])] if j < 31 else [comb[j]]
        value = exact_dot(jnp.concatenate(rows, axis=0), spread[pl.ds(0, 128), :])
        for k in range(len(rows)):
            for h in range(2):
                for side in range(2):
                    begin = k * 16 + h * 8
                    store_row(block * 16 + k, side, h, value[begin : begin + 8, side * 128 : side * 128 + 128])

    lax.fori_loop(0, CHUNKS, send_waits, 0)

    @pl.when(has_e)
    def _():
        col_copy.wait_send()
        end_col_copy.wait_recv()

    @pl.when(has_n)
    def _():
        row_copy.wait_send()
        dp_north.wait_send()
        end_row_copy.wait_recv()

    @pl.when(has_e & has_n)
    def _():
        corner_copy.wait_send()
        end_corner_copy.wait_recv()

    for h in range(2):
        levels = pl.ds(h * 8, 8)
        edge = jnp.where(lane == 32, roll(end_corner_in[levels, :], 32), end_col_in[levels, :])
        half_edge = 0.5 * (edge + roll(edge, -1))
        for y in range(63):
            add = roll((half_edge, edge)[y % 2 == 0], 127 - y // 2)
            store_row(y, 1, h, row_of(y, h) + jnp.where(lane == 127, 0.5 * add, 0.0))
        last = 0.5 * (comb[31, levels, :] + end_row_in[levels, :])
        value = exact_dot(jnp.concatenate([last, roll(half_edge, -31)], axis=1), spread[...])
        for side in range(2):
            store_row(63, side, h, value[:, side * 128 : side * 128 + 128])

    @pl.when(has_s)
    def _():
        end_row_copy.wait_send()
        first_coarse.wait_send()
        dp_south.wait_send()

    @pl.when(has_w)
    def _():
        end_col_copy.wait_send()

    @pl.when(has_w & has_s)
    def _():
        end_corner_copy.wait_send()


def output_kernel(padded, out_hbm, sem):
    copies = [
        pltpu.make_async_copy(
            padded.at[side, :, pl.ds(0, 64), :], out_hbm.at[:, :, pl.ds(side * 128, 128)], sem.at[side]
        )
        for side in range(2)
    ]
    for copy in copies:
        copy.start()
    for copy in copies:
        copy.wait()


def shards(nx, ny, gradient, members):
    filters, rows, small, spread = constants()
    w1, w2, w4 = (jnp.asarray(value) for value in filters)
    any_space = pl.BlockSpec(memory_space=pltpu.HBM)
    in_vmem = pl.BlockSpec(memory_space=pltpu.VMEM)
    dma = pltpu.SemaphoreType.DMA

    def vmem(*shape, dtype=F32):
        return pltpu.VMEM(shape, dtype)

    padded = pl.pallas_call(
        functools.partial(main_kernel, nx, ny),
        name="localise",
        out_shape=jax.ShapeDtypeStruct((2, LEV, APAD, 128), F32),
        in_specs=[any_space] * 8,
        out_specs=in_vmem,
        scratch_shapes=[
            vmem(2, LEV, APAD, 128),
            vmem(MEM, LEV, MPAD, 128),
            vmem(256, 256, dtype=BF16),
            vmem(2, 256, 256, dtype=BF16),
            vmem(2, 256, 512, dtype=BF16),
            vmem(2, 3, 128, 512, dtype=BF16),
            vmem(5, 256, 128, dtype=BF16),
            vmem(256, 256, dtype=BF16),
            vmem(32, 16, 128),
            vmem(LEV, APAD, 128),
            vmem(32, 16, 128),
            vmem(CHUNKS, 48, 32, 128),
            vmem(CHUNKS, 32, 16, 128),
            vmem(CHUNKS, 24, 8, 128),
            vmem(CHUNKS, 32, 32, 128),
            vmem(CHUNKS, 16, 16, 128),
            vmem(CHUNKS, 8, 8, 128),
            vmem(2, CHUNKS, 112, 128),
            vmem(2, CHUNKS, 112, 128),
            vmem(256, 256),
            vmem(64, 512),
            vmem(16, 128),
            vmem(16, 128),
            vmem(2, 16, 128),
            vmem(2, 16, 128),
            vmem(16, 128),
            vmem(CHUNKS, 32, 128),
            vmem(CHUNKS, 32, 128),
            vmem(16, 128),
            vmem(16, 128),
            vmem(16, 128),
            vmem(32, 128),
            vmem(2, 32, 128),
            vmem(CHUNKS, 32, 128),
            vmem(CHUNKS, 32, 32, 128),
            vmem(CHUNKS, 16, 16, 128),
            vmem(CHUNKS, 8, 8, 128),
            vmem(16, 128),
            vmem(16, 128),
            vmem(16, 128),
            vmem(16, 128),
            dma((8,)),
            dma((2, 3, CHUNKS)),
            dma((3,)),
            dma((3,)),
            dma((4,)),
            dma((4,)),
            dma((2, CHUNKS, 4)),
            dma((2, CHUNKS, 4)),
            dma((2, CHUNKS)),
            dma((2, CHUNKS)),
            dma((3,)),
            dma((3,)),
        ],
        compiler_params=pltpu.CompilerParams(collective_id=0, has_side_effects=True, vmem_limit_bytes=48 << 20),
    )(*(pltpu.with_memory_space_constraint(value, pltpu.HBM) for value in (gradient, members, w1, w2, w4, jnp.asarray(rows), jnp.asarray(small), jnp.asarray(spread))))
    return pl.pallas_call(
        output_kernel,
        name="output",
        out_shape=jax.ShapeDtypeStruct((LEV, 64, 256), F32),
        in_specs=[in_vmem],
        out_specs=any_space,
        scratch_shapes=[dma((2,))],
        compiler_params=pltpu.CompilerParams(vmem_limit_bytes=8 << 20),
    )(padded)


def solution(mesh):
    in_specs = (P(None, "gy", "gx"), P(None, None, "gy", "gx"))
    return jax.shard_map(
        functools.partial(shards, mesh.shape["gx"], mesh.shape["gy"]),
        mesh=mesh,
        in_specs=in_specs,
        out_specs=P(None, "gy", "gx"),
        check_vma=False,
    )
```
